128 devices in a mesh: tm: 32 (over z_hi, y, x), freq: 4 (over z_lo, core).
Axes of the slice: x: 4, y: 4, z: 4 (z_hi: 2, z_lo: 2; z = z_hi * 2 + z_lo), core: 2. Of those that a mesh axis runs over, the one named last changes fastest.
Arguments:
- sfts: float32 [1536, 2, 4096], P('tm', None, 'freq'), may hold values from -40 to 40
- detector_ids: int32 [1536], replicated, may hold values from 0 to 2
- intersection: float32 [3, 3], replicated, may hold values from 0.3 to 1
- lags: int32 [12], replicated, may hold values from 1 to 16, as said below
- template_ids: int32 [4096, 2], P('tm'), may hold values from 0 to 63
Outputs:
- stat: float32 [4096, 4096], P('tm', 'freq')
The draws below stay inside these ranges and needn't reach their ends.
Inputs may be any that keep to these rules, and one draw needn't show every extreme that they name: 12 distinct lags, one of them 16.
All inputs are finite; a program needn't handle non-finite values.
Results may differ from the reference program's by a relative error of at most 0.009.
Values may be sent and summed in bfloat16 or wider, within the bound.
A program may use at most 64 MiB of HBM per device.

```python
import math
import jax
import jax.numpy as jnp
from jax import lax

NBIN = 4096
NTEMPL = 4096
LAGMAX = 16
NLAG = 12
NDET = 3
NGRID = 64
PERIOD = 283
SFT_DEV = 48
NSFT = 1536


def draw_sfts(key, part):
    key_base = jax.random.fold_in(key, 11)
    key_rough = jax.random.fold_in(key, 12)
    key_rows = jax.random.fold_in(key, 13)
    bins = jnp.arange(NBIN, dtype=jnp.float32)
    ramp = jnp.exp(0.55 * bins / NBIN)
    rough = jax.random.uniform(key_rough, (NBIN,), jnp.float32, 0.6, 1.4)
    base = jnp.clip(jax.random.normal(key_base, (NSFT, 2, NBIN), jnp.float32), -6.0, 6.0)
    row_scale = jnp.exp(jax.random.uniform(key_rows, (NSFT,), jnp.float32, math.log(0.5), math.log(2.0)))
    values = base * row_scale[:, None, None] * (ramp * rough)[None, None, :]
    return jnp.clip(values, -40.0, 40.0).astype(jnp.float32)


def draw_lags(key, part):
    order = jax.random.permutation(jax.random.fold_in(key, 21), LAGMAX - 1)[:NLAG - 1].astype(jnp.int32) + 1
    return jnp.concatenate([jnp.full((1,), LAGMAX, jnp.int32), order])


def place_ends(array, stream_key, least, largest):
    longest = array.shape.index(max(array.shape))
    spots = []
    for shift in (0, 1):
        where = [jax.random.randint(jax.random.fold_in(stream_key, axis), (), 0, length) for axis, length in enumerate(array.shape)]
        where[longest] = (where[longest] + shift) % array.shape[longest]
        spots.append(tuple(where))
    return array.at[spots[0]].set(least).at[spots[1]].set(largest)


def setup_inputs(seed: int = 0) -> dict:
    key_list = jax.random.split(jax.random.key(seed), 6)
    sfts = draw_sfts(jax.random.fold_in(key_list[5], 71), 0)
    detector_ids = place_ends(jax.random.randint(key_list[1], (NSFT,), 0, NDET), jax.random.fold_in(key_list[1], 1), 0, NDET - 1).astype(jnp.int32)
    intersection = jnp.clip(jax.random.uniform(key_list[2], (NDET, NDET), jnp.float32, 0.3, 1.0), 0.3, 1.0)
    lags = draw_lags(jax.random.fold_in(key_list[5], 71), 0)
    template_ids = place_ends(jax.random.randint(key_list[4], (NTEMPL, 2), 0, NGRID), jax.random.fold_in(key_list[4], 1), 0, NGRID - 1).astype(jnp.int32)
    return {"sfts": sfts, "detector_ids": detector_ids, "intersection": intersection, "lags": lags, "template_ids": template_ids}


def block_term(extended, first_row, ids_padded, lag_list, intersection, amplitude_idx, phase_idx, total):
    span = extended.shape[0] - LAGMAX
    here = jnp.arange(span, dtype=jnp.int32)
    partner = here[None, :] + lag_list[:, None]
    own_rows = extended[:span].astype(jnp.float32)
    far_rows = extended[partner].astype(jnp.float32)
    det_block = lax.dynamic_slice_in_dim(ids_padded, first_row, extended.shape[0], 0)
    det_near = det_block[:span]
    det_far = det_block[partner]
    levels = jnp.arange(intersection.shape[0], dtype=jnp.int32)
    hot_near = (det_near[:, None] == levels[None, :]).astype(jnp.float32)
    hot_far = (det_far[:, :, None] == levels[None, None, :]).astype(jnp.float32)
    weight = jnp.einsum('sa,ab,lsb->ls', hot_near, intersection.astype(jnp.float32), hot_far)
    inside = first_row + partner < total
    weight = jnp.where(inside, weight, jnp.float32(0.0))
    re_own = own_rows[None, :, 0]
    im_own = own_rows[None, :, 1]
    re_far = far_rows[:, :, 0]
    im_far = far_rows[:, :, 1]
    pair_re = (weight[:, :, None] * (re_own * re_far + im_own * im_far)).astype(jnp.bfloat16)
    pair_im = (weight[:, :, None] * (re_own * im_far - im_own * re_far)).astype(jnp.bfloat16)
    width = extended.shape[2]
    stacked = jnp.concatenate([pair_re.reshape(-1, width), pair_im.reshape(-1, width)], 0)
    position = first_row + jnp.arange(extended.shape[0], dtype=jnp.int32)
    orbit = 2.0 * math.pi / PERIOD * (position % PERIOD).astype(jnp.float32)
    offset = 2.0 * math.pi / NGRID * phase_idx.astype(jnp.float32)
    sine = jnp.sin(offset[:, None] + orbit[None, :])
    amplitude = 8.0 + 4.0 * amplitude_idx.astype(jnp.float32)
    phase = amplitude[:, None, None] * (sine[:, partner] - sine[:, None, :span])
    rows = phase.shape[0]
    factors = jnp.concatenate([jnp.cos(phase).reshape(rows, -1).astype(jnp.bfloat16), jnp.sin(phase).reshape(rows, -1).astype(jnp.bfloat16)], 1)
    return jnp.dot(factors, stacked, preferred_element_type=jnp.float32)

def reference(sfts, detector_ids, intersection, lags, template_ids):
    power = lax.optimization_barrier(jnp.sum(sfts[:, 0] * sfts[:, 0] + sfts[:, 1] * sfts[:, 1], axis=1)) / NBIN
    white = (sfts * lax.rsqrt(power + 1e-06)[:, None, None]).astype(jnp.bfloat16)
    padded = jnp.pad(white, ((0, LAGMAX), (0, 0), (0, 0)))
    ids_padded = jnp.pad(detector_ids, (0, LAGMAX))
    total = sfts.shape[0]

    def add_block(number, totals):
        first_row = (number * SFT_DEV).astype(jnp.int32)
        extended = lax.dynamic_slice_in_dim(padded, first_row, SFT_DEV + LAGMAX, 0)
        return totals + block_term(extended, first_row, ids_padded, lags, intersection, template_ids[:, 0], template_ids[:, 1], total)
    totals = lax.fori_loop(0, total // SFT_DEV, add_block, jnp.zeros((NTEMPL, NBIN), jnp.float32))
    return totals * jnp.float32(1.0 / math.sqrt(total * NLAG))
```

```python
import math

import jax
import jax.numpy as jnp
from jax import lax
from jax.experimental import pallas as pl
from jax.experimental.pallas import tpu as pltpu
from jax.sharding import PartitionSpec as P

NSFT = 1536
NBIN = 4096
LAGMAX = 16
NLAG = 12
NDET = 3
NGRID = 64
PERIOD = 283
TM = 32
SPAN = 48
FOLD = 288
TURNS = 6
LANES = 128
ROWS = 1792
ZROWS = 304
DEPTH = 2 * NLAG * FOLD
PART = 1024
MESH = pl.DeviceIdType.MESH

COS = (0.9999999890590238, -19.739204499453965, 64.93911745989729, -85.45013953090921,
       60.167630951124465, -25.967599248993793, 6.528658161871135)
SIN = (6.28318527244795, -41.34169703820007, 81.60502363804078, -76.7015376703427,
       42.016075762415646, -14.86832275264805, 3.199338844584104)


def cos_sin(turns):
    u = turns - jnp.floor(turns + 0.5)
    t = u * u
    c = jnp.full_like(t, COS[-1])
    for k in COS[-2::-1]:
        c = c * t + k
    s = jnp.full_like(t, SIN[-1])
    for k in SIN[-2::-1]:
        s = s * t + k
    return c, s * u


def kernel(x_ref, det_ref, tid_ref, inter_ref, lag_ref, o_ref,
           pbuf, idbuf, send_buf, xrecv, osend, orecv,
           xre, xim, det, mat, wl, zc, zs, fac, pairs, pairs_t, acc,
           p_send, p_recv, i_send, i_recv, c_send, c_recv, f_send, o_send, o_recv):
    tm = lax.axis_index("tm")
    h = lax.axis_index("freq")
    core = h % 2
    f32 = jnp.float32
    home = (tm // 8) == h
    own_chunk = jnp.logical_and(home, (tm % 2) == core)
    own_ids = jnp.logical_and(home, (tm % 4) == h)

    barrier = pltpu.get_barrier_semaphore()

    def hail(peer_tm, peer_h, unless):
        @pl.when(jnp.logical_not(unless))
        def _():
            pl.semaphore_signal(barrier, inc=1, device_id=(peer_tm, peer_h), device_id_type=MESH)

    for k in range(8):
        for lo in range(2):
            to_tm, to_h = 8 * h + k, 2 * lo + tm % 2
            hail(to_tm, to_h, jnp.logical_and(to_tm == tm, to_h == h))
    for s in range(16):
        from_tm, from_h = 2 * s + core, tm // 8
        hail(from_tm, from_h, jnp.logical_and(from_tm == tm, from_h == h))
    for d in range(1, 4):
        pl.semaphore_signal(barrier, inc=1, device_id=(tm, (h + d) % 4), device_id_type=MESH)

    re = x_ref[:, 0, :]
    im = x_ref[:, 1, :]
    sq = re * re + im * im
    part = sq[:, 0:LANES]
    for k in range(1, 8):
        part = part + sq[:, k * LANES:(k + 1) * LANES]
    pbuf[h] = part
    idx = tm // 4

    @pl.when(own_chunk)
    def _():
        pl.semaphore_wait(barrier, 33)

    @pl.when(jnp.logical_not(own_chunk))
    def _():
        pl.semaphore_wait(barrier, 35)

    power_copies = []
    for d in range(1, 4):
        copy = pltpu.make_async_remote_copy(
            src_ref=pbuf.at[h], dst_ref=pbuf.at[h], send_sem=p_send.at[d], recv_sem=p_recv.at[4 - d],
            device_id=(tm, (h + d) % 4), device_id_type=MESH)
        copy.start()
        power_copies.append(copy)

    def id_copy(k):
        return pltpu.make_async_remote_copy(
            src_ref=tid_ref, dst_ref=idbuf.at[idx], send_sem=i_send.at[k], recv_sem=i_recv.at[idx],
            device_id=(8 * h + k, tm % 4), device_id_type=MESH)

    def id_is_me(k):
        return jnp.logical_and(8 * h + k == tm, tm % 4 == h)

    for k in range(8):
        @pl.when(jnp.logical_not(id_is_me(k)))
        def _(k=k):
            id_copy(k).start()

    @pl.when(own_ids)
    def _():
        idbuf[idx] = tid_ref[...]

    det[...] = jnp.zeros_like(det)
    for k in range(12):
        row = jnp.broadcast_to(det_ref[k:k + 1, :].astype(f32), (LANES, LANES))
        det[k * LANES:(k + 1) * LANES, :] = row.T

    def mat_rows(b, carry):
        r0 = pl.multiple_of(b * 16, 16)
        d = det[pl.ds(r0, 16), :]
        real = lax.broadcasted_iota(jnp.int32, (16, LANES), 0) + r0 < NSFT
        for e in range(NDET):
            m = jnp.where(d == 0.0, inter_ref[e, 0], jnp.where(d == 1.0, inter_ref[e, 1], inter_ref[e, 2]))
            mat[e, pl.ds(r0, 16), :] = jnp.where(real, m, 0.0)
        return carry

    lax.fori_loop(0, ROWS // 16, mat_rows, 0)

    def weight_rows(b, carry):
        r0 = pl.multiple_of(b * 16, 16)
        d = det[pl.ds(r0, 16), :]
        for l in range(NLAG):
            at = pl.ds(r0 + lag_ref[l], 16)
            wl[l, pl.ds(r0, 16), :] = jnp.where(
                d == 0.0, mat[0, at, :], jnp.where(d == 1.0, mat[1, at, :], mat[2, at, :]))
        return carry

    lax.fori_loop(0, NSFT // 16, weight_rows, 0)
    for l in range(NLAG):
        wl[l, NSFT:, :] = jnp.zeros((ROWS - LAGMAX - NSFT, LANES), f32)
    xre[NSFT:, :] = jnp.zeros((ROWS - NSFT, LANES), f32)
    xim[NSFT:, :] = jnp.zeros((ROWS - NSFT, LANES), f32)

    for copy in power_copies:
        copy.wait()
    power = jnp.sum((pbuf[0] + pbuf[1]) + (pbuf[2] + pbuf[3]), axis=1, keepdims=True) / NBIN
    inv = lax.rsqrt(power + 1e-06)
    re = x_ref[:, 0, :] * inv
    im = x_ref[:, 1, :] * inv
    for k in range(8):
        send_buf[k, 0:SPAN, :] = re[:, k * LANES:(k + 1) * LANES].astype(jnp.bfloat16)
        send_buf[k, SPAN:, :] = im[:, k * LANES:(k + 1) * LANES].astype(jnp.bfloat16)

    def chunk_copy(k, lo):
        return pltpu.make_async_remote_copy(
            src_ref=send_buf.at[k], dst_ref=xrecv.at[tm], send_sem=c_send.at[2 * k + lo], recv_sem=c_recv.at[tm],
            device_id=(8 * h + k, 2 * lo + tm % 2), device_id_type=MESH)

    def chunk_is_me(k, lo):
        return jnp.logical_and(8 * h + k == tm, 2 * lo + tm % 2 == h)

    for k in range(8):
        for lo in range(2):
            @pl.when(jnp.logical_not(chunk_is_me(k, lo)))
            def _(k=k, lo=lo):
                chunk_copy(k, lo).start()

    @pl.when(own_chunk)
    def _():
        xrecv[tm] = send_buf[tm % 8]

    def id_from(s):
        return pltpu.make_async_remote_copy(
            src_ref=tid_ref, dst_ref=idbuf.at[s], send_sem=i_send.at[0], recv_sem=i_recv.at[s],
            device_id=(4 * s + h, tm // 8), device_id_type=MESH)

    for s in range(8):
        @pl.when(jnp.logical_not(jnp.logical_and(4 * s + h == tm, tm // 8 == h)))
        def _(s=s):
            id_from(s).wait_recv()

    for s in range(8):
        ids = idbuf[s].astype(f32)
        amp = (8.0 + 4.0 * ids[0:1, :]) * (0.5 / math.pi)
        cq, sq_ = cos_sin(ids[1:2, :] * (1.0 / NGRID))
        ac = jnp.broadcast_to(amp * cq, (8, LANES))
        as_ = jnp.broadcast_to(amp * sq_, (8, LANES))

        def z_rows(b, carry, s=s, ac=ac, as_=as_):
            r0 = pl.multiple_of(b * 8, 8)
            row = lax.broadcasted_iota(jnp.int32, (8, LANES), 0) + r0
            row = jnp.where(row >= PERIOD, row - PERIOD, row).astype(f32)
            cr, sr = cos_sin(row * (1.0 / PERIOD))
            c, si = cos_sin(sr * ac + cr * as_)
            zc[s, pl.ds(r0, 8), :] = c
            zs[s, pl.ds(r0, 8), :] = si
            return carry

        lax.fori_loop(0, ZROWS // 8, z_rows, 0)

    def factor_rows(n, carry):
        l, b = n // 18, n % 18
        r0 = pl.multiple_of(b * 16, 16)
        lag = lag_ref[l]
        out = pl.multiple_of(l * (2 * FOLD) + r0, 16)
        for s in range(8):
            ci, si = zc[s, pl.ds(r0, 16), :], zs[s, pl.ds(r0, 16), :]
            cj, sj = zc[s, pl.ds(r0 + lag, 16), :], zs[s, pl.ds(r0 + lag, 16), :]
            at = slice(s * LANES, (s + 1) * LANES)
            fac[pl.ds(out, 16), at] = (cj * ci + sj * si).astype(jnp.bfloat16)
            fac[pl.ds(out + FOLD, 16), at] = (sj * ci - cj * si).astype(jnp.bfloat16)
        return carry

    lax.fori_loop(0, NLAG * 18, factor_rows, 0)

    def chunk_from(src):
        return pltpu.make_async_remote_copy(
            src_ref=xrecv.at[src], dst_ref=xrecv.at[src], send_sem=c_send.at[0], recv_sem=c_recv.at[src],
            device_id=(tm, h), device_id_type=MESH)

    def forward(s):
        src = 2 * s + core
        return pltpu.make_async_remote_copy(
            src_ref=xrecv.at[src], dst_ref=xrecv.at[src], send_sem=f_send.at[s], recv_sem=c_recv.at[src],
            device_id=(tm, h + 1 - 2 * core), device_id_type=MESH)

    for s in range(16):
        @pl.when(jnp.logical_not(jnp.logical_and(2 * s + core == tm, tm // 8 == h)))
        def _(s=s):
            pltpu.make_async_remote_copy(
                src_ref=xrecv.at[2 * s + core], dst_ref=xrecv.at[2 * s + core], send_sem=c_send.at[0],
                recv_sem=c_recv.at[2 * s + core], device_id=(2 * s + core, tm // 8),
                device_id_type=MESH).wait_recv()
        forward(s).start()
    for s in range(16):
        pltpu.make_async_remote_copy(
            src_ref=xrecv.at[2 * s + 1 - core], dst_ref=xrecv.at[2 * s + 1 - core], send_sem=f_send.at[s],
            recv_sem=c_recv.at[2 * s + 1 - core], device_id=(tm, h + 1 - 2 * core),
            device_id_type=MESH).wait_recv()

    def unpack(b, carry):
        at = pl.ds(pl.multiple_of(b * SPAN, 16), SPAN)
        xre[at, :] = xrecv[b, 0:SPAN, :].astype(f32)
        xim[at, :] = xrecv[b, SPAN:, :].astype(f32)
        return carry

    lax.fori_loop(0, TM, unpack, 0)

    def pair_rows(n, carry):
        b, l = n // NLAG, n % NLAG
        r0 = pl.multiple_of(b * 16, 16)
        lag = lag_ref[l]
        real = lax.broadcasted_iota(jnp.int32, (16, LANES), 0) + r0 < PERIOD
        sum_re = jnp.zeros((16, LANES), f32)
        sum_im = jnp.zeros((16, LANES), f32)
        for m in range(TURNS):
            here = pl.ds(r0 + PERIOD * m, 16)
            far = pl.ds(r0 + PERIOD * m + lag, 16)
            w = wl[l, here, :]
            a, bb = xre[here, :] * w, xim[here, :] * w
            c, d = xre[far, :], xim[far, :]
            sum_re = sum_re + (a * c + bb * d)
            sum_im = sum_im + (a * d - bb * c)
        out = pl.multiple_of(l * (2 * FOLD) + r0, 16)
        pairs[pl.ds(out, 16), :] = jnp.where(real, sum_re, 0.0)
        pairs[pl.ds(out + FOLD, 16), :] = jnp.where(real, sum_im, 0.0)
        return carry

    lax.fori_loop(0, NLAG * 18, pair_rows, 0)

    def turn(b, carry):
        at = pl.ds(pl.multiple_of(b * LANES, LANES), LANES)
        pairs_t[:, at] = pairs[at, :].T.astype(jnp.bfloat16)
        return carry

    lax.fori_loop(0, DEPTH // LANES, turn, 0)

    acc[...] = jnp.zeros_like(acc)

    def multiply(b, carry):
        at = pl.ds(pl.multiple_of(b * 768, 256), 768)
        acc[...] += jnp.dot(pairs_t[:, at], fac[at, :], preferred_element_type=f32)
        return carry

    lax.fori_loop(0, DEPTH // 768, multiply, 0)

    scale = 1.0 / math.sqrt(NSFT * NLAG)
    group = tm // 8

    def out_copy(s):
        return pltpu.make_async_remote_copy(
            src_ref=osend.at[s], dst_ref=orecv.at[tm % 8], send_sem=o_send.at[s], recv_sem=o_recv.at[tm % 8],
            device_id=(4 * s + h, group), device_id_type=MESH)

    def out_is_me(s):
        return jnp.logical_and(4 * s + h == tm, group == h)

    for s in range(8):
        osend[s] = (acc[:, s * LANES:(s + 1) * LANES].T * scale).astype(jnp.bfloat16)

        @pl.when(jnp.logical_not(out_is_me(s)))
        def _(s=s):
            out_copy(s).start()

    @pl.when(own_ids)
    def _():
        orecv[tm % 8] = osend[tm // 4]

    for k in range(8):
        @pl.when(jnp.logical_not(jnp.logical_and(8 * h + k == tm, tm % 4 == h)))
        def _(k=k):
            pltpu.make_async_remote_copy(
                src_ref=osend.at[k], dst_ref=orecv.at[k], send_sem=o_send.at[k], recv_sem=o_recv.at[k],
                device_id=(8 * h + k, tm % 4), device_id_type=MESH).wait_recv()
        o_ref[:, k * LANES:(k + 1) * LANES] = orecv[k]

    for k in range(8):
        @pl.when(jnp.logical_not(id_is_me(k)))
        def _(k=k):
            id_copy(k).wait_send()
        for lo in range(2):
            @pl.when(jnp.logical_not(chunk_is_me(k, lo)))
            def _(k=k, lo=lo):
                chunk_copy(k, lo).wait_send()

        @pl.when(jnp.logical_not(out_is_me(k)))
        def _(k=k):
            out_copy(k).wait_send()
    for s in range(16):
        forward(s).wait_send()


def shards(sfts, detector_ids, intersection, lags, template_ids):
    bf16, f32 = jnp.bfloat16, jnp.float32
    vmem = pl.BlockSpec(memory_space=pltpu.VMEM)
    smem = pl.BlockSpec(memory_space=pltpu.SMEM)
    dma = pltpu.SemaphoreType.DMA
    out = pl.pallas_call(
        kernel,
        out_shape=jax.ShapeDtypeStruct((LANES, 8 * LANES), bf16),
        in_specs=[vmem, vmem, vmem, smem, smem],
        out_specs=vmem,
        scratch_shapes=[
            pltpu.VMEM((4, SPAN, LANES), f32),
            pltpu.VMEM((8, 2, LANES), jnp.int32),
            pltpu.VMEM((8, 2 * SPAN, LANES), bf16),
            pltpu.VMEM((TM, 2 * SPAN, LANES), bf16),
            pltpu.VMEM((8, LANES, LANES), bf16),
            pltpu.VMEM((8, LANES, LANES), bf16),
            pltpu.VMEM((ROWS, LANES), f32),
            pltpu.VMEM((ROWS, LANES), f32),
            pltpu.VMEM((ROWS + LAGMAX, LANES), f32),
            pltpu.VMEM((NDET, ROWS + LAGMAX, LANES), f32),
            pltpu.VMEM((NLAG, ROWS - LAGMAX, LANES), f32),
            pltpu.VMEM((8, ZROWS, LANES), f32),
            pltpu.VMEM((8, ZROWS, LANES), f32),
            pltpu.VMEM((DEPTH, PART), bf16),
            pltpu.VMEM((DEPTH, LANES), f32),
            pltpu.VMEM((LANES, DEPTH), bf16),
            pltpu.VMEM((LANES, PART), f32),
            dma((4,)), dma((4,)), dma((8,)), dma((8,)), dma((16,)), dma((TM,)), dma((16,)), dma((8,)), dma((8,)),
        ],
        compiler_params=pltpu.CompilerParams(
            collective_id=0, has_side_effects=True, vmem_limit_bytes=60 * 1024 * 1024),
    )(sfts, detector_ids.reshape(12, LANES), template_ids.T, intersection, lags)
    return out.astype(f32)


def solution(mesh):
    in_specs = (P("tm", None, "freq"), P(), P(), P(), P("tm", None))
    out_specs = P("tm", "freq")
    return jax.shard_map(shards, mesh=mesh, in_specs=in_specs, out_specs=out_specs, check_vma=False)
```

```python
import functools
import math

import jax
import jax.numpy as jnp
from jax import lax
from jax.experimental import pallas as pl
from jax.experimental.pallas import tpu as pltpu
from jax.sharding import PartitionSpec as P

NSFT = 1536
NBIN = 4096
LAGMAX = 16
NLAG = 12
NDET = 3
NGRID = 64
PERIOD = 283
TM = 32
SPAN = 48
FOLD = 288
TURNS = 6
LANES = 128
ROWS = 1792
ZROWS = 304
DEPTH = 2 * NLAG * FOLD
PART = 1024
WIDE = 256
MESH = pl.DeviceIdType.MESH

COS = (0.9999999890590238, -19.739204499453965, 64.93911745989729, -85.45013953090921,
       60.167630951124465, -25.967599248993793, 6.528658161871135)
SIN = (6.28318527244795, -41.34169703820007, 81.60502363804078, -76.7015376703427,
       42.016075762415646, -14.86832275264805, 3.199338844584104)


def cos_sin(turns):
    u = turns - jnp.floor(turns + 0.5)
    t = u * u
    c = jnp.full_like(t, COS[-1])
    for k in COS[-2::-1]:
        c = c * t + k
    s = jnp.full_like(t, SIN[-1])
    for k in SIN[-2::-1]:
        s = s * t + k
    return c, s * u


def kernel(x_hbm, det_hbm, tid_hbm, inter_ref, lag_ref, o_ref,
           x_ref, det_ref, tid_ref, pbuf, gsend, gbuf, idbuf, send_buf, xrecv, osend, orecv,
           xre, xim, det, mat, wl, amp_cos, amp_sin, zc, zs, fac, pairs, pairs_t,
           l_sem, p_send, p_recv, i_send, i_recv, g_send, g_recv, c_send, c_recv, fg_send, f_send, o_send, o_recv):
    tm = lax.axis_index("tm")
    h = lax.axis_index("freq")
    core, z_lo = h % 2, h // 2
    x = tm % 4
    f32, bf16 = jnp.float32, jnp.bfloat16

    quarter = (1 - z_lo) * 2 + x % 2
    group = 2 * (x // 2) + core

    def home(k, e):
        return 4 * k + core + 2 * e, (1 - z_lo) * 2 + x % 2

    def source(s):
        return 4 * (s // 2) + 2 * (s % 2) + core, quarter

    def owner(s):
        return 4 * s + group, quarter

    def remote(src, dst, send, recv, to):
        return pltpu.make_async_remote_copy(
            src_ref=src, dst_ref=dst, send_sem=send, recv_sem=recv, device_id=to, device_id_type=MESH)

    barrier = pltpu.get_barrier_semaphore()
    for k in range(8):
        for e in range(2):
            pl.semaphore_signal(barrier, inc=1, device_id=home(k, e), device_id_type=MESH)
    for s in range(16):
        pl.semaphore_signal(barrier, inc=1, device_id=source(s), device_id_type=MESH)
    for d in range(1, 4):
        pl.semaphore_signal(barrier, inc=1, device_id=(tm, (h + d) % 4), device_id_type=MESH)

    det_in = pltpu.make_async_copy(det_hbm, det_ref, l_sem.at[0])
    x_in = pltpu.make_async_copy(x_hbm, x_ref, l_sem.at[1])
    tid_in = pltpu.make_async_copy(tid_hbm, tid_ref, l_sem.at[2])
    det_in.start()
    x_in.start()
    tid_in.start()

    x_in.wait()
    re = x_ref[:, 0, :]
    im = x_ref[:, 1, :]
    sq = re * re + im * im
    part = sq[:, 0:LANES]
    for k in range(1, 8):
        part = part + sq[:, k * LANES:(k + 1) * LANES]
    part = jnp.concatenate([part, jnp.zeros((LANES - SPAN, LANES), f32)], 0)
    pbuf[h] = jnp.sum(part.T, axis=0, keepdims=True)
    for k in range(8):
        send_buf[k, 0:SPAN, :] = re[:, k * LANES:(k + 1) * LANES].astype(bf16)
        send_buf[k, SPAN:, :] = im[:, k * LANES:(k + 1) * LANES].astype(bf16)

    det_in.wait()
    for k in range(12):
        row = jnp.broadcast_to(det_ref[k:k + 1, :].astype(f32), (LANES, LANES))
        det[k * LANES:(k + 1) * LANES, :] = row.T
    for e in range(NDET):
        mat[e, NSFT:, :] = jnp.zeros((ROWS - NSFT, LANES), f32)

    def mat_rows(b, carry):
        at = pl.ds(pl.multiple_of(b * 32, 32), 32)
        d = det[at, :]
        for e in range(NDET):
            mat[e, at, :] = jnp.where(d == 0.0, inter_ref[e, 0], jnp.where(d == 1.0, inter_ref[e, 1], inter_ref[e, 2]))
        return carry

    lax.fori_loop(0, NSFT // 32, mat_rows, 0)

    def weight_rows(b, carry):
        r0 = pl.multiple_of(b * 16, 16)
        d = det[pl.ds(r0, 16), :]
        for l in range(NLAG):
            at = pl.ds(r0 + lag_ref[l], 16)
            wl[l, pl.ds(r0, 16), :] = jnp.where(
                d == 0.0, mat[0, at, :], jnp.where(d == 1.0, mat[1, at, :], mat[2, at, :]))
        return carry

    lax.fori_loop(0, NSFT // 16, weight_rows, 0)
    for l in range(NLAG):
        wl[l, NSFT:, :] = jnp.zeros((ROWS - NSFT, LANES), f32)
    xre[NSFT:, :] = jnp.zeros((ROWS - NSFT, LANES), f32)
    xim[NSFT:, :] = jnp.zeros((ROWS - NSFT, LANES), f32)
    tid_in.wait()

    pl.semaphore_wait(barrier, 35)

    power_copies = [
        remote(pbuf.at[h], pbuf.at[h], p_send.at[d], p_recv.at[4 - d], (tm, (h + d) % 4)) for d in range(1, 4)]
    id_copies = [
        remote(tid_ref, idbuf.at[tm // 4], i_send.at[k], i_recv.at[tm // 4], home(k, x // 2)) for k in range(8)]
    chunk_copies = [
        remote(send_buf.at[k], xrecv.at[tm], c_send.at[2 * k + e], c_recv.at[tm], home(k, e))
        for k in range(8) for e in range(2)]
    for copy in power_copies + id_copies + chunk_copies:
        copy.start()

    for copy in power_copies:
        copy.wait()
    power = ((pbuf[0] + pbuf[1]) + (pbuf[2] + pbuf[3])) / NBIN
    gsend[...] = lax.rsqrt(power + 1e-06)
    scale_copies = [
        remote(gsend, gbuf.at[tm], g_send.at[2 * k + e], g_recv.at[tm], home(k, e))
        for k in range(8) for e in range(2)]
    for copy in scale_copies:
        copy.start()

    for s in range(8):
        remote(tid_ref, idbuf.at[s], i_send.at[s], i_recv.at[s], owner(s)).wait_recv()
    ids = idbuf[...].astype(f32)
    amp = (8.0 + 4.0 * ids[:, 0, :]) * (0.5 / math.pi)
    cq, sq_ = cos_sin(ids[:, 1, :] * (1.0 / NGRID))
    amp_cos[...] = amp * cq
    amp_sin[...] = amp * sq_

    def z_rows(b, carry):
        at = pl.ds(pl.multiple_of(b * 16, 16), 16)
        row = lax.broadcasted_iota(jnp.int32, (16, LANES), 0) + b * 16
        row = jnp.where(row >= PERIOD, row - PERIOD, row).astype(f32)
        cr, sr = cos_sin(row * (1.0 / PERIOD))
        for s in range(8):
            c, si = cos_sin(sr * amp_cos[s:s + 1, :] + cr * amp_sin[s:s + 1, :])
            zc[s, at, :] = c
            zs[s, at, :] = si
        return carry

    lax.fori_loop(0, ZROWS // 16, z_rows, 0)

    def factor_rows(n, carry):
        l, b = n // 9, n % 9
        r0 = pl.multiple_of(b * 32, 32)
        lag = lag_ref[l]
        out = pl.multiple_of(l * (2 * FOLD) + r0, 32)
        for s in range(8):
            ci, si = zc[s, pl.ds(r0, 32), :], zs[s, pl.ds(r0, 32), :]
            cj, sj = zc[s, pl.ds(r0 + lag, 32), :], zs[s, pl.ds(r0 + lag, 32), :]
            at = slice(s * LANES, (s + 1) * LANES)
            fac[pl.ds(out, 32), at] = (cj * ci + sj * si).astype(bf16)
            fac[pl.ds(out + FOLD, 32), at] = (sj * ci - cj * si).astype(bf16)
        return carry

    lax.fori_loop(0, NLAG * 9, factor_rows, 0)

    other = (tm, h + 1 - 2 * core)
    forwards = []
    for s in range(16):
        slot = source(s)[0]
        remote(send_buf.at[0], xrecv.at[slot], c_send.at[s], c_recv.at[slot], source(s)).wait_recv()
        remote(gsend, gbuf.at[slot], g_send.at[s], g_recv.at[slot], source(s)).wait_recv()
        forwards.append(remote(xrecv.at[slot], xrecv.at[slot], f_send.at[s], c_recv.at[slot], other))
        forwards.append(remote(gbuf.at[slot], gbuf.at[slot], fg_send.at[s], g_recv.at[slot], other))
        forwards[-1].start()
        forwards[-2].start()
    for s in range(16):
        slot = source(s)[0] + 1 - 2 * core
        remote(xrecv.at[slot], xrecv.at[slot], f_send.at[s], c_recv.at[slot], other).wait_recv()
        remote(gbuf.at[slot], gbuf.at[slot], fg_send.at[s], g_recv.at[slot], other).wait_recv()

    scales = gbuf[:, 0, :]
    scales = jnp.concatenate([scales, jnp.zeros((LANES - TM, LANES), f32)], 0).T[0:SPAN]
    for b in range(TM):
        g = jnp.broadcast_to(scales[:, b:b + 1], (SPAN, LANES))
        xre[b * SPAN:(b + 1) * SPAN, :] = xrecv[b, 0:SPAN, :].astype(f32) * g
        xim[b * SPAN:(b + 1) * SPAN, :] = xrecv[b, SPAN:, :].astype(f32) * g

    def pair_rows(turns, n, carry):
        b, part = n // 4, n % 4
        r0 = pl.multiple_of(b * 16, 16)
        real = lax.broadcasted_iota(jnp.int32, (16, LANES), 0) + r0 < PERIOD
        lags = [lag_ref[3 * part + q] for q in range(3)]
        sums = [[jnp.zeros((16, LANES), f32)] * 2 for _ in range(3)]
        for m in range(turns):
            here = pl.ds(r0 + PERIOD * m, 16)
            a, bb = xre[here, :], xim[here, :]
            for q in range(3):
                far = pl.ds(r0 + PERIOD * m + lags[q], 16)
                w = wl[3 * part + q, here, :]
                c, d = xre[far, :] * w, xim[far, :] * w
                sums[q] = [sums[q][0] + (a * c + bb * d), sums[q][1] + (a * d - bb * c)]
        for q in range(3):
            out = pl.multiple_of((3 * part + q) * (2 * FOLD) + r0, 16)
            pairs[pl.ds(out, 16), :] = jnp.where(real, sums[q][0], 0.0)
            pairs[pl.ds(out + FOLD, 16), :] = jnp.where(real, sums[q][1], 0.0)
        return carry

    last = (NSFT - PERIOD * (TURNS - 1) + 15) // 16
    lax.fori_loop(0, last * 4, functools.partial(pair_rows, TURNS), 0)
    lax.fori_loop(last * 4, 18 * 4, functools.partial(pair_rows, TURNS - 1), 0)

    def turn(b, carry):
        for q in range(6):
            at = pl.ds(pl.multiple_of((b * 6 + q) * LANES, LANES), LANES)
            pairs_t[:, at] = pairs[at, :].T.astype(bf16)
        return carry

    lax.fori_loop(0, DEPTH // LANES // 6, turn, 0)

    scale = 1.0 / math.sqrt(NSFT * NLAG)

    def multiply(b, carry):
        at = pl.ds(pl.multiple_of(b * WIDE, WIDE), WIDE)
        stat = jnp.dot(pairs_t[...], fac[:, at], preferred_element_type=f32) * scale
        for q in range(2):
            s = 2 * b + q
            osend[s] = stat[:, q * LANES:(q + 1) * LANES].T.astype(bf16)
            remote(osend.at[s], orecv.at[tm // 4], o_send.at[s], o_recv.at[tm // 4], owner(s)).start()
        return carry

    lax.fori_loop(0, PART // WIDE, multiply, 0)

    for k in range(8):
        remote(osend.at[k], orecv.at[k], o_send.at[k], o_recv.at[k], home(k, x // 2)).wait_recv()
        o_ref[:, k * LANES:(k + 1) * LANES] = orecv[k]

    for copy in id_copies + chunk_copies + scale_copies + forwards:
        copy.wait_send()
    for s in range(8):
        remote(osend.at[s], orecv.at[tm // 4], o_send.at[s], o_recv.at[tm // 4], owner(s)).wait_send()


def shards(sfts, detector_ids, intersection, lags, template_ids):
    bf16, f32 = jnp.bfloat16, jnp.float32
    vmem = pl.BlockSpec(memory_space=pltpu.VMEM)
    smem = pl.BlockSpec(memory_space=pltpu.SMEM)
    hbm = pl.BlockSpec(memory_space=pl.ANY)
    dma = pltpu.SemaphoreType.DMA
    out = pl.pallas_call(
        kernel,
        out_shape=jax.ShapeDtypeStruct((LANES, 8 * LANES), bf16),
        in_specs=[hbm, hbm, hbm, smem, smem],
        out_specs=vmem,
        scratch_shapes=[
            pltpu.VMEM((SPAN, 2, 8 * LANES), f32),
            pltpu.VMEM((12, LANES), jnp.int32),
            pltpu.VMEM((2, LANES), jnp.int32),
            pltpu.VMEM((4, 1, LANES), f32),
            pltpu.VMEM((1, LANES), f32),
            pltpu.VMEM((TM, 1, LANES), f32),
            pltpu.VMEM((8, 2, LANES), jnp.int32),
            pltpu.VMEM((8, 2 * SPAN, LANES), bf16),
            pltpu.VMEM((TM, 2 * SPAN, LANES), bf16),
            pltpu.VMEM((8, LANES, LANES), bf16),
            pltpu.VMEM((8, LANES, LANES), bf16),
            pltpu.VMEM((ROWS, LANES), f32),
            pltpu.VMEM((ROWS, LANES), f32),
            pltpu.VMEM((NSFT, LANES), f32),
            pltpu.VMEM((NDET, ROWS, LANES), f32),
            pltpu.VMEM((NLAG, ROWS, LANES), f32),
            pltpu.VMEM((8, LANES), f32),
            pltpu.VMEM((8, LANES), f32),
            pltpu.VMEM((8, ZROWS, LANES), f32),
            pltpu.VMEM((8, ZROWS, LANES), f32),
            pltpu.VMEM((DEPTH, PART), bf16),
            pltpu.VMEM((DEPTH, LANES), f32),
            pltpu.VMEM((LANES, DEPTH), bf16),
            dma((3,)), dma((4,)), dma((4,)), dma((8,)), dma((8,)), dma((16,)), dma((TM,)), dma((16,)), dma((TM,)),
            dma((16,)), dma((16,)), dma((8,)), dma((8,)),
        ],
        compiler_params=pltpu.CompilerParams(
            collective_id=0, has_side_effects=True, vmem_limit_bytes=60 * 1024 * 1024),
    )(sfts, detector_ids.reshape(12, LANES), template_ids.T, intersection, lags)
    return out.astype(f32)


def solution(mesh):
    in_specs = (P("tm", None, "freq"), P(), P(), P(), P("tm", None))
    out_specs = P("tm", "freq")
    return jax.shard_map(shards, mesh=mesh, in_specs=in_specs, out_specs=out_specs, check_vma=False)
```

```python
import math

import jax
import jax.numpy as jnp
from jax import lax
from jax.experimental import pallas as pl
from jax.experimental.pallas import tpu as pltpu
from jax.sharding import PartitionSpec as P

NSFT = 1536
NBIN = 4096
LAGMAX = 16
NLAG = 12
NDET = 3
NGRID = 64
PERIOD = 283
TM = 32
SPAN = 48
FOLD = 288
TURNS = 6
LANES = 128
ROWS = 1792
ZROWS = 304
DEPTH = 2 * NLAG * FOLD
PART = 1024
WIDE = 256
MESH = pl.DeviceIdType.MESH

COS = (0.9999999890590238, -19.739204499453965, 64.93911745989729, -85.45013953090921,
       60.167630951124465, -25.967599248993793, 6.528658161871135)
SIN = (6.28318527244795, -41.34169703820007, 81.60502363804078, -76.7015376703427,
       42.016075762415646, -14.86832275264805, 3.199338844584104)


def cos_sin(turns):
    u = turns - jnp.floor(turns + 0.5)
    t = u * u
    c = jnp.full_like(t, COS[-1])
    for k in COS[-2::-1]:
        c = c * t + k
    s = jnp.full_like(t, SIN[-1])
    for k in SIN[-2::-1]:
        s = s * t + k
    return c, s * u


def kernel(x_hbm, det_hbm, tid_hbm, inter_ref, lag_ref, o_ref,
           x_ref, det_ref, tid_ref, pbuf, gsend, gbuf, idbuf, send_buf, xrecv, osend, orecv,
           xre, xim, det, mat, wl, amp_cos, amp_sin, zc, zs, fac, folded, turned, acc,
           l_sem, p_send, p_recv, i_send, i_recv, g_send, g_recv, c_send, c_recv, fg_send, f_send, o_send, o_recv):
    tm = lax.axis_index("tm")
    h = lax.axis_index("freq")
    core, z_lo = h % 2, h // 2
    x = tm % 4
    f32, bf16 = jnp.float32, jnp.bfloat16

    quarter = (1 - z_lo) * 2 + x % 2
    group = 2 * (x // 2) + core

    def home(k, e):
        return 4 * k + core + 2 * e, (1 - z_lo) * 2 + x % 2

    def source(s):
        return 4 * (s // 2) + 2 * (s % 2) + core, quarter

    def owner(s):
        return 4 * s + group, quarter

    def remote(src, dst, send, recv, to):
        return pltpu.make_async_remote_copy(
            src_ref=src, dst_ref=dst, send_sem=send, recv_sem=recv, device_id=to, device_id_type=MESH)

    barrier = pltpu.get_barrier_semaphore()
    for k in range(8):
        for e in range(2):
            pl.semaphore_signal(barrier, inc=1, device_id=home(k, e), device_id_type=MESH)
    for s in range(16):
        pl.semaphore_signal(barrier, inc=1, device_id=source(s), device_id_type=MESH)
    for d in range(1, 4):
        pl.semaphore_signal(barrier, inc=1, device_id=(tm, (h + d) % 4), device_id_type=MESH)

    det_in = pltpu.make_async_copy(det_hbm, det_ref, l_sem.at[0])
    x_in = pltpu.make_async_copy(x_hbm, x_ref, l_sem.at[1])
    tid_in = pltpu.make_async_copy(tid_hbm, tid_ref, l_sem.at[2])
    det_in.start()
    x_in.start()
    tid_in.start()

    x_in.wait()
    re = x_ref[:, 0, :]
    im = x_ref[:, 1, :]
    sq = re * re + im * im
    part = sq[:, 0:LANES]
    for k in range(1, 8):
        part = part + sq[:, k * LANES:(k + 1) * LANES]
    part = jnp.concatenate([part, jnp.zeros((LANES - SPAN, LANES), f32)], 0)
    pbuf[h] = jnp.sum(part.T, axis=0, keepdims=True)
    for k in range(8):
        send_buf[k, 0:SPAN, :] = re[:, k * LANES:(k + 1) * LANES].astype(bf16)
        send_buf[k, SPAN:, :] = im[:, k * LANES:(k + 1) * LANES].astype(bf16)

    det_in.wait()
    for k in range(12):
        row = jnp.broadcast_to(det_ref[k:k + 1, :].astype(f32), (LANES, LANES))
        det[k * LANES:(k + 1) * LANES, :] = row.T
    for e in range(NDET):
        mat[e, NSFT:, :] = jnp.zeros((ROWS - NSFT, LANES), f32)

    def mat_rows(b, carry):
        at = pl.ds(pl.multiple_of(b * 32, 32), 32)
        d = det[at, :]
        for e in range(NDET):
            mat[e, at, :] = jnp.where(d == 0.0, inter_ref[e, 0], jnp.where(d == 1.0, inter_ref[e, 1], inter_ref[e, 2]))
        return carry

    lax.fori_loop(0, NSFT // 32, mat_rows, 0)

    def weight_rows(b, carry):
        r0 = pl.multiple_of(b * 16, 16)
        d = det[pl.ds(r0, 16), :]
        for l in range(NLAG):
            at = pl.ds(r0 + lag_ref[l], 16)
            wl[l, pl.ds(r0, 16), :] = jnp.where(
                d == 0.0, mat[0, at, :], jnp.where(d == 1.0, mat[1, at, :], mat[2, at, :]))
        return carry

    lax.fori_loop(0, NSFT // 16, weight_rows, 0)
    for l in range(NLAG):
        wl[l, NSFT:, :] = jnp.zeros((ROWS - NSFT, LANES), f32)
    xre[NSFT:, :] = jnp.zeros((ROWS - NSFT, LANES), f32)
    xim[NSFT:, :] = jnp.zeros((ROWS - NSFT, LANES), f32)
    tid_in.wait()

    pl.semaphore_wait(barrier, 35)

    power_copies = [
        remote(pbuf.at[h], pbuf.at[h], p_send.at[d], p_recv.at[4 - d], (tm, (h + d) % 4)) for d in range(1, 4)]
    id_copies = [
        remote(tid_ref, idbuf.at[tm // 4], i_send.at[k], i_recv.at[tm // 4], home(k, x // 2)) for k in range(8)]
    chunk_copies = [
        remote(send_buf.at[k], xrecv.at[tm], c_send.at[2 * k + e], c_recv.at[tm], home(k, e))
        for k in range(8) for e in range(2)]
    for copy in power_copies + id_copies + chunk_copies:
        copy.start()

    for copy in power_copies:
        copy.wait()
    power = ((pbuf[0] + pbuf[1]) + (pbuf[2] + pbuf[3])) / NBIN
    gsend[...] = lax.rsqrt(power + 1e-06)
    scale_copies = [
        remote(gsend, gbuf.at[tm], g_send.at[2 * k + e], g_recv.at[tm], home(k, e))
        for k in range(8) for e in range(2)]
    for copy in scale_copies:
        copy.start()

    for s in range(8):
        remote(tid_ref, idbuf.at[s], i_send.at[s], i_recv.at[s], owner(s)).wait_recv()
    ids = idbuf[...].astype(f32)
    amp = (8.0 + 4.0 * ids[:, 0, :]) * (0.5 / math.pi)
    cq, sq_ = cos_sin(ids[:, 1, :] * (1.0 / NGRID))
    amp_cos[...] = amp * cq
    amp_sin[...] = amp * sq_

    def z_rows(b, carry):
        at = pl.ds(pl.multiple_of(b * 16, 16), 16)
        row = lax.broadcasted_iota(jnp.int32, (16, LANES), 0) + b * 16
        row = jnp.where(row >= PERIOD, row - PERIOD, row).astype(f32)
        cr, sr = cos_sin(row * (1.0 / PERIOD))
        for s in range(8):
            c, si = cos_sin(sr * amp_cos[s:s + 1, :] + cr * amp_sin[s:s + 1, :])
            zc[s, at, :] = c
            zs[s, at, :] = si
        return carry

    lax.fori_loop(0, ZROWS // 16, z_rows, 0)

    def factor_rows(n, carry):
        l, b = n // 9 * 2, n % 9
        r0 = pl.multiple_of(b * 32, 32)
        lags = lag_ref[l], lag_ref[l + 1]
        for s in range(8):
            ci, si = zc[s, pl.ds(r0, 32), :], zs[s, pl.ds(r0, 32), :]
            for q in range(2):
                far = pl.ds(r0 + lags[q], 32)
                cj, sj = zc[s, far, :], zs[s, far, :]
                out = pl.multiple_of((l + q) * (2 * FOLD) + r0, 32)
                fac[s, pl.ds(out, 32), :] = (cj * ci + sj * si).astype(bf16)
                fac[s, pl.ds(out + FOLD, 32), :] = (sj * ci - cj * si).astype(bf16)
        return carry

    lax.fori_loop(0, NLAG // 2 * 9, factor_rows, 0)

    other = (tm, h + 1 - 2 * core)
    forwards = []
    for s in range(16):
        slot = source(s)[0]
        remote(send_buf.at[0], xrecv.at[slot], c_send.at[s], c_recv.at[slot], source(s)).wait_recv()
        remote(gsend, gbuf.at[slot], g_send.at[s], g_recv.at[slot], source(s)).wait_recv()
        forwards.append(remote(xrecv.at[slot], xrecv.at[slot], f_send.at[s], c_recv.at[slot], other))
        forwards.append(remote(gbuf.at[slot], gbuf.at[slot], fg_send.at[s], g_recv.at[slot], other))
        forwards[-1].start()
        forwards[-2].start()
    for s in range(16):
        slot = source(s)[0] + 1 - 2 * core
        remote(xrecv.at[slot], xrecv.at[slot], f_send.at[s], c_recv.at[slot], other).wait_recv()
        remote(gbuf.at[slot], gbuf.at[slot], fg_send.at[s], g_recv.at[slot], other).wait_recv()

    scales = gbuf[:, 0, :]
    scales = jnp.concatenate([scales, jnp.zeros((LANES - TM, LANES), f32)], 0).T[0:SPAN]
    for b in range(TM):
        g = jnp.broadcast_to(scales[:, b:b + 1], (SPAN, LANES))
        xre[b * SPAN:(b + 1) * SPAN, :] = xrecv[b, 0:SPAN, :].astype(f32) * g
        xim[b * SPAN:(b + 1) * SPAN, :] = xrecv[b, SPAN:, :].astype(f32) * g

    acc[...] = jnp.zeros_like(acc)
    turned[...] = jnp.zeros_like(turned)

    def pairs_of(l):
        lags = lag_ref[l], lag_ref[l + 1]
        for b in range(FOLD // 16):
            r0 = 16 * b
            turns = TURNS if r0 + PERIOD * (TURNS - 1) < NSFT else TURNS - 1
            sums = [[jnp.zeros((16, LANES), f32)] * 2 for _ in range(2)]
            for m in range(turns):
                here = pl.ds(r0 + PERIOD * m, 16)
                a, bb = xre[here, :], xim[here, :]
                for q in range(2):
                    far = pl.ds(r0 + PERIOD * m + lags[q], 16)
                    w = wl[l + q, here, :]
                    c, d = xre[far, :], xim[far, :]
                    sums[q] = [sums[q][0] + (a * c + bb * d) * w, sums[q][1] + (a * d - bb * c) * w]
            for q in range(2):
                for p in range(2):
                    total = sums[q][p]
                    if r0 + 16 > PERIOD:
                        real = lax.broadcasted_iota(jnp.int32, (16, LANES), 0) + r0 < PERIOD
                        total = jnp.where(real, total, 0.0)
                    at = (2 * q + p) * FOLD + r0
                    folded[at:at + 16, :] = total

    def turn():
        for at in range(0, 4 * FOLD, LANES):
            turned[:, at:at + LANES] = folded[at:at + LANES, :].T.astype(bf16)

    def product(l, n):
        rows = pl.ds(pl.multiple_of(l * (2 * FOLD), 2 * FOLD), 4 * FOLD)
        rhs = jnp.concatenate([fac[2 * n, rows, :], fac[2 * n + 1, rows, :]], 1)
        return acc[:, n * WIDE:(n + 1) * WIDE] + jnp.dot(turned[...], rhs, preferred_element_type=f32)

    def two_lags(i, carry):
        for n in range(PART // WIDE):
            acc[:, n * WIDE:(n + 1) * WIDE] = product(jnp.maximum(2 * i - 2, 0), n)
        pairs_of(2 * i)
        turn()
        return carry

    lax.fori_loop(0, NLAG // 2, two_lags, 0)

    scale = 1.0 / math.sqrt(NSFT * NLAG)
    for n in range(PART // WIDE):
        stat = product(NLAG - 2, n) * scale
        for q in range(2):
            s = 2 * n + q
            osend[s] = stat[:, q * LANES:(q + 1) * LANES].T.astype(bf16)
            remote(osend.at[s], orecv.at[tm // 4], o_send.at[s], o_recv.at[tm // 4], owner(s)).start()

    for k in range(8):
        remote(osend.at[k], orecv.at[k], o_send.at[k], o_recv.at[k], home(k, x // 2)).wait_recv()
        o_ref[:, k * LANES:(k + 1) * LANES] = orecv[k]

    for copy in id_copies + chunk_copies + scale_copies + forwards:
        copy.wait_send()
    for s in range(8):
        remote(osend.at[s], orecv.at[tm // 4], o_send.at[s], o_recv.at[tm // 4], owner(s)).wait_send()


def shards(sfts, detector_ids, intersection, lags, template_ids):
    bf16, f32 = jnp.bfloat16, jnp.float32
    vmem = pl.BlockSpec(memory_space=pltpu.VMEM)
    smem = pl.BlockSpec(memory_space=pltpu.SMEM)
    hbm = pl.BlockSpec(memory_space=pl.ANY)
    dma = pltpu.SemaphoreType.DMA
    out = pl.pallas_call(
        kernel,
        out_shape=jax.ShapeDtypeStruct((LANES, 8 * LANES), bf16),
        in_specs=[hbm, hbm, hbm, smem, smem],
        out_specs=vmem,
        scratch_shapes=[
            pltpu.VMEM((SPAN, 2, 8 * LANES), f32),
            pltpu.VMEM((12, LANES), jnp.int32),
            pltpu.VMEM((2, LANES), jnp.int32),
            pltpu.VMEM((4, 1, LANES), f32),
            pltpu.VMEM((1, LANES), f32),
            pltpu.VMEM((TM, 1, LANES), f32),
            pltpu.VMEM((8, 2, LANES), jnp.int32),
            pltpu.VMEM((8, 2 * SPAN, LANES), bf16),
            pltpu.VMEM((TM, 2 * SPAN, LANES), bf16),
            pltpu.VMEM((8, LANES, LANES), bf16),
            pltpu.VMEM((8, LANES, LANES), bf16),
            pltpu.VMEM((ROWS, LANES), f32),
            pltpu.VMEM((ROWS, LANES), f32),
            pltpu.VMEM((NSFT, LANES), f32),
            pltpu.VMEM((NDET, ROWS, LANES), f32),
            pltpu.VMEM((NLAG, ROWS, LANES), f32),
            pltpu.VMEM((8, LANES), f32),
            pltpu.VMEM((8, LANES), f32),
            pltpu.VMEM((8, ZROWS, LANES), f32),
            pltpu.VMEM((8, ZROWS, LANES), f32),
            pltpu.VMEM((8, DEPTH, LANES), bf16),
            pltpu.VMEM((4 * FOLD, LANES), f32),
            pltpu.VMEM((LANES, 4 * FOLD), bf16),
            pltpu.VMEM((LANES, PART), f32),
            dma((3,)), dma((4,)), dma((4,)), dma((8,)), dma((8,)), dma((16,)), dma((TM,)), dma((16,)), dma((TM,)),
            dma((16,)), dma((16,)), dma((8,)), dma((8,)),
        ],
        compiler_params=pltpu.CompilerParams(
            collective_id=0, has_side_effects=True, vmem_limit_bytes=60 * 1024 * 1024),
    )(sfts, detector_ids.reshape(12, LANES), template_ids.T, intersection, lags)
    return out.astype(f32)


def solution(mesh):
    in_specs = (P("tm", None, "freq"), P(), P(), P(), P("tm", None))
    out_specs = P("tm", "freq")
    return jax.shard_map(shards, mesh=mesh, in_specs=in_specs, out_specs=out_specs, check_vma=False)
```

```python
import functools
import math

import jax
import jax.numpy as jnp
from jax import lax
from jax.experimental import pallas as pl
from jax.experimental.pallas import tpu as pltpu
from jax.sharding import PartitionSpec as P

NSFT = 1536
NBIN = 4096
LAGMAX = 16
NLAG = 12
NDET = 3
NGRID = 64
PERIOD = 283
TM = 32
SPAN = 48
FOLD = 288
TURNS = 6
LANES = 128
ROWS = 1600
ZROWS = 304
DEPTH = 2 * NLAG * FOLD
PART = 1024
WIDE = 256
MESH = pl.DeviceIdType.MESH

COS = (0.9999999890590238, -19.739204499453965, 64.93911745989729, -85.45013953090921,
       60.167630951124465, -25.967599248993793, 6.528658161871135)
SIN = (6.28318527244795, -41.34169703820007, 81.60502363804078, -76.7015376703427,
       42.016075762415646, -14.86832275264805, 3.199338844584104)


def cos_sin(turns):
    u = turns - jnp.floor(turns + 0.5)
    t = u * u
    c = jnp.full_like(t, COS[-1])
    for k in COS[-2::-1]:
        c = c * t + k
    s = jnp.full_like(t, SIN[-1])
    for k in SIN[-2::-1]:
        s = s * t + k
    return c, s * u


def kernel(x_hbm, det_hbm, tid_hbm, inter_hbm, lag_hbm, o_ref,
           x_ref, det_ref, tid_ref, inter_ref, lag_ref, pbuf, gsend, gbuf, idbuf, send_buf, xrecv, osend, orecv,
           xre, xim, det, mat, wl, amp_cos, amp_sin, zc, zs, fac, pairs, pairs_t,
           l_sem, p_send, p_recv, i_send, i_recv, g_send, g_recv, c_send, c_recv, fg_send, f_send, o_send, o_recv):
    tm = lax.axis_index("tm")
    h = lax.axis_index("freq")
    core, z_lo = h % 2, h // 2
    x = tm % 4
    f32, bf16 = jnp.float32, jnp.bfloat16

    quarter = (1 - z_lo) * 2 + x % 2
    group = 2 * (x // 2) + core

    def home(k, e):
        return 4 * k + core + 2 * e, (1 - z_lo) * 2 + x % 2

    def source(s):
        return 4 * (s // 2) + 2 * (s % 2) + core, quarter

    def owner(s):
        return 4 * s + group, quarter

    def remote(src, dst, send, recv, to):
        return pltpu.make_async_remote_copy(
            src_ref=src, dst_ref=dst, send_sem=send, recv_sem=recv, device_id=to, device_id_type=MESH)

    barrier = pltpu.get_barrier_semaphore()
    for k in range(8):
        for e in range(2):
            pl.semaphore_signal(barrier, inc=1, device_id=home(k, e), device_id_type=MESH)
    for s in range(16):
        pl.semaphore_signal(barrier, inc=1, device_id=source(s), device_id_type=MESH)
    for d in range(1, 4):
        pl.semaphore_signal(barrier, inc=1, device_id=(tm, (h + d) % 4), device_id_type=MESH)

    det_in = pltpu.make_async_copy(det_hbm, det_ref, l_sem.at[0])
    x_in = pltpu.make_async_copy(x_hbm, x_ref, l_sem.at[1])
    tid_in = pltpu.make_async_copy(tid_hbm, tid_ref, l_sem.at[2])
    inter_in = pltpu.make_async_copy(inter_hbm, inter_ref, l_sem.at[3])
    lag_in = pltpu.make_async_copy(lag_hbm, lag_ref, l_sem.at[4])
    x_in.start()
    det_in.start()
    inter_in.start()
    lag_in.start()
    tid_in.start()

    x_in.wait()
    re = x_ref[:, 0, :]
    im = x_ref[:, 1, :]
    sq = re * re + im * im
    part = sq[:, 0:LANES]
    for k in range(1, 8):
        part = part + sq[:, k * LANES:(k + 1) * LANES]
    part = jnp.concatenate([part, jnp.zeros((LANES - SPAN, LANES), f32)], 0)
    pbuf[h] = jnp.sum(part.T, axis=0, keepdims=True)
    for k in range(8):
        send_buf[k, 0:SPAN, :] = re[:, k * LANES:(k + 1) * LANES].astype(bf16)
        send_buf[k, SPAN:, :] = im[:, k * LANES:(k + 1) * LANES].astype(bf16)

    det_in.wait()
    inter_in.wait()
    lag_in.wait()
    for k in range(12):
        row = jnp.broadcast_to(det_ref[k:k + 1, :].astype(f32), (LANES, LANES))
        det[k * LANES:(k + 1) * LANES, :] = row.T
    for e in range(NDET):
        mat[e, NSFT:, :] = jnp.zeros((ROWS - NSFT, LANES), f32)

    def mat_rows(b, carry):
        at = pl.ds(pl.multiple_of(b * 32, 32), 32)
        d = det[at, :]
        for e in range(NDET):
            mat[e, at, :] = jnp.where(d == 0.0, inter_ref[e, 0], jnp.where(d == 1.0, inter_ref[e, 1], inter_ref[e, 2]))
        return carry

    lax.fori_loop(0, NSFT // 32, mat_rows, 0)

    def weight_rows(b, carry):
        r0 = pl.multiple_of(b * 16, 16)
        d = det[pl.ds(r0, 16), :]
        for l in range(NLAG):
            at = pl.ds(r0 + lag_ref[l], 16)
            wl[l, pl.ds(r0, 16), :] = jnp.where(
                d == 0.0, mat[0, at, :], jnp.where(d == 1.0, mat[1, at, :], mat[2, at, :]))
        return carry

    lax.fori_loop(0, NSFT // 16, weight_rows, 0)
    for l in range(NLAG):
        wl[l, NSFT:, :] = jnp.zeros((ROWS - NSFT, LANES), f32)
    xre[NSFT:, :] = jnp.zeros((ROWS - NSFT, LANES), f32)
    xim[NSFT:, :] = jnp.zeros((ROWS - NSFT, LANES), f32)
    tid_in.wait()

    pl.semaphore_wait(barrier, 35)

    power_copies = [
        remote(pbuf.at[h], pbuf.at[h], p_send.at[d], p_recv.at[4 - d], (tm, (h + d) % 4)) for d in range(1, 4)]
    id_copies = [
        remote(tid_ref, idbuf.at[tm // 4], i_send.at[k], i_recv.at[tm // 4], home(k, x // 2)) for k in range(8)]
    chunk_copies = [
        remote(send_buf.at[k], xrecv.at[tm], c_send.at[2 * k + e], c_recv.at[tm], home(k, e))
        for k in range(8) for e in range(2)]
    for copy in power_copies + id_copies + chunk_copies:
        copy.start()

    for copy in power_copies:
        copy.wait()
    power = ((pbuf[0] + pbuf[1]) + (pbuf[2] + pbuf[3])) / NBIN
    gsend[...] = lax.rsqrt(power + 1e-06)
    scale_copies = [
        remote(gsend, gbuf.at[tm], g_send.at[2 * k + e], g_recv.at[tm], home(k, e))
        for k in range(8) for e in range(2)]
    for copy in scale_copies:
        copy.start()

    for s in range(8):
        remote(tid_ref, idbuf.at[s], i_send.at[s], i_recv.at[s], owner(s)).wait_recv()
    ids = idbuf[...].astype(f32)
    amp = (8.0 + 4.0 * ids[:, 0, :]) * (0.5 / math.pi)
    cq, sq_ = cos_sin(ids[:, 1, :] * (1.0 / NGRID))
    amp_cos[...] = amp * cq
    amp_sin[...] = amp * sq_

    def z_rows(b, carry):
        at = pl.ds(pl.multiple_of(b * 16, 16), 16)
        row = lax.broadcasted_iota(jnp.int32, (16, LANES), 0) + b * 16
        row = jnp.where(row >= PERIOD, row - PERIOD, row).astype(f32)
        cr, sr = cos_sin(row * (1.0 / PERIOD))
        for s in range(8):
            c, si = cos_sin(sr * amp_cos[s:s + 1, :] + cr * amp_sin[s:s + 1, :])
            zc[s, at, :] = c
            zs[s, at, :] = si
        return carry

    lax.fori_loop(0, ZROWS // 16, z_rows, 0)

    def factor_rows(n, carry):
        l, b = n // 9 * 2, n % 9
        r0 = pl.multiple_of(b * 32, 32)
        lags = lag_ref[l], lag_ref[l + 1]
        for s in range(8):
            ci, si = zc[s, pl.ds(r0, 32), :], zs[s, pl.ds(r0, 32), :]
            for q in range(2):
                far = pl.ds(r0 + lags[q], 32)
                cj, sj = zc[s, far, :], zs[s, far, :]
                out = pl.multiple_of((l + q) * (2 * FOLD) + r0, 32)
                fac[s, pl.ds(out, 32), :] = (cj * ci + sj * si).astype(bf16)
                fac[s, pl.ds(out + FOLD, 32), :] = (sj * ci - cj * si).astype(bf16)
        return carry

    lax.fori_loop(0, NLAG // 2 * 9, factor_rows, 0)

    other = (tm, h + 1 - 2 * core)
    forwards = []
    for s in range(16):
        slot = source(s)[0]
        remote(send_buf.at[0], xrecv.at[slot], c_send.at[s], c_recv.at[slot], source(s)).wait_recv()
        remote(gsend, gbuf.at[slot], g_send.at[s], g_recv.at[slot], source(s)).wait_recv()
        forwards.append(remote(xrecv.at[slot], xrecv.at[slot], f_send.at[s], c_recv.at[slot], other))
        forwards.append(remote(gbuf.at[slot], gbuf.at[slot], fg_send.at[s], g_recv.at[slot], other))
        forwards[-1].start()
        forwards[-2].start()
    for s in range(16):
        slot = source(s)[0] + 1 - 2 * core
        remote(xrecv.at[slot], xrecv.at[slot], f_send.at[s], c_recv.at[slot], other).wait_recv()
        remote(gbuf.at[slot], gbuf.at[slot], fg_send.at[s], g_recv.at[slot], other).wait_recv()

    scales = gbuf[:, 0, :]
    scales = jnp.concatenate([scales, jnp.zeros((LANES - TM, LANES), f32)], 0).T[0:SPAN]
    for b in range(TM):
        g = jnp.broadcast_to(scales[:, b:b + 1], (SPAN, LANES))
        xre[b * SPAN:(b + 1) * SPAN, :] = xrecv[b, 0:SPAN, :].astype(f32) * g
        xim[b * SPAN:(b + 1) * SPAN, :] = xrecv[b, SPAN:, :].astype(f32) * g

    def pair_rows(turns, n, carry):
        b, part = n // 4, n % 4
        r0 = pl.multiple_of(b * 16, 16)
        real = lax.broadcasted_iota(jnp.int32, (16, LANES), 0) + r0 < PERIOD
        lags = [lag_ref[3 * part + q] for q in range(3)]
        sums = [[jnp.zeros((16, LANES), f32)] * 2 for _ in range(3)]
        for m in range(turns):
            here = pl.ds(r0 + PERIOD * m, 16)
            a, bb = xre[here, :], xim[here, :]
            for q in range(3):
                far = pl.ds(r0 + PERIOD * m + lags[q], 16)
                w = wl[3 * part + q, here, :]
                c, d = xre[far, :] * w, xim[far, :] * w
                sums[q] = [sums[q][0] + (a * c + bb * d), sums[q][1] + (a * d - bb * c)]
        for q in range(3):
            out = pl.multiple_of((3 * part + q) * (2 * FOLD) + r0, 16)
            pairs[pl.ds(out, 16), :] = jnp.where(real, sums[q][0], 0.0)
            pairs[pl.ds(out + FOLD, 16), :] = jnp.where(real, sums[q][1], 0.0)
        return carry

    last = (NSFT - PERIOD * (TURNS - 1) + 15) // 16
    lax.fori_loop(0, last * 4, functools.partial(pair_rows, TURNS), 0)
    lax.fori_loop(last * 4, 18 * 4, functools.partial(pair_rows, TURNS - 1), 0)

    def turn(b, carry):
        for q in range(6):
            at = pl.ds(pl.multiple_of((b * 6 + q) * LANES, LANES), LANES)
            pairs_t[b * 6 + q] = pairs[at, :].T.astype(bf16)
        return carry

    lax.fori_loop(0, DEPTH // LANES // 6, turn, 0)

    scale = 1.0 / math.sqrt(NSFT * NLAG)

    def multiply(b, carry):
        lhs = jnp.concatenate([pairs_t[k] for k in range(DEPTH // LANES)], 1)
        rhs = jnp.concatenate([fac[2 * b], fac[2 * b + 1]], 1)
        stat = jnp.dot(lhs, rhs, preferred_element_type=f32) * scale
        for q in range(2):
            s = 2 * b + q
            osend[s] = stat[:, q * LANES:(q + 1) * LANES].T.astype(bf16)
            remote(osend.at[s], orecv.at[tm // 4], o_send.at[s], o_recv.at[tm // 4], owner(s)).start()
        return carry

    lax.fori_loop(0, PART // WIDE, multiply, 0)

    for copy in id_copies + chunk_copies + scale_copies + forwards:
        copy.wait_send()

    for k in range(8):
        remote(osend.at[k], orecv.at[k], o_send.at[k], o_recv.at[k], home(k, x // 2)).wait_recv()
        o_ref[:, k * LANES:(k + 1) * LANES] = orecv[k]

    for s in range(8):
        remote(osend.at[s], orecv.at[tm // 4], o_send.at[s], o_recv.at[tm // 4], owner(s)).wait_send()


def shards(sfts, detector_ids, intersection, lags, template_ids):
    bf16, f32 = jnp.bfloat16, jnp.float32
    vmem = pl.BlockSpec(memory_space=pltpu.VMEM)
    hbm = pl.BlockSpec(memory_space=pltpu.HBM)
    dma = pltpu.SemaphoreType.DMA
    out = pl.pallas_call(
        kernel,
        out_shape=jax.ShapeDtypeStruct((LANES, 8 * LANES), bf16),
        in_specs=[hbm] * 5,
        out_specs=vmem,
        scratch_shapes=[
            pltpu.VMEM((SPAN, 2, 8 * LANES), f32),
            pltpu.VMEM((12, LANES), jnp.int32),
            pltpu.VMEM((2, LANES), jnp.int32),
            pltpu.SMEM((NDET, NDET), f32),
            pltpu.SMEM((NLAG,), jnp.int32),
            pltpu.VMEM((4, 1, LANES), f32),
            pltpu.VMEM((1, LANES), f32),
            pltpu.VMEM((TM, 1, LANES), f32),
            pltpu.VMEM((8, 2, LANES), jnp.int32),
            pltpu.VMEM((8, 2 * SPAN, LANES), bf16),
            pltpu.VMEM((TM, 2 * SPAN, LANES), bf16),
            pltpu.VMEM((8, LANES, LANES), bf16),
            pltpu.VMEM((8, LANES, LANES), bf16),
            pltpu.VMEM((ROWS, LANES), f32),
            pltpu.VMEM((ROWS, LANES), f32),
            pltpu.VMEM((NSFT, LANES), f32),
            pltpu.VMEM((NDET, ROWS, LANES), f32),
            pltpu.VMEM((NLAG, ROWS, LANES), f32),
            pltpu.VMEM((8, LANES), f32),
            pltpu.VMEM((8, LANES), f32),
            pltpu.VMEM((8, ZROWS, LANES), f32),
            pltpu.VMEM((8, ZROWS, LANES), f32),
            pltpu.VMEM((8, DEPTH, LANES), bf16),
            pltpu.VMEM((DEPTH, LANES), f32),
            pltpu.VMEM((DEPTH // LANES, LANES, LANES), bf16),
            dma((5,)), dma((4,)), dma((4,)), dma((8,)), dma((8,)), dma((16,)), dma((TM,)), dma((16,)), dma((TM,)),
            dma((16,)), dma((16,)), dma((8,)), dma((8,)),
        ],
        compiler_params=pltpu.CompilerParams(
            collective_id=0, has_side_effects=True, vmem_limit_bytes=48 * 1024 * 1024),
    )(sfts, detector_ids.reshape(12, LANES), template_ids.T, intersection, lags)
    return out.astype(f32)


def solution(mesh):
    in_specs = (P("tm", None, "freq"), P(), P(), P(), P("tm", None))
    out_specs = P("tm", "freq")
    return jax.shard_map(shards, mesh=mesh, in_specs=in_specs, out_specs=out_specs, check_vma=False)
```

```python
import functools
import math

import jax
import jax.numpy as jnp
from jax import lax
from jax.experimental import pallas as pl
from jax.experimental.pallas import tpu as pltpu
from jax.sharding import PartitionSpec as P

NSFT = 1536
NBIN = 4096
LAGMAX = 16
NLAG = 12
NDET = 3
NGRID = 64
PERIOD = 283
TM = 32
SPAN = 48
FOLD = 288
TURNS = 6
LANES = 128
HALF = 64
PEERS = 16
ROWS = 1600
ZROWS = 304
DEPTH = NLAG * FOLD
POINTS = 1024
WIDE = 256
MESH = pl.DeviceIdType.MESH

COS = (0.9999999890590238, -19.739204499453965, 64.93911745989729, -85.45013953090921,
       60.167630951124465, -25.967599248993793, 6.528658161871135)
SIN = (6.28318527244795, -41.34169703820007, 81.60502363804078, -76.7015376703427,
       42.016075762415646, -14.86832275264805, 3.199338844584104)


def cos_sin(turns):
    u = turns - jnp.floor(turns + 0.5)
    t = u * u
    c = jnp.full_like(t, COS[-1])
    for k in COS[-2::-1]:
        c = c * t + k
    s = jnp.full_like(t, SIN[-1])
    for k in SIN[-2::-1]:
        s = s * t + k
    return c, s * u


def swapped(v):
    return pltpu.roll(v, HALF, 1)


def low_lanes(rows):
    return lax.broadcasted_iota(jnp.int32, (rows, LANES), 1) < HALF


def kernel(x_hbm, det_hbm, tid_hbm, inter_hbm, lag_hbm, o_ref,
           x_ref, det_ref, tid_ref, inter_ref, lag_ref, pbuf, gsend, gbuf, idbuf, rowbuf, rows_s, upper,
           send_buf, xrecv, table, picked, osend, orecv,
           own, cross, det, mat, wl, zc, zs, fac_c, fac_s, pairs_c, pairs_s, turned_c, turned_s,
           l_sem, p_send, p_recv, i_send, i_recv, g_send, g_recv, c_send, c_recv, fg_send, f_send,
           t_send, t_recv, o_send, o_recv):
    tm = lax.axis_index("tm")
    h = lax.axis_index("freq")
    core, z_lo = h % 2, h // 2
    x = tm % 4
    f32, bf16 = jnp.float32, jnp.bfloat16

    quarter = (1 - z_lo) * 2 + x % 2
    mine = tm // 16 * 8 + tm // 4 % 4 * 2 + x // 2
    slot_of_me = tm // 4 * 2 + x // 2
    other = (tm, h + 1 - 2 * core)

    def home(j):
        return j // 8 * 16 + j // 2 % 4 * 4 + core + j % 2 * 2, (1 - z_lo) * 2 + x % 2

    def source(s):
        return 4 * (s // 2) + 2 * (s % 2) + core, quarter

    def remote(src, dst, send, recv, to):
        return pltpu.make_async_remote_copy(
            src_ref=src, dst_ref=dst, send_sem=send, recv_sem=recv, device_id=to, device_id_type=MESH)

    barrier = pltpu.get_barrier_semaphore()
    for k in range(PEERS):
        pl.semaphore_signal(barrier, inc=1, device_id=home(k), device_id_type=MESH)
        pl.semaphore_signal(barrier, inc=1, device_id=source(k), device_id_type=MESH)
    for d in range(1, 4):
        pl.semaphore_signal(barrier, inc=1, device_id=(tm, (h + d) % 4), device_id_type=MESH)

    x_in = pltpu.make_async_copy(x_hbm, x_ref, l_sem.at[0])
    det_in = pltpu.make_async_copy(det_hbm, det_ref, l_sem.at[1])
    inter_in = pltpu.make_async_copy(inter_hbm, inter_ref, l_sem.at[2])
    lag_in = pltpu.make_async_copy(lag_hbm, lag_ref, l_sem.at[3])
    tid_in = pltpu.make_async_copy(tid_hbm, tid_ref, l_sem.at[4])
    for copy in (x_in, det_in, inter_in, lag_in, tid_in):
        copy.start()

    lane = lax.broadcasted_iota(jnp.int32, (1, LANES), 1)
    cq, sq_ = cos_sin((lane % 32).astype(f32) * (1.0 / NGRID))
    p_low = (lane // 32 + 32 * core).astype(f32)

    def z_rows(b, carry):
        at = pl.ds(pl.multiple_of(b * 16, 16), 16)
        row = lax.broadcasted_iota(jnp.int32, (16, LANES), 0) + b * 16
        row = jnp.where(row >= PERIOD, row - PERIOD, row).astype(f32)
        cr, sr = cos_sin(row * (1.0 / PERIOD))
        sine = (sr * cq + cr * sq_) * (0.5 / math.pi)
        for s in range(8):
            c, si = cos_sin(sine * (8.0 + 4.0 * (p_low + 4.0 * s)))
            zc[s, at, :] = c
            zs[s, at, :] = si
        return carry

    lax.fori_loop(0, ZROWS // 16, z_rows, 0)

    x_in.wait()
    re = x_ref[:, 0, :]
    im = x_ref[:, 1, :]
    sq = re * re + im * im
    part = sq[:, 0:LANES]
    for k in range(1, 8):
        part = part + sq[:, k * LANES:(k + 1) * LANES]
    part = jnp.concatenate([part, jnp.zeros((LANES - SPAN, LANES), f32)], 0)
    pbuf[h] = jnp.sum(part.T, axis=0, keepdims=True)
    low = low_lanes(SPAN)
    for k in range(8):
        r, i = re[:, k * LANES:(k + 1) * LANES], im[:, k * LANES:(k + 1) * LANES]
        send_buf[2 * k] = jnp.where(low, r, swapped(i)).astype(bf16)
        send_buf[2 * k + 1] = jnp.where(low, swapped(r), i).astype(bf16)

    lag_in.wait()

    def factor_rows(n, carry):
        l, b = n // 9 * 2, n % 9
        r0 = pl.multiple_of(b * 32, 32)
        lags = lag_ref[l], lag_ref[l + 1]
        for s in range(8):
            ci, si = zc[s, pl.ds(r0, 32), :], zs[s, pl.ds(r0, 32), :]
            for q in range(2):
                far = pl.ds(r0 + lags[q], 32)
                cj, sj = zc[s, far, :], zs[s, far, :]
                out = pl.ds(pl.multiple_of((l + q) * FOLD + r0, 32), 32)
                fac_c[s, out, :] = (cj * ci + sj * si).astype(bf16)
                fac_s[s, out, :] = (sj * ci - cj * si).astype(bf16)
        return carry

    lax.fori_loop(0, NLAG // 2 * 9, factor_rows, 0)
    tid_in.wait()

    pl.semaphore_wait(barrier, 2 * PEERS + 3)

    power_copies = [
        remote(pbuf.at[h], pbuf.at[h], p_send.at[d], p_recv.at[4 - d], (tm, (h + d) % 4)) for d in range(1, 4)]
    chunk_copies = [
        remote(send_buf.at[k], xrecv.at[tm], c_send.at[k], c_recv.at[tm], home(k)) for k in range(PEERS)]
    id_copies = [
        remote(tid_ref, idbuf.at[slot_of_me], i_send.at[k], i_recv.at[slot_of_me], home(k)) for k in range(PEERS)]
    for copy in power_copies + chunk_copies + id_copies:
        copy.start()

    for copy in power_copies:
        copy.wait()
    power = ((pbuf[0] + pbuf[1]) + (pbuf[2] + pbuf[3])) / NBIN
    gsend[...] = lax.rsqrt(power + 1e-06)
    scale_copies = [
        remote(gsend, gbuf.at[tm], g_send.at[k], g_recv.at[tm], home(k)) for k in range(PEERS)]
    for copy in scale_copies:
        copy.start()

    det_in.wait()
    inter_in.wait()
    for k in range(12):
        row = jnp.broadcast_to(det_ref[k:k + 1, :].astype(f32), (LANES, LANES))
        det[k * LANES:(k + 1) * LANES, :] = row.T
    for e in range(NDET):
        mat[e, NSFT:, :] = jnp.zeros((ROWS - NSFT, LANES), f32)

    def mat_rows(b, carry):
        at = pl.ds(pl.multiple_of(b * 32, 32), 32)
        d = det[at, :]
        for e in range(NDET):
            mat[e, at, :] = jnp.where(d == 0.0, inter_ref[e, 0], jnp.where(d == 1.0, inter_ref[e, 1], inter_ref[e, 2]))
        return carry

    lax.fori_loop(0, NSFT // 32, mat_rows, 0)

    def weight_rows(b, carry):
        r0 = pl.multiple_of(b * 16, 16)
        d = det[pl.ds(r0, 16), :]
        for l in range(NLAG):
            at = pl.ds(r0 + lag_ref[l], 16)
            wl[l, pl.ds(r0, 16), :] = jnp.where(
                d == 0.0, mat[0, at, :], jnp.where(d == 1.0, mat[1, at, :], mat[2, at, :]))
        return carry

    lax.fori_loop(0, NSFT // 16, weight_rows, 0)
    for l in range(NLAG):
        wl[l, NSFT:, :] = jnp.zeros((ROWS - NSFT, LANES), f32)
    own[NSFT:, :] = jnp.zeros((ROWS - NSFT, LANES), f32)
    cross[NSFT:, :] = jnp.zeros((ROWS - NSFT, LANES), f32)

    forwards = []
    for s in range(PEERS):
        slot = source(s)[0]
        remote(send_buf.at[0], xrecv.at[slot], c_send.at[s], c_recv.at[slot], source(s)).wait_recv()
        remote(gsend, gbuf.at[slot], g_send.at[s], g_recv.at[slot], source(s)).wait_recv()
        forwards.append(remote(xrecv.at[slot], xrecv.at[slot], f_send.at[s], c_recv.at[slot], other))
        forwards.append(remote(gbuf.at[slot], gbuf.at[slot], fg_send.at[s], g_recv.at[slot], other))
        forwards[-1].start()
        forwards[-2].start()

    for s in range(PEERS):
        remote(tid_ref, idbuf.at[s], i_send.at[s], i_recv.at[s], source(s)).wait_recv()
    ids = idbuf[...]
    turn_half = ids[:, 1, :] // 32
    rowbuf[...] = ids[:, 0, :] * 32 + (ids[:, 1, :] - 32 * turn_half)
    rows_in = pltpu.make_async_copy(rowbuf, rows_s, l_sem.at[5])
    rows_in.start()
    halves = jnp.concatenate([turn_half.astype(f32), jnp.zeros((LANES - PEERS, LANES), f32)], 0).T
    for s in range(PEERS):
        upper[s] = jnp.broadcast_to(halves[:, s:s + 1], (LANES, LANES))

    for s in range(PEERS):
        slot = source(s)[0] + 1 - 2 * core
        remote(xrecv.at[slot], xrecv.at[slot], f_send.at[s], c_recv.at[slot], other).wait_recv()
        remote(gbuf.at[slot], gbuf.at[slot], fg_send.at[s], g_recv.at[slot], other).wait_recv()

    scales = gbuf[:, 0, :]
    scales = jnp.concatenate([scales, jnp.zeros((LANES - TM, LANES), f32)], 0).T[0:SPAN]
    sign = jnp.where(low, 1.0, -1.0)
    for b in range(TM):
        g = jnp.broadcast_to(scales[:, b:b + 1], (SPAN, LANES))
        v = xrecv[b].astype(f32) * g
        own[b * SPAN:(b + 1) * SPAN, :] = v
        cross[b * SPAN:(b + 1) * SPAN, :] = swapped(v) * sign

    def pair_rows(turns, n, carry):
        b, part = n // 3, n % 3
        r0 = pl.multiple_of(b * 16, 16)
        real = lax.broadcasted_iota(jnp.int32, (16, LANES), 0) + r0 < PERIOD
        lags = [lag_ref[4 * part + q] for q in range(4)]
        sums = [[jnp.zeros((16, LANES), f32)] * 2 for _ in range(4)]
        for m in range(turns):
            here = pl.ds(r0 + PERIOD * m, 16)
            u = own[here, :]
            for q in range(4):
                far = pl.ds(r0 + PERIOD * m + lags[q], 16)
                uw = u * wl[4 * part + q, here, :]
                sums[q] = [sums[q][0] + uw * own[far, :], sums[q][1] + uw * cross[far, :]]
        for q in range(4):
            out = pl.ds(pl.multiple_of((4 * part + q) * FOLD + r0, 16), 16)
            pairs_c[out, :] = jnp.where(real, sums[q][0], 0.0)
            pairs_s[out, :] = jnp.where(real, sums[q][1], 0.0)
        return carry

    last = (NSFT - PERIOD * (TURNS - 1) + 15) // 16
    lax.fori_loop(0, last * 3, functools.partial(pair_rows, TURNS), 0)
    lax.fori_loop(last * 3, 18 * 3, functools.partial(pair_rows, TURNS - 1), 0)

    def turn(b, carry):
        for q in range(3):
            at = pl.ds(pl.multiple_of((b * 3 + q) * LANES, LANES), LANES)
            turned_c[b * 3 + q] = pairs_c[at, :].T.astype(bf16)
            turned_s[b * 3 + q] = pairs_s[at, :].T.astype(bf16)
        return carry

    lax.fori_loop(0, DEPTH // LANES // 3, turn, 0)

    scale = 1.0 / math.sqrt(NSFT * NLAG)

    def swap_copy(b):
        rows = pl.ds(pl.multiple_of(core * POINTS + b * WIDE, WIDE), WIDE)
        return remote(table.at[rows], table.at[rows], t_send.at[b], t_recv.at[b], other)

    def multiply(b, carry):
        sums = []
        for turned, fac in ((turned_c, fac_c), (turned_s, fac_s)):
            lhs = jnp.concatenate([turned[k] for k in range(DEPTH // LANES)], 1)
            rhs = jnp.concatenate([fac[2 * b], fac[2 * b + 1]], 1)
            both = jnp.dot(lhs, rhs, preferred_element_type=f32) * scale
            sums.append(both[0:HALF] + both[HALF:])
        stat = jnp.concatenate([sums[0] + sums[1], sums[0] - sums[1]], 0)
        for q in range(2):
            at = pl.ds(pl.multiple_of(core * POINTS + b * WIDE + q * LANES, LANES), LANES)
            table[at, :] = stat[:, q * LANES:(q + 1) * LANES].T
        swap_copy(b).start()
        return carry

    lax.fori_loop(0, POINTS // WIDE, multiply, 0)

    for copy in id_copies + chunk_copies + scale_copies + forwards:
        copy.wait_send()
    rows_in.wait()
    for b in range(POINTS // WIDE):
        rows = pl.ds(pl.multiple_of((1 - core) * POINTS + b * WIDE, WIDE), WIDE)
        remote(table.at[rows], table.at[rows], t_send.at[b], t_recv.at[b], other).wait_recv()

    low = low_lanes(HALF)

    def serve(s, carry):
        for t in range(LANES):
            picked[t:t + 1, :] = table[pl.ds(rows_s[s, t], 1), :]
        first, second = picked[0:HALF, :], picked[HALF:, :]
        first = jnp.where(upper[s, 0:HALF, :] == 0.0, first, swapped(first))
        second = jnp.where(upper[s, HALF:, :] == 0.0, swapped(second), second)
        osend[s] = jnp.where(low, first, second).astype(bf16)
        remote(osend.at[s], orecv.at[mine], o_send.at[s], o_recv.at[mine], source(s)).start()
        return carry

    lax.fori_loop(0, PEERS, serve, 0)

    for b in range(POINTS // WIDE):
        swap_copy(b).wait_send()
    for k in range(8):
        for j in (2 * k, 2 * k + 1):
            remote(osend.at[j], orecv.at[j], o_send.at[j], o_recv.at[j], home(j)).wait_recv()
        a, b = orecv[2 * k].astype(f32), orecv[2 * k + 1].astype(f32)
        o_ref[0:HALF, k * LANES:(k + 1) * LANES] = jnp.where(low, a, swapped(b)).astype(bf16)
        o_ref[HALF:, k * LANES:(k + 1) * LANES] = jnp.where(low, swapped(a), b).astype(bf16)

    for s in range(PEERS):
        remote(osend.at[s], orecv.at[mine], o_send.at[s], o_recv.at[mine], source(s)).wait_send()


def shards(sfts, detector_ids, intersection, lags, template_ids):
    bf16, f32, i32 = jnp.bfloat16, jnp.float32, jnp.int32
    vmem = pl.BlockSpec(memory_space=pltpu.VMEM)
    hbm = pl.BlockSpec(memory_space=pltpu.HBM)
    dma = pltpu.SemaphoreType.DMA
    out = pl.pallas_call(
        kernel,
        out_shape=jax.ShapeDtypeStruct((LANES, 8 * LANES), bf16),
        in_specs=[hbm] * 5,
        out_specs=vmem,
        scratch_shapes=[
            pltpu.VMEM((SPAN, 2, 8 * LANES), f32),
            pltpu.VMEM((12, LANES), i32),
            pltpu.VMEM((2, LANES), i32),
            pltpu.SMEM((NDET, NDET), f32),
            pltpu.SMEM((NLAG,), i32),
            pltpu.VMEM((4, 1, LANES), f32),
            pltpu.VMEM((1, LANES), f32),
            pltpu.VMEM((TM, 1, LANES), f32),
            pltpu.VMEM((PEERS, 2, LANES), i32),
            pltpu.VMEM((PEERS, LANES), i32),
            pltpu.SMEM((PEERS, LANES), i32),
            pltpu.VMEM((PEERS, LANES, LANES), f32),
            pltpu.VMEM((PEERS, SPAN, LANES), bf16),
            pltpu.VMEM((TM, SPAN, LANES), bf16),
            pltpu.VMEM((2 * POINTS, LANES), f32),
            pltpu.VMEM((LANES, LANES), f32),
            pltpu.VMEM((PEERS, HALF, LANES), bf16),
            pltpu.VMEM((PEERS, HALF, LANES), bf16),
            pltpu.VMEM((ROWS, LANES), f32),
            pltpu.VMEM((ROWS, LANES), f32),
            pltpu.VMEM((NSFT, LANES), f32),
            pltpu.VMEM((NDET, ROWS, LANES), f32),
            pltpu.VMEM((NLAG, ROWS, LANES), f32),
            pltpu.VMEM((8, ZROWS, LANES), f32),
            pltpu.VMEM((8, ZROWS, LANES), f32),
            pltpu.VMEM((8, DEPTH, LANES), bf16),
            pltpu.VMEM((8, DEPTH, LANES), bf16),
            pltpu.VMEM((DEPTH, LANES), f32),
            pltpu.VMEM((DEPTH, LANES), f32),
            pltpu.VMEM((DEPTH // LANES, LANES, LANES), bf16),
            pltpu.VMEM((DEPTH // LANES, LANES, LANES), bf16),
            dma((6,)), dma((4,)), dma((4,)), dma((PEERS,)), dma((PEERS,)), dma((PEERS,)), dma((TM,)),
            dma((PEERS,)), dma((TM,)), dma((PEERS,)), dma((PEERS,)), dma((4,)), dma((4,)), dma((PEERS,)), dma((PEERS,)),
        ],
        compiler_params=pltpu.CompilerParams(
            collective_id=0, has_side_effects=True, vmem_limit_bytes=66_700_000),
    )(sfts, detector_ids.reshape(12, LANES), template_ids.T, intersection, lags)
    return out.astype(f32)


def solution(mesh):
    in_specs = (P("tm", None, "freq"), P(), P(), P(), P("tm", None))
    out_specs = P("tm", "freq")
    return jax.shard_map(shards, mesh=mesh, in_specs=in_specs, out_specs=out_specs, check_vma=False)
```

```python
import functools
import math

import jax
import jax.numpy as jnp
from jax import lax
from jax.experimental import pallas as pl
from jax.experimental.pallas import tpu as pltpu
from jax.sharding import PartitionSpec as P

NSFT = 1536
NBIN = 4096
LAGMAX = 16
NLAG = 12
NDET = 3
NGRID = 64
PERIOD = 283
TM = 32
SPAN = 48
FOLD = 288
TURNS = 6
LANES = 128
ROWS = 1600
ZROWS = 304
DEPTH = 2 * NLAG * FOLD
PART = 1024
WIDE = 256
MESH = pl.DeviceIdType.MESH

COS = (0.9999999890590238, -19.739204499453965, 64.93911745989729, -85.45013953090921,
       60.167630951124465, -25.967599248993793, 6.528658161871135)
SIN = (6.28318527244795, -41.34169703820007, 81.60502363804078, -76.7015376703427,
       42.016075762415646, -14.86832275264805, 3.199338844584104)


def cos_sin(turns):
    u = turns - jnp.floor(turns + 0.5)
    t = u * u
    c = jnp.full_like(t, COS[-1])
    for k in COS[-2::-1]:
        c = c * t + k
    s = jnp.full_like(t, SIN[-1])
    for k in SIN[-2::-1]:
        s = s * t + k
    return c, s * u


def kernel(x_hbm, det_hbm, tid_hbm, inter_hbm, lag_hbm, o_ref,
           x_ref, det_ref, tid_ref, inter_ref, lag_ref, pbuf, gsend, gbuf, idbuf, send_buf, xrecv, osend, orecv,
           xre, xim, det, wl, amp_cos, amp_sin, zc, zs, fac, pairs, pairs_t,
           l_sem, p_send, p_recv, i_send, i_recv, g_send, g_recv, c_send, c_recv, fg_send, f_send, o_send, o_recv):
    tm = lax.axis_index("tm")
    h = lax.axis_index("freq")
    core, z_lo = h % 2, h // 2
    x = tm % 4
    f32, bf16 = jnp.float32, jnp.bfloat16

    quarter = (1 - z_lo) * 2 + x % 2
    group = 2 * (x // 2) + core

    def home(k, e):
        return 4 * k + core + 2 * e, (1 - z_lo) * 2 + x % 2

    def source(s):
        return 4 * (s // 2) + 2 * (s % 2) + core, quarter

    def owner(s):
        return 4 * s + group, quarter

    def remote(src, dst, send, recv, to):
        return pltpu.make_async_remote_copy(
            src_ref=src, dst_ref=dst, send_sem=send, recv_sem=recv, device_id=to, device_id_type=MESH)

    barrier = pltpu.get_barrier_semaphore()
    for k in range(8):
        for e in range(2):
            pl.semaphore_signal(barrier, inc=1, device_id=home(k, e), device_id_type=MESH)
    for s in range(16):
        pl.semaphore_signal(barrier, inc=1, device_id=source(s), device_id_type=MESH)
    for d in range(1, 4):
        pl.semaphore_signal(barrier, inc=1, device_id=(tm, (h + d) % 4), device_id_type=MESH)

    det_in = pltpu.make_async_copy(det_hbm, det_ref, l_sem.at[0])
    x_in = pltpu.make_async_copy(x_hbm, x_ref, l_sem.at[1])
    tid_in = pltpu.make_async_copy(tid_hbm, tid_ref, l_sem.at[2])
    inter_in = pltpu.make_async_copy(inter_hbm, inter_ref, l_sem.at[3])
    lag_in = pltpu.make_async_copy(lag_hbm, lag_ref, l_sem.at[4])
    x_in.start()
    det_in.start()
    inter_in.start()
    lag_in.start()
    tid_in.start()

    x_in.wait()
    part = jnp.zeros((SPAN, LANES), f32)
    for k in range(8):
        re = x_ref[pl.ds(2 * k, SPAN, stride=16), :]
        im = x_ref[pl.ds(2 * k + 1, SPAN, stride=16), :]
        part = part + (re * re + im * im)
        send_buf[k, 0:SPAN, :] = re.astype(bf16)
        send_buf[k, SPAN:, :] = im.astype(bf16)
    part = jnp.concatenate([part, jnp.zeros((LANES - SPAN, LANES), f32)], 0)
    pbuf[h] = jnp.sum(part.T, axis=0, keepdims=True)
    tid_in.wait()

    pl.semaphore_wait(barrier, 35)

    power_copies = [
        remote(pbuf.at[h], pbuf.at[h], p_send.at[d], p_recv.at[4 - d], (tm, (h + d) % 4)) for d in range(1, 4)]
    id_copies = [
        remote(tid_ref, idbuf.at[tm // 4], i_send.at[k], i_recv.at[tm // 4], home(k, x // 2)) for k in range(8)]
    chunk_copies = [
        remote(send_buf.at[k], xrecv.at[tm], c_send.at[2 * k + e], c_recv.at[tm], home(k, e))
        for k in range(8) for e in range(2)]
    for copy in power_copies + id_copies + chunk_copies:
        copy.start()

    det_in.wait()
    inter_in.wait()
    lag_in.wait()
    det[NSFT:, :] = jnp.full((ROWS - NSFT, LANES), float(NDET), f32)
    for k in range(12):
        row = jnp.broadcast_to(det_ref[k:k + 1, :].astype(f32), (LANES, LANES))
        det[k * LANES:(k + 1) * LANES, :] = row.T

    def weight_rows(last, b, carry):
        at = pl.ds(pl.multiple_of(b * 16, 16), 16)
        d = det[at, :]
        with_far = [
            jnp.where(d == 0.0, inter_ref[0, e], jnp.where(d == 1.0, inter_ref[1, e], inter_ref[2, e]))
            for e in range(NDET)]
        for l in range(NLAG):
            far = det[pl.ds(b * 16 + lag_ref[l], 16), :]
            w = jnp.where(far == 0.0, with_far[0], jnp.where(far == 1.0, with_far[1], with_far[2]))
            wl[l, at, :] = jnp.where(far == float(NDET), 0.0, w) if last else w
        return carry

    whole = NSFT // 16 - 1
    lax.fori_loop(0, whole, functools.partial(weight_rows, False), 0)
    weight_rows(True, whole, 0)
    for l in range(NLAG):
        wl[l, NSFT:, :] = jnp.zeros((ROWS - NSFT, LANES), f32)
    xre[NSFT:, :] = jnp.zeros((ROWS - NSFT, LANES), f32)
    xim[NSFT:, :] = jnp.zeros((ROWS - NSFT, LANES), f32)

    for copy in power_copies:
        copy.wait()
    power = ((pbuf[0] + pbuf[1]) + (pbuf[2] + pbuf[3])) / NBIN
    gsend[...] = lax.rsqrt(power + 1e-06)
    scale_copies = [
        remote(gsend, gbuf.at[tm], g_send.at[2 * k + e], g_recv.at[tm], home(k, e))
        for k in range(8) for e in range(2)]
    for copy in scale_copies:
        copy.start()

    for s in range(8):
        remote(tid_ref, idbuf.at[s], i_send.at[s], i_recv.at[s], owner(s)).wait_recv()
    ids = idbuf[...].astype(f32)
    amp = (8.0 + 4.0 * ids[:, 0, :]) * (0.5 / math.pi)
    cq, sq_ = cos_sin(ids[:, 1, :] * (1.0 / NGRID))
    amp_cos[...] = amp * cq
    amp_sin[...] = amp * sq_

    def z_rows(b, carry):
        at = pl.ds(pl.multiple_of(b * 16, 16), 16)
        row = lax.broadcasted_iota(jnp.int32, (16, LANES), 0) + b * 16
        row = jnp.where(row >= PERIOD, row - PERIOD, row).astype(f32)
        cr, sr = cos_sin(row * (1.0 / PERIOD))
        for s in range(8):
            c, si = cos_sin(sr * amp_cos[s:s + 1, :] + cr * amp_sin[s:s + 1, :])
            zc[s, at, :] = c
            zs[s, at, :] = si
        return carry

    lax.fori_loop(0, ZROWS // 16, z_rows, 0)

    def factor_rows(n, carry):
        l, b = n // 9 * 2, n % 9
        r0 = pl.multiple_of(b * 32, 32)
        lags = lag_ref[l], lag_ref[l + 1]
        for s in range(8):
            ci, si = zc[s, pl.ds(r0, 32), :], zs[s, pl.ds(r0, 32), :]
            for q in range(2):
                far = pl.ds(r0 + lags[q], 32)
                cj, sj = zc[s, far, :], zs[s, far, :]
                out = pl.multiple_of((l + q) * (2 * FOLD) + r0, 32)
                fac[s, pl.ds(out, 32), :] = (cj * ci + sj * si).astype(bf16)
                fac[s, pl.ds(out + FOLD, 32), :] = (sj * ci - cj * si).astype(bf16)
        return carry

    lax.fori_loop(0, 40, factor_rows, 0)

    other = (tm, h + 1 - 2 * core)
    forwards = []
    for s in range(16):
        slot = source(s)[0]
        remote(send_buf.at[0], xrecv.at[slot], c_send.at[s], c_recv.at[slot], source(s)).wait_recv()
        remote(gsend, gbuf.at[slot], g_send.at[s], g_recv.at[slot], source(s)).wait_recv()
        forwards.append(remote(xrecv.at[slot], xrecv.at[slot], f_send.at[s], c_recv.at[slot], other))
        forwards.append(remote(gbuf.at[slot], gbuf.at[slot], fg_send.at[s], g_recv.at[slot], other))
        forwards[-1].start()
        forwards[-2].start()
    lax.fori_loop(40, NLAG // 2 * 9, factor_rows, 0)

    for s in range(16):
        slot = source(s)[0] + 1 - 2 * core
        remote(xrecv.at[slot], xrecv.at[slot], f_send.at[s], c_recv.at[slot], other).wait_recv()
        remote(gbuf.at[slot], gbuf.at[slot], fg_send.at[s], g_recv.at[slot], other).wait_recv()

    scales = gbuf[:, 0, :]
    scales = jnp.concatenate([scales, jnp.zeros((LANES - TM, LANES), f32)], 0).T[0:SPAN]
    for b in range(TM):
        g = jnp.broadcast_to(scales[:, b:b + 1], (SPAN, LANES))
        xre[b * SPAN:(b + 1) * SPAN, :] = xrecv[b, 0:SPAN, :].astype(f32) * g
        xim[b * SPAN:(b + 1) * SPAN, :] = xrecv[b, SPAN:, :].astype(f32) * g

    def pair_rows(turns, n, carry):
        b, part = n // 2, n % 2
        r0 = pl.multiple_of(b * 16, 16)
        real = lax.broadcasted_iota(jnp.int32, (16, LANES), 0) + r0 < PERIOD
        lags = [lag_ref[6 * part + q] for q in range(6)]
        sums = [[jnp.zeros((16, LANES), f32)] * 2 for _ in range(6)]
        for m in range(turns):
            here = pl.ds(r0 + PERIOD * m, 16)
            a, bb = xre[here, :], xim[here, :]
            for q in range(6):
                far = pl.ds(r0 + PERIOD * m + lags[q], 16)
                w = wl[6 * part + q, here, :]
                c, d = xre[far, :] * w, xim[far, :] * w
                sums[q] = [sums[q][0] + (a * c + bb * d), sums[q][1] + (a * d - bb * c)]
        for q in range(6):
            out = pl.multiple_of((6 * part + q) * (2 * FOLD) + r0, 16)
            pairs[pl.ds(out, 16), :] = jnp.where(real, sums[q][0], 0.0)
            pairs[pl.ds(out + FOLD, 16), :] = jnp.where(real, sums[q][1], 0.0)
        return carry

    last = (NSFT - PERIOD * (TURNS - 1) + 15) // 16
    lax.fori_loop(0, last * 2, functools.partial(pair_rows, TURNS), 0)
    lax.fori_loop(last * 2, 18 * 2, functools.partial(pair_rows, TURNS - 1), 0)

    def turn(b, carry):
        for q in range(6):
            at = pl.ds(pl.multiple_of((b * 6 + q) * LANES, LANES), LANES)
            pairs_t[b * 6 + q] = pairs[at, :].T.astype(bf16)
        return carry

    lax.fori_loop(0, DEPTH // LANES // 6, turn, 0)

    scale = 1.0 / math.sqrt(NSFT * NLAG)

    def multiply(b, carry):
        lhs = jnp.concatenate([pairs_t[k] for k in range(DEPTH // LANES)], 1)
        rhs = jnp.concatenate([fac[2 * b], fac[2 * b + 1]], 1)
        stat = jnp.dot(lhs, rhs, preferred_element_type=f32) * scale
        for q in range(2):
            s = 2 * b + q
            osend[s] = stat[:, q * LANES:(q + 1) * LANES].T.astype(bf16)
            remote(osend.at[s], orecv.at[tm // 4], o_send.at[s], o_recv.at[tm // 4], owner(s)).start()
        return carry

    lax.fori_loop(0, PART // WIDE, multiply, 0)

    for copy in id_copies + chunk_copies + scale_copies + forwards:
        copy.wait_send()

    for k in range(8):
        remote(osend.at[k], orecv.at[k], o_send.at[k], o_recv.at[k], home(k, x // 2)).wait_recv()
        o_ref[:, k * LANES:(k + 1) * LANES] = orecv[k]

    for s in range(8):
        remote(osend.at[s], orecv.at[tm // 4], o_send.at[s], o_recv.at[tm // 4], owner(s)).wait_send()


def shards(sfts, detector_ids, intersection, lags, template_ids):
    bf16, f32 = jnp.bfloat16, jnp.float32
    vmem = pl.BlockSpec(memory_space=pltpu.VMEM)
    hbm = pl.BlockSpec(memory_space=pltpu.HBM)
    dma = pltpu.SemaphoreType.DMA
    rows = sfts.reshape(SPAN, 2, 8, LANES).transpose(0, 2, 1, 3).reshape(SPAN * 16, LANES)
    out = pl.pallas_call(
        kernel,
        out_shape=pltpu.VMEM((LANES, 8 * LANES), bf16),
        in_specs=[hbm] * 5,
        out_specs=vmem,
        scratch_shapes=[
            pltpu.VMEM((SPAN * 16, LANES), f32),
            pltpu.VMEM((12, LANES), jnp.int32),
            pltpu.VMEM((2, LANES), jnp.int32),
            pltpu.SMEM((NDET, NDET), f32),
            pltpu.SMEM((NLAG,), jnp.int32),
            pltpu.VMEM((4, 1, LANES), f32),
            pltpu.VMEM((1, LANES), f32),
            pltpu.VMEM((TM, 1, LANES), f32),
            pltpu.VMEM((8, 2, LANES), jnp.int32),
            pltpu.VMEM((8, 2 * SPAN, LANES), bf16),
            pltpu.VMEM((TM, 2 * SPAN, LANES), bf16),
            pltpu.VMEM((8, LANES, LANES), bf16),
            pltpu.VMEM((8, LANES, LANES), bf16),
            pltpu.VMEM((ROWS, LANES), f32),
            pltpu.VMEM((ROWS, LANES), f32),
            pltpu.VMEM((ROWS, LANES), f32),
            pltpu.VMEM((NLAG, ROWS, LANES), f32),
            pltpu.VMEM((8, LANES), f32),
            pltpu.VMEM((8, LANES), f32),
            pltpu.VMEM((8, ZROWS, LANES), f32),
            pltpu.VMEM((8, ZROWS, LANES), f32),
            pltpu.VMEM((8, DEPTH, LANES), bf16),
            pltpu.VMEM((DEPTH, LANES), f32),
            pltpu.VMEM((DEPTH // LANES, LANES, LANES), bf16),
            dma((5,)), dma((4,)), dma((4,)), dma((8,)), dma((8,)), dma((16,)), dma((TM,)), dma((16,)), dma((TM,)),
            dma((16,)), dma((16,)), dma((8,)), dma((8,)),
        ],
        compiler_params=pltpu.CompilerParams(
            collective_id=0, has_side_effects=True, vmem_limit_bytes=60 * 1024 * 1024),
    )(rows, detector_ids.reshape(12, LANES), template_ids.T, intersection, lags)
    return out.astype(f32)


def solution(mesh):
    in_specs = (P("tm", None, "freq"), P(), P(), P(), P("tm", None))
    out_specs = P("tm", "freq")
    return jax.shard_map(shards, mesh=mesh, in_specs=in_specs, out_specs=out_specs, check_vma=False)
```

```python
import functools
import math

import jax
import jax.numpy as jnp
from jax import lax
from jax.experimental import pallas as pl
from jax.experimental.pallas import tpu as pltpu
from jax.sharding import PartitionSpec as P

NSFT = 1536
NBIN = 4096
LAGMAX = 16
NLAG = 12
NDET = 3
NGRID = 64
PERIOD = 283
TM = 32
SPAN = 48
FOLD = 288
TURNS = 6
LANES = 128
ROWS = 1600
ZROWS = 320
DEPTH = 2 * NLAG * FOLD
PART = 1024
WIDE = 256
MESH = pl.DeviceIdType.MESH

COS = (0.9999999890590238, -19.739204499453965, 64.93911745989729, -85.45013953090921,
       60.167630951124465, -25.967599248993793, 6.528658161871135)
SIN = (6.28318527244795, -41.34169703820007, 81.60502363804078, -76.7015376703427,
       42.016075762415646, -14.86832275264805, 3.199338844584104)


def cos_sin(turns):
    u = turns - jnp.floor(turns + 0.5)
    t = u * u
    c = jnp.full_like(t, COS[-1])
    for k in COS[-2::-1]:
        c = c * t + k
    s = jnp.full_like(t, SIN[-1])
    for k in SIN[-2::-1]:
        s = s * t + k
    return c, s * u


def kernel(x_hbm, det_hbm, tid_hbm, inter_hbm, lag_hbm, o_ref,
           x_ref, det_ref, tid_ref, inter_ref, lag_ref, pbuf, gsend, gbuf, idbuf, send_buf, xrecv, osend, orecv,
           xre, xim, det, wl, amp_cos, amp_sin, orbit_cos, orbit_sin, zc, zs, fac, pairs, pairs_t,
           l_sem, p_send, p_recv, i_send, i_recv, g_send, g_recv, c_send, c_recv, fg_send, f_send, o_send, o_recv):
    tm = lax.axis_index("tm")
    h = lax.axis_index("freq")
    core, z_lo = h % 2, h // 2
    x = tm % 4
    f32, bf16 = jnp.float32, jnp.bfloat16

    quarter = (1 - z_lo) * 2 + x % 2
    group = 2 * (x // 2) + core

    def home(k, e):
        return 4 * k + core + 2 * e, (1 - z_lo) * 2 + x % 2

    def source(s):
        return 4 * (s // 2) + 2 * (s % 2) + core, quarter

    y = tm // 4 % 4

    def owner(p):
        return p % 2 * 16 + (y + p // 2 + 2) % 4 * 4 + group, quarter

    def place(to):
        return (y - to[0] // 4 % 4 + 2) % 4 * 2 + tm // 16

    def remote(src, dst, send, recv, to):
        return pltpu.make_async_remote_copy(
            src_ref=src, dst_ref=dst, send_sem=send, recv_sem=recv, device_id=to, device_id_type=MESH)

    barrier = pltpu.get_barrier_semaphore()
    for k in range(8):
        for e in range(2):
            pl.semaphore_signal(barrier, inc=1, device_id=home(k, e), device_id_type=MESH)
    for s in range(16):
        pl.semaphore_signal(barrier, inc=1, device_id=source(s), device_id_type=MESH)
    for d in range(1, 4):
        pl.semaphore_signal(barrier, inc=1, device_id=(tm, (h + d) % 4), device_id_type=MESH)

    det_in = pltpu.make_async_copy(det_hbm, det_ref, l_sem.at[0])
    x_in = pltpu.make_async_copy(x_hbm, x_ref, l_sem.at[1])
    tid_in = pltpu.make_async_copy(tid_hbm, tid_ref, l_sem.at[2])
    inter_in = pltpu.make_async_copy(inter_hbm, inter_ref, l_sem.at[3])
    lag_in = pltpu.make_async_copy(lag_hbm, lag_ref, l_sem.at[4])
    x_in.start()
    det_in.start()
    inter_in.start()
    lag_in.start()
    tid_in.start()

    x_in.wait()
    part = jnp.zeros((SPAN, LANES), f32)
    for k in range(8):
        re = x_ref[pl.ds(2 * k, SPAN, stride=16), :]
        im = x_ref[pl.ds(2 * k + 1, SPAN, stride=16), :]
        part = part + (re * re + im * im)
        send_buf[k, 0:SPAN, :] = re.astype(bf16)
        send_buf[k, SPAN:, :] = im.astype(bf16)
    part = jnp.concatenate([part, jnp.zeros((LANES - SPAN, LANES), f32)], 0)
    pbuf[h] = jnp.sum(part.T, axis=0, keepdims=True)
    tid_in.wait()

    pl.semaphore_wait(barrier, 35)

    power_copies = [
        remote(pbuf.at[h], pbuf.at[h], p_send.at[d], p_recv.at[4 - d], (tm, (h + d) % 4)) for d in range(1, 4)]
    id_copies = [
        remote(tid_ref, idbuf.at[place(home(k, x // 2))], i_send.at[k], i_recv.at[place(home(k, x // 2))], home(k, x // 2))
        for k in range(8)]
    chunk_copies = [
        remote(send_buf.at[k], xrecv.at[tm], c_send.at[2 * k + e], c_recv.at[tm], home(k, e))
        for e in range(2) for k in range(8)]
    for copy in power_copies + id_copies + chunk_copies[:8]:
        copy.start()

    det_in.wait()
    inter_in.wait()
    lag_in.wait()
    det[NSFT:, :] = jnp.full((ROWS - NSFT, LANES), float(NDET), f32)
    for k in range(12):
        row = jnp.broadcast_to(det_ref[k:k + 1, :].astype(f32), (LANES, LANES))
        det[k * LANES:(k + 1) * LANES, :] = row.T

    def weight_rows(last, b, carry):
        at = pl.ds(pl.multiple_of(b * 16, 16), 16)
        d = det[at, :]
        with_far = [
            jnp.where(d == 0.0, inter_ref[0, e], jnp.where(d == 1.0, inter_ref[1, e], inter_ref[2, e]))
            for e in range(NDET)]
        for l in range(NLAG):
            far = det[pl.ds(b * 16 + lag_ref[l], 16), :]
            w = jnp.where(far == 0.0, with_far[0], jnp.where(far == 1.0, with_far[1], with_far[2]))
            wl[l, at, :] = jnp.where(far == float(NDET), 0.0, w) if last else w
        return carry

    whole = NSFT // 16 - 1
    lax.fori_loop(0, whole, functools.partial(weight_rows, False), 0)
    weight_rows(True, whole, 0)
    for l in range(NLAG):
        wl[l, NSFT:, :] = jnp.zeros((ROWS - NSFT, LANES), f32)
    xre[NSFT:, :] = jnp.zeros((ROWS - NSFT, LANES), f32)
    xim[NSFT:, :] = jnp.zeros((ROWS - NSFT, LANES), f32)

    for copy in power_copies:
        copy.wait()
    power = ((pbuf[0] + pbuf[1]) + (pbuf[2] + pbuf[3])) / NBIN
    gsend[...] = lax.rsqrt(power + 1e-06)
    scale_copies = [
        remote(gsend, gbuf.at[tm], g_send.at[2 * k + e], g_recv.at[tm], home(k, e))
        for k in range(8) for e in range(2)]
    for copy in scale_copies + chunk_copies[8:]:
        copy.start()

    def orbit_rows(b, carry):
        at = pl.ds(pl.multiple_of(b * 64, 64), 64)
        row = lax.broadcasted_iota(jnp.int32, (64, LANES), 0) + b * 64
        row = jnp.where(row >= PERIOD, row - PERIOD, row).astype(f32)
        orbit_cos[at, :], orbit_sin[at, :] = cos_sin(row * (1.0 / PERIOD))
        return carry

    lax.fori_loop(0, ZROWS // 64, orbit_rows, 0)

    def factors(s):
        remote(tid_ref, idbuf.at[s], i_send.at[s], i_recv.at[s], owner(s)).wait_recv()
        ids = idbuf[s].astype(f32)
        amp = (8.0 + 4.0 * ids[0:1, :]) * (0.5 / math.pi)
        cq, sq_ = cos_sin(ids[1:2, :] * (1.0 / NGRID))
        amp_cos[...] = jnp.broadcast_to(amp * cq, (8, LANES))
        amp_sin[...] = jnp.broadcast_to(amp * sq_, (8, LANES))

        def z_rows(b, carry):
            at = pl.ds(pl.multiple_of(b * 64, 64), 64)
            turns = orbit_sin[at, :] * amp_cos[0:1, :] + orbit_cos[at, :] * amp_sin[0:1, :]
            zc[s, at, :], zs[s, at, :] = cos_sin(turns)
            return carry

        lax.fori_loop(0, ZROWS // 64, z_rows, 0)

        def factor_rows(b, carry):
            r0 = pl.multiple_of(b * 32, 32)
            ci, si = zc[s, pl.ds(r0, 32), :], zs[s, pl.ds(r0, 32), :]
            for l in range(NLAG):
                far = pl.ds(r0 + lag_ref[l], 32)
                cj, sj = zc[s, far, :], zs[s, far, :]
                out = pl.multiple_of(l * (2 * FOLD) + r0, 32)
                fac[s, pl.ds(out, 32), :] = (cj * ci + sj * si).astype(bf16)
                fac[s, pl.ds(out + FOLD, 32), :] = (sj * ci - cj * si).astype(bf16)
            return carry

        lax.fori_loop(0, FOLD // 32, factor_rows, 0)

    for s in (4, 5, 6, 7, 2, 3, 0):
        factors(s)

    other = (tm, h + 1 - 2 * core)
    forwards = []
    for s in range(16):
        slot = source(s)[0]
        remote(send_buf.at[0], xrecv.at[slot], c_send.at[s], c_recv.at[slot], source(s)).wait_recv()
        remote(gsend, gbuf.at[slot], g_send.at[s], g_recv.at[slot], source(s)).wait_recv()
        forwards.append(remote(xrecv.at[slot], xrecv.at[slot], f_send.at[s], c_recv.at[slot], other))
        forwards.append(remote(gbuf.at[slot], gbuf.at[slot], fg_send.at[s], g_recv.at[slot], other))
        forwards[-1].start()
        forwards[-2].start()
    factors(1)

    for s in range(16):
        slot = source(s)[0] + 1 - 2 * core
        remote(xrecv.at[slot], xrecv.at[slot], f_send.at[s], c_recv.at[slot], other).wait_recv()
        remote(gbuf.at[slot], gbuf.at[slot], fg_send.at[s], g_recv.at[slot], other).wait_recv()

    scales = gbuf[:, 0, :]
    scales = jnp.concatenate([scales, jnp.zeros((LANES - TM, LANES), f32)], 0).T[0:SPAN]
    for b in range(TM):
        g = jnp.broadcast_to(scales[:, b:b + 1], (SPAN, LANES))
        xre[b * SPAN:(b + 1) * SPAN, :] = xrecv[b, 0:SPAN, :].astype(f32) * g
        xim[b * SPAN:(b + 1) * SPAN, :] = xrecv[b, SPAN:, :].astype(f32) * g

    def pair_rows(turns, n, carry):
        b, part = n // 2, n % 2
        r0 = pl.multiple_of(b * 16, 16)
        real = lax.broadcasted_iota(jnp.int32, (16, LANES), 0) + r0 < PERIOD
        lags = [lag_ref[6 * part + q] for q in range(6)]
        sums = [[jnp.zeros((16, LANES), f32)] * 2 for _ in range(6)]
        for m in range(turns):
            here = pl.ds(r0 + PERIOD * m, 16)
            a, bb = xre[here, :], xim[here, :]
            for q in range(6):
                far = pl.ds(r0 + PERIOD * m + lags[q], 16)
                w = wl[6 * part + q, here, :]
                c, d = xre[far, :] * w, xim[far, :] * w
                sums[q] = [sums[q][0] + (a * c + bb * d), sums[q][1] + (a * d - bb * c)]
        for q in range(6):
            out = pl.multiple_of((6 * part + q) * (2 * FOLD) + r0, 16)
            pairs[pl.ds(out, 16), :] = jnp.where(real, sums[q][0], 0.0)
            pairs[pl.ds(out + FOLD, 16), :] = jnp.where(real, sums[q][1], 0.0)
        return carry

    last = (NSFT - PERIOD * (TURNS - 1) + 15) // 16
    lax.fori_loop(0, last * 2, functools.partial(pair_rows, TURNS), 0)
    lax.fori_loop(last * 2, 18 * 2, functools.partial(pair_rows, TURNS - 1), 0)

    def turn(b, carry):
        for q in range(6):
            at = pl.ds(pl.multiple_of((b * 6 + q) * LANES, LANES), LANES)
            pairs_t[b * 6 + q] = pairs[at, :].T.astype(bf16)
        return carry

    lax.fori_loop(0, DEPTH // LANES // 6, turn, 0)

    scale = 1.0 / math.sqrt(NSFT * NLAG)

    def multiply(n, carry):
        b = n + n // 2 * (1 - n % 2 * 2)
        lhs = jnp.concatenate([pairs_t[k] for k in range(DEPTH // LANES)], 1)
        rhs = jnp.concatenate([fac[2 * b], fac[2 * b + 1]], 1)
        stat = jnp.dot(lhs, rhs, preferred_element_type=f32) * scale
        for q in range(2):
            s = 2 * b + q
            osend[s] = stat[:, q * LANES:(q + 1) * LANES].T.astype(bf16)
            remote(osend.at[s], orecv.at[tm // 4], o_send.at[s], o_recv.at[tm // 4], owner(s)).start()
        return carry

    lax.fori_loop(0, PART // WIDE, multiply, 0)

    for copy in id_copies + chunk_copies + scale_copies + forwards:
        copy.wait_send()

    for k in range(8):
        remote(osend.at[k], orecv.at[k], o_send.at[k], o_recv.at[k], home(k, x // 2)).wait_recv()
        o_ref[:, k * LANES:(k + 1) * LANES] = orecv[k]

    for s in range(8):
        remote(osend.at[s], orecv.at[tm // 4], o_send.at[s], o_recv.at[tm // 4], owner(s)).wait_send()


def shards(sfts, detector_ids, intersection, lags, template_ids):
    bf16, f32 = jnp.bfloat16, jnp.float32
    vmem = pl.BlockSpec(memory_space=pltpu.VMEM)
    hbm = pl.BlockSpec(memory_space=pltpu.HBM)
    dma = pltpu.SemaphoreType.DMA
    rows = sfts.reshape(SPAN, 2, 8, LANES).transpose(0, 2, 1, 3).reshape(SPAN * 16, LANES)
    out = pl.pallas_call(
        kernel,
        out_shape=pltpu.VMEM((LANES, 8 * LANES), bf16),
        in_specs=[hbm] * 5,
        out_specs=vmem,
        scratch_shapes=[
            pltpu.VMEM((SPAN * 16, LANES), f32),
            pltpu.VMEM((12, LANES), jnp.int32),
            pltpu.VMEM((2, LANES), jnp.int32),
            pltpu.SMEM((NDET, NDET), f32),
            pltpu.SMEM((NLAG,), jnp.int32),
            pltpu.VMEM((4, 1, LANES), f32),
            pltpu.VMEM((1, LANES), f32),
            pltpu.VMEM((TM, 1, LANES), f32),
            pltpu.VMEM((8, 2, LANES), jnp.int32),
            pltpu.VMEM((8, 2 * SPAN, LANES), bf16),
            pltpu.VMEM((TM, 2 * SPAN, LANES), bf16),
            pltpu.VMEM((8, LANES, LANES), bf16),
            pltpu.VMEM((8, LANES, LANES), bf16),
            pltpu.VMEM((ROWS, LANES), f32),
            pltpu.VMEM((ROWS, LANES), f32),
            pltpu.VMEM((ROWS, LANES), f32),
            pltpu.VMEM((NLAG, ROWS, LANES), f32),
            pltpu.VMEM((8, LANES), f32),
            pltpu.VMEM((8, LANES), f32),
            pltpu.VMEM((ZROWS, LANES), f32),
            pltpu.VMEM((ZROWS, LANES), f32),
            pltpu.VMEM((8, ZROWS, LANES), f32),
            pltpu.VMEM((8, ZROWS, LANES), f32),
            pltpu.VMEM((8, DEPTH, LANES), bf16),
            pltpu.VMEM((DEPTH, LANES), f32),
            pltpu.VMEM((DEPTH // LANES, LANES, LANES), bf16),
            dma((5,)), dma((4,)), dma((4,)), dma((8,)), dma((8,)), dma((16,)), dma((TM,)), dma((16,)), dma((TM,)),
            dma((16,)), dma((16,)), dma((8,)), dma((8,)),
        ],
        compiler_params=pltpu.CompilerParams(
            collective_id=0, has_side_effects=True, vmem_limit_bytes=60 * 1024 * 1024),
    )(rows, detector_ids.reshape(12, LANES), template_ids.T, intersection, lags)
    return out.astype(f32)


def solution(mesh):
    in_specs = (P("tm", None, "freq"), P(), P(), P(), P("tm", None))
    out_specs = P("tm", "freq")
    return jax.shard_map(shards, mesh=mesh, in_specs=in_specs, out_specs=out_specs, check_vma=False)
```

```python
import functools
import math

import jax
import jax.numpy as jnp
from jax import lax
from jax.experimental import pallas as pl
from jax.experimental.pallas import tpu as pltpu
from jax.sharding import PartitionSpec as P

NSFT = 1536
NBIN = 4096
LAGMAX = 16
NLAG = 12
NDET = 3
NGRID = 64
PERIOD = 283
TM = 32
SPAN = 48
FOLD = 288
TURNS = 6
LANES = 128
ROWS = 1600
ZROWS = 320
DEPTH = 2 * NLAG * FOLD
PART = 1024
WIDE = 256
MESH = pl.DeviceIdType.MESH

COS = (0.9999999890590238, -19.739204499453965, 64.93911745989729, -85.45013953090921,
       60.167630951124465, -25.967599248993793, 6.528658161871135)
SIN = (6.28318527244795, -41.34169703820007, 81.60502363804078, -76.7015376703427,
       42.016075762415646, -14.86832275264805, 3.199338844584104)


def cos_sin(turns):
    u = turns - jnp.floor(turns + 0.5)
    t = u * u
    c = jnp.full_like(t, COS[-1])
    for k in COS[-2::-1]:
        c = c * t + k
    s = jnp.full_like(t, SIN[-1])
    for k in SIN[-2::-1]:
        s = s * t + k
    return c, s * u


def kernel(x_hbm, det_hbm, tid_hbm, inter_hbm, lag_hbm, o_ref,
           x_ref, det_ref, tid_ref, inter_ref, lag_ref, pbuf, gsend, gbuf, idbuf, send_buf, xrecv, osend, orecv,
           xre, xim, det, wl, amp_cos, amp_sin, orbit_cos, orbit_sin, zc, zs, fac, pairs, pairs_t,
           l_sem, p_send, p_recv, i_send, i_recv, g_send, g_recv, c_send, c_recv, fg_send, f_send, o_send, o_recv):
    tm = lax.axis_index("tm")
    h = lax.axis_index("freq")
    core, z_lo = h % 2, h // 2
    x = tm % 4
    f32, bf16 = jnp.float32, jnp.bfloat16

    quarter = (1 - z_lo) * 2 + x % 2
    group = 2 * (x // 2) + core

    def home(k, e):
        return 4 * k + core + 2 * e, (1 - z_lo) * 2 + x % 2

    def source(s):
        return 4 * (s // 2) + 2 * (s % 2) + core, quarter

    y = tm // 4 % 4

    def owner(p):
        return 4 * p + group, quarter

    def place(to):
        return tm // 4

    def remote(src, dst, send, recv, to):
        return pltpu.make_async_remote_copy(
            src_ref=src, dst_ref=dst, send_sem=send, recv_sem=recv, device_id=to, device_id_type=MESH)

    barrier = pltpu.get_barrier_semaphore()
    for k in range(8):
        for e in range(2):
            pl.semaphore_signal(barrier, inc=1, device_id=home(k, e), device_id_type=MESH)
    for s in range(16):
        pl.semaphore_signal(barrier, inc=1, device_id=source(s), device_id_type=MESH)
    for d in range(1, 4):
        pl.semaphore_signal(barrier, inc=1, device_id=(tm, (h + d) % 4), device_id_type=MESH)

    det_in = pltpu.make_async_copy(det_hbm, det_ref, l_sem.at[0])
    x_in = pltpu.make_async_copy(x_hbm, x_ref, l_sem.at[1])
    tid_in = pltpu.make_async_copy(tid_hbm, tid_ref, l_sem.at[2])
    inter_in = pltpu.make_async_copy(inter_hbm, inter_ref, l_sem.at[3])
    lag_in = pltpu.make_async_copy(lag_hbm, lag_ref, l_sem.at[4])
    x_in.start()
    det_in.start()
    inter_in.start()
    lag_in.start()
    tid_in.start()

    x_in.wait()
    part = jnp.zeros((SPAN, LANES), f32)
    for k in range(8):
        re = x_ref[pl.ds(2 * k, SPAN, stride=16), :]
        im = x_ref[pl.ds(2 * k + 1, SPAN, stride=16), :]
        part = part + (re * re + im * im)
        send_buf[k, 0:SPAN, :] = re.astype(bf16)
        send_buf[k, SPAN:, :] = im.astype(bf16)
    part = jnp.concatenate([part, jnp.zeros((LANES - SPAN, LANES), f32)], 0)
    pbuf[h] = jnp.sum(part.T, axis=0, keepdims=True)
    tid_in.wait()

    pl.semaphore_wait(barrier, 35)

    power_copies = [
        remote(pbuf.at[h], pbuf.at[h], p_send.at[d], p_recv.at[4 - d], (tm, (h + d) % 4)) for d in range(1, 4)]
    id_copies = [
        remote(tid_ref, idbuf.at[place(home(k, x // 2))], i_send.at[k], i_recv.at[place(home(k, x // 2))], home(k, x // 2))
        for k in range(8)]
    chunk_copies = [
        remote(send_buf.at[k], xrecv.at[tm], c_send.at[2 * k + e], c_recv.at[tm], home(k, e))
        for e in range(2) for k in range(8)]
    for copy in power_copies + id_copies + chunk_copies[:12]:
        copy.start()

    det_in.wait()
    inter_in.wait()
    lag_in.wait()
    det[NSFT:, :] = jnp.full((ROWS - NSFT, LANES), float(NDET), f32)
    for k in range(12):
        row = jnp.broadcast_to(det_ref[k:k + 1, :].astype(f32), (LANES, LANES))
        det[k * LANES:(k + 1) * LANES, :] = row.T

    def weight_rows(last, b, carry):
        at = pl.ds(pl.multiple_of(b * 16, 16), 16)
        d = det[at, :]
        with_far = [
            jnp.where(d == 0.0, inter_ref[0, e], jnp.where(d == 1.0, inter_ref[1, e], inter_ref[2, e]))
            for e in range(NDET)]
        for l in range(NLAG):
            far = det[pl.ds(b * 16 + lag_ref[l], 16), :]
            w = jnp.where(far == 0.0, with_far[0], jnp.where(far == 1.0, with_far[1], with_far[2]))
            wl[l, at, :] = jnp.where(far == float(NDET), 0.0, w) if last else w
        return carry

    whole = NSFT // 16 - 1
    lax.fori_loop(0, 40, functools.partial(weight_rows, False), 0)
    weight_rows(True, whole, 0)
    for l in range(NLAG):
        wl[l, NSFT:, :] = jnp.zeros((ROWS - NSFT, LANES), f32)
    xre[NSFT:, :] = jnp.zeros((ROWS - NSFT, LANES), f32)
    xim[NSFT:, :] = jnp.zeros((ROWS - NSFT, LANES), f32)

    for copy in power_copies:
        copy.wait()
    power = ((pbuf[0] + pbuf[1]) + (pbuf[2] + pbuf[3])) / NBIN
    gsend[...] = lax.rsqrt(power + 1e-06)
    scale_copies = [
        remote(gsend, gbuf.at[tm], g_send.at[2 * k + e], g_recv.at[tm], home(k, e))
        for k in range(8) for e in range(2)]
    for copy in scale_copies + chunk_copies[12:]:
        copy.start()
    lax.fori_loop(40, whole, functools.partial(weight_rows, False), 0)

    def orbit_rows(b, carry):
        at = pl.ds(pl.multiple_of(b * 64, 64), 64)
        row = lax.broadcasted_iota(jnp.int32, (64, LANES), 0) + b * 64
        row = jnp.where(row >= PERIOD, row - PERIOD, row).astype(f32)
        orbit_cos[at, :], orbit_sin[at, :] = cos_sin(row * (1.0 / PERIOD))
        return carry

    lax.fori_loop(0, ZROWS // 64, orbit_rows, 0)

    def factors(s):
        remote(tid_ref, idbuf.at[s], i_send.at[s], i_recv.at[s], owner(s)).wait_recv()
        ids = idbuf[s].astype(f32)
        amp = (8.0 + 4.0 * ids[0:1, :]) * (0.5 / math.pi)
        cq, sq_ = cos_sin(ids[1:2, :] * (1.0 / NGRID))
        amp_cos[...] = jnp.broadcast_to(amp * cq, (8, LANES))
        amp_sin[...] = jnp.broadcast_to(amp * sq_, (8, LANES))

        def z_rows(b, carry):
            at = pl.ds(pl.multiple_of(b * 64, 64), 64)
            turns = orbit_sin[at, :] * amp_cos[0:1, :] + orbit_cos[at, :] * amp_sin[0:1, :]
            zc[s, at, :], zs[s, at, :] = cos_sin(turns)
            return carry

        lax.fori_loop(0, ZROWS // 64, z_rows, 0)

        def factor_rows(b, carry):
            r0 = pl.multiple_of(b * 32, 32)
            ci, si = zc[s, pl.ds(r0, 32), :], zs[s, pl.ds(r0, 32), :]
            for l in range(NLAG):
                far = pl.ds(r0 + lag_ref[l], 32)
                cj, sj = zc[s, far, :], zs[s, far, :]
                out = pl.multiple_of(l * (2 * FOLD) + r0, 32)
                fac[s, pl.ds(out, 32), :] = (cj * ci + sj * si).astype(bf16)
                fac[s, pl.ds(out + FOLD, 32), :] = (sj * ci - cj * si).astype(bf16)
            return carry

        lax.fori_loop(0, FOLD // 32, factor_rows, 0)

    for s in (4, 5, 6, 7, 2, 3, 0):
        factors(s)

    other = (tm, h + 1 - 2 * core)
    forwards = []
    for s in range(16):
        slot = source(s)[0]
        remote(send_buf.at[0], xrecv.at[slot], c_send.at[s], c_recv.at[slot], source(s)).wait_recv()
        remote(gsend, gbuf.at[slot], g_send.at[s], g_recv.at[slot], source(s)).wait_recv()
        forwards.append(remote(xrecv.at[slot], xrecv.at[slot], f_send.at[s], c_recv.at[slot], other))
        forwards.append(remote(gbuf.at[slot], gbuf.at[slot], fg_send.at[s], g_recv.at[slot], other))
        forwards[-1].start()
        forwards[-2].start()
    factors(1)

    for s in range(16):
        slot = source(s)[0] + 1 - 2 * core
        remote(xrecv.at[slot], xrecv.at[slot], f_send.at[s], c_recv.at[slot], other).wait_recv()
        remote(gbuf.at[slot], gbuf.at[slot], fg_send.at[s], g_recv.at[slot], other).wait_recv()

    scales = gbuf[:, 0, :]
    scales = jnp.concatenate([scales, jnp.zeros((LANES - TM, LANES), f32)], 0).T[0:SPAN]
    for b in range(TM):
        g = jnp.broadcast_to(scales[:, b:b + 1], (SPAN, LANES))
        xre[b * SPAN:(b + 1) * SPAN, :] = xrecv[b, 0:SPAN, :].astype(f32) * g
        xim[b * SPAN:(b + 1) * SPAN, :] = xrecv[b, SPAN:, :].astype(f32) * g

    def pair_rows(turns, n, carry):
        b, part = n // 2, n % 2
        r0 = pl.multiple_of(b * 16, 16)
        real = lax.broadcasted_iota(jnp.int32, (16, LANES), 0) + r0 < PERIOD
        lags = [lag_ref[6 * part + q] for q in range(6)]
        sums = [[jnp.zeros((16, LANES), f32)] * 2 for _ in range(6)]
        for m in range(turns):
            here = pl.ds(r0 + PERIOD * m, 16)
            a, bb = xre[here, :], xim[here, :]
            for q in range(6):
                far = pl.ds(r0 + PERIOD * m + lags[q], 16)
                w = wl[6 * part + q, here, :]
                c, d = xre[far, :] * w, xim[far, :] * w
                sums[q] = [sums[q][0] + (a * c + bb * d), sums[q][1] + (a * d - bb * c)]
        for q in range(6):
            out = pl.multiple_of((6 * part + q) * (2 * FOLD) + r0, 16)
            pairs[pl.ds(out, 16), :] = jnp.where(real, sums[q][0], 0.0)
            pairs[pl.ds(out + FOLD, 16), :] = jnp.where(real, sums[q][1], 0.0)
        return carry

    last = (NSFT - PERIOD * (TURNS - 1) + 15) // 16
    lax.fori_loop(0, last * 2, functools.partial(pair_rows, TURNS), 0)
    lax.fori_loop(last * 2, 18 * 2, functools.partial(pair_rows, TURNS - 1), 0)

    def turn(b, carry):
        for q in range(6):
            at = pl.ds(pl.multiple_of((b * 6 + q) * LANES, LANES), LANES)
            pairs_t[b * 6 + q] = pairs[at, :].T.astype(bf16)
        return carry

    lax.fori_loop(0, DEPTH // LANES // 6, turn, 0)

    scale = 1.0 / math.sqrt(NSFT * NLAG)

    def multiply(n, carry):
        b = n
        lhs = jnp.concatenate([pairs_t[k] for k in range(DEPTH // LANES)], 1)
        rhs = jnp.concatenate([fac[2 * b], fac[2 * b + 1]], 1)
        stat = jnp.dot(lhs, rhs, preferred_element_type=f32) * scale
        for q in range(2):
            s = 2 * b + q
            osend[s] = stat[:, q * LANES:(q + 1) * LANES].T.astype(bf16)
            remote(osend.at[s], orecv.at[tm // 4], o_send.at[s], o_recv.at[tm // 4], owner(s)).start()
        return carry

    lax.fori_loop(0, PART // WIDE, multiply, 0)

    for copy in id_copies + chunk_copies + scale_copies + forwards:
        copy.wait_send()

    for k in range(8):
        remote(osend.at[k], orecv.at[k], o_send.at[k], o_recv.at[k], home(k, x // 2)).wait_recv()
        o_ref[:, k * LANES:(k + 1) * LANES] = orecv[k]

    for s in range(8):
        remote(osend.at[s], orecv.at[tm // 4], o_send.at[s], o_recv.at[tm // 4], owner(s)).wait_send()


def shards(sfts, detector_ids, intersection, lags, template_ids):
    bf16, f32 = jnp.bfloat16, jnp.float32
    vmem = pl.BlockSpec(memory_space=pltpu.VMEM)
    hbm = pl.BlockSpec(memory_space=pltpu.HBM)
    dma = pltpu.SemaphoreType.DMA
    rows = sfts.reshape(SPAN, 2, 8, LANES).transpose(0, 2, 1, 3).reshape(SPAN * 16, LANES)
    out = pl.pallas_call(
        kernel,
        out_shape=pltpu.VMEM((LANES, 8 * LANES), bf16),
        in_specs=[hbm] * 5,
        out_specs=vmem,
        scratch_shapes=[
            pltpu.VMEM((SPAN * 16, LANES), f32),
            pltpu.VMEM((12, LANES), jnp.int32),
            pltpu.VMEM((2, LANES), jnp.int32),
            pltpu.SMEM((NDET, NDET), f32),
            pltpu.SMEM((NLAG,), jnp.int32),
            pltpu.VMEM((4, 1, LANES), f32),
            pltpu.VMEM((1, LANES), f32),
            pltpu.VMEM((TM, 1, LANES), f32),
            pltpu.VMEM((8, 2, LANES), jnp.int32),
            pltpu.VMEM((8, 2 * SPAN, LANES), bf16),
            pltpu.VMEM((TM, 2 * SPAN, LANES), bf16),
            pltpu.VMEM((8, LANES, LANES), bf16),
            pltpu.VMEM((8, LANES, LANES), bf16),
            pltpu.VMEM((ROWS, LANES), f32),
            pltpu.VMEM((ROWS, LANES), f32),
            pltpu.VMEM((ROWS, LANES), f32),
            pltpu.VMEM((NLAG, ROWS, LANES), f32),
            pltpu.VMEM((8, LANES), f32),
            pltpu.VMEM((8, LANES), f32),
            pltpu.VMEM((ZROWS, LANES), f32),
            pltpu.VMEM((ZROWS, LANES), f32),
            pltpu.VMEM((8, ZROWS, LANES), f32),
            pltpu.VMEM((8, ZROWS, LANES), f32),
            pltpu.VMEM((8, DEPTH, LANES), bf16),
            pltpu.VMEM((DEPTH, LANES), f32),
            pltpu.VMEM((DEPTH // LANES, LANES, LANES), bf16),
            dma((5,)), dma((4,)), dma((4,)), dma((8,)), dma((8,)), dma((16,)), dma((TM,)), dma((16,)), dma((TM,)),
            dma((16,)), dma((16,)), dma((8,)), dma((8,)),
        ],
        compiler_params=pltpu.CompilerParams(
            collective_id=0, has_side_effects=True, vmem_limit_bytes=60 * 1024 * 1024),
    )(rows, detector_ids.reshape(12, LANES), template_ids.T, intersection, lags)
    return out.astype(f32)


def solution(mesh):
    in_specs = (P("tm", None, "freq"), P(), P(), P(), P("tm", None))
    out_specs = P("tm", "freq")
    return jax.shard_map(shards, mesh=mesh, in_specs=in_specs, out_specs=out_specs, check_vma=False)
```

```python
import functools
import math

import jax
import jax.numpy as jnp
from jax import lax
from jax.experimental import pallas as pl
from jax.experimental.pallas import tpu as pltpu
from jax.sharding import PartitionSpec as P

NSFT = 1536
NBIN = 4096
LAGMAX = 16
NLAG = 12
NDET = 3
NGRID = 64
PERIOD = 283
TM = 32
SPAN = 48
FOLD = 288
TURNS = 6
LANES = 128
ROWS = 1600
ZROWS = 320
DEPTH = 2 * NLAG * FOLD
PART = 1024
WIDE = 256
MESH = pl.DeviceIdType.MESH

COS = (0.9999999890590238, -19.739204499453965, 64.93911745989729, -85.45013953090921,
       60.167630951124465, -25.967599248993793, 6.528658161871135)
SIN = (6.28318527244795, -41.34169703820007, 81.60502363804078, -76.7015376703427,
       42.016075762415646, -14.86832275264805, 3.199338844584104)


def cos_sin(turns):
    u = turns - jnp.floor(turns + 0.5)
    t = u * u
    c = jnp.full_like(t, COS[-1])
    for k in COS[-2::-1]:
        c = c * t + k
    s = jnp.full_like(t, SIN[-1])
    for k in SIN[-2::-1]:
        s = s * t + k
    return c, s * u


def kernel(x_hbm, det_hbm, tid_hbm, inter_hbm, lag_hbm, o_ref,
           x_ref, det_ref, tid_ref, inter_ref, lag_ref, pbuf, gsend, gbuf, idbuf, send_buf, xrecv, osend, orecv,
           xre, xim, det, wl, amp_cos, amp_sin, orbit_cos, orbit_sin, zc, zs, fac, pairs, pairs_t,
           l_sem, p_send, p_recv, i_send, i_recv, g_send, g_recv, c_send, c_recv, fg_send, f_send, o_send, o_recv):
    tm = lax.axis_index("tm")
    h = lax.axis_index("freq")
    core, z_lo = h % 2, h // 2
    x = tm % 4
    f32, bf16 = jnp.float32, jnp.bfloat16

    quarter = (1 - z_lo) * 2 + x % 2
    group = 2 * (x // 2) + core

    def home(k, e):
        return 4 * k + core + 2 * e, (1 - z_lo) * 2 + x % 2

    def source(s):
        return 4 * (s // 2) + 2 * (s % 2) + core, quarter

    y = tm // 4 % 4

    def owner(p):
        return 4 * p + group, quarter

    def place(to):
        return tm // 4

    def remote(src, dst, send, recv, to):
        return pltpu.make_async_remote_copy(
            src_ref=src, dst_ref=dst, send_sem=send, recv_sem=recv, device_id=to, device_id_type=MESH)

    det_in = pltpu.make_async_copy(det_hbm, det_ref, l_sem.at[0])
    x_in = pltpu.make_async_copy(x_hbm, x_ref, l_sem.at[1])
    tid_in = pltpu.make_async_copy(tid_hbm, tid_ref, l_sem.at[2])
    inter_in = pltpu.make_async_copy(inter_hbm, inter_ref, l_sem.at[3])
    lag_in = pltpu.make_async_copy(lag_hbm, lag_ref, l_sem.at[4])
    x_in.start()
    det_in.start()
    inter_in.start()
    lag_in.start()
    tid_in.start()

    barrier = pltpu.get_barrier_semaphore()
    for k in range(8):
        for e in range(2):
            pl.semaphore_signal(barrier, inc=1, device_id=home(k, e), device_id_type=MESH)
    for s in range(16):
        pl.semaphore_signal(barrier, inc=1, device_id=source(s), device_id_type=MESH)
    for d in range(1, 4):
        pl.semaphore_signal(barrier, inc=1, device_id=(tm, (h + d) % 4), device_id_type=MESH)

    x_in.wait()
    part = jnp.zeros((SPAN, LANES), f32)
    for k in range(8):
        re = x_ref[pl.ds(2 * k, SPAN, stride=16), :]
        im = x_ref[pl.ds(2 * k + 1, SPAN, stride=16), :]
        part = part + (re * re + im * im)
        send_buf[k, 0:SPAN, :] = re.astype(bf16)
        send_buf[k, SPAN:, :] = im.astype(bf16)
    part = jnp.concatenate([part, jnp.zeros((LANES - SPAN, LANES), f32)], 0)
    pbuf[h] = jnp.sum(part.T, axis=0, keepdims=True)
    det_in.wait()
    inter_in.wait()
    lag_in.wait()
    det[NSFT:, :] = jnp.full((ROWS - NSFT, LANES), float(NDET), f32)
    for k in range(12):
        row = jnp.broadcast_to(det_ref[k:k + 1, :].astype(f32), (LANES, LANES))
        det[k * LANES:(k + 1) * LANES, :] = row.T

    def weight_rows(last, b, carry):
        at = pl.ds(pl.multiple_of(b * 16, 16), 16)
        d = det[at, :]
        with_far = [
            jnp.where(d == 0.0, inter_ref[0, e], jnp.where(d == 1.0, inter_ref[1, e], inter_ref[2, e]))
            for e in range(NDET)]
        for l in range(NLAG):
            far = det[pl.ds(b * 16 + lag_ref[l], 16), :]
            w = jnp.where(far == 0.0, with_far[0], jnp.where(far == 1.0, with_far[1], with_far[2]))
            wl[l, at, :] = jnp.where(far == float(NDET), 0.0, w) if last else w
        return carry

    whole = NSFT // 16 - 1
    lax.fori_loop(0, 40, functools.partial(weight_rows, False), 0)
    weight_rows(True, whole, 0)
    for l in range(NLAG):
        wl[l, NSFT:, :] = jnp.zeros((ROWS - NSFT, LANES), f32)
    xre[NSFT:, :] = jnp.zeros((ROWS - NSFT, LANES), f32)
    xim[NSFT:, :] = jnp.zeros((ROWS - NSFT, LANES), f32)

    def orbit_rows(b, carry):
        at = pl.ds(pl.multiple_of(b * 64, 64), 64)
        row = lax.broadcasted_iota(jnp.int32, (64, LANES), 0) + b * 64
        row = jnp.where(row >= PERIOD, row - PERIOD, row).astype(f32)
        orbit_cos[at, :], orbit_sin[at, :] = cos_sin(row * (1.0 / PERIOD))
        return carry

    lax.fori_loop(0, ZROWS // 64, orbit_rows, 0)

    tid_in.wait()

    pl.semaphore_wait(barrier, 35)

    power_copies = [
        remote(pbuf.at[h], pbuf.at[h], p_send.at[d], p_recv.at[4 - d], (tm, (h + d) % 4)) for d in range(1, 4)]
    id_copies = [
        remote(tid_ref, idbuf.at[place(home(k, x // 2))], i_send.at[k], i_recv.at[place(home(k, x // 2))], home(k, x // 2))
        for k in range(8)]
    chunk_copies = [
        remote(send_buf.at[k], xrecv.at[tm], c_send.at[2 * k + e], c_recv.at[tm], home(k, e))
        for e in range(2) for k in range(8)]
    for copy in power_copies + id_copies + chunk_copies[:12]:
        copy.start()

    for copy in power_copies:
        copy.wait()
    power = ((pbuf[0] + pbuf[1]) + (pbuf[2] + pbuf[3])) / NBIN
    gsend[...] = lax.rsqrt(power + 1e-06)
    scale_copies = [
        remote(gsend, gbuf.at[tm], g_send.at[2 * k + e], g_recv.at[tm], home(k, e))
        for k in range(8) for e in range(2)]
    for copy in scale_copies + chunk_copies[12:]:
        copy.start()
    lax.fori_loop(40, whole, functools.partial(weight_rows, False), 0)

    def factors(s):
        remote(tid_ref, idbuf.at[s], i_send.at[s], i_recv.at[s], owner(s)).wait_recv()
        ids = idbuf[s].astype(f32)
        amp = (8.0 + 4.0 * ids[0:1, :]) * (0.5 / math.pi)
        cq, sq_ = cos_sin(ids[1:2, :] * (1.0 / NGRID))
        amp_cos[...] = jnp.broadcast_to(amp * cq, (8, LANES))
        amp_sin[...] = jnp.broadcast_to(amp * sq_, (8, LANES))

        def z_rows(b, carry):
            at = pl.ds(pl.multiple_of(b * 64, 64), 64)
            turns = orbit_sin[at, :] * amp_cos[0:1, :] + orbit_cos[at, :] * amp_sin[0:1, :]
            zc[s, at, :], zs[s, at, :] = cos_sin(turns)
            return carry

        lax.fori_loop(0, ZROWS // 64, z_rows, 0)

        def factor_rows(b, carry):
            r0 = pl.multiple_of(b * 32, 32)
            ci, si = zc[s, pl.ds(r0, 32), :], zs[s, pl.ds(r0, 32), :]
            for l in range(NLAG):
                far = pl.ds(r0 + lag_ref[l], 32)
                cj, sj = zc[s, far, :], zs[s, far, :]
                out = pl.multiple_of(l * (2 * FOLD) + r0, 32)
                fac[s, pl.ds(out, 32), :] = (cj * ci + sj * si).astype(bf16)
                fac[s, pl.ds(out + FOLD, 32), :] = (sj * ci - cj * si).astype(bf16)
            return carry

        lax.fori_loop(0, FOLD // 32, factor_rows, 0)

    for s in (4, 5, 6, 7, 2, 3, 0):
        factors(s)

    other = (tm, h + 1 - 2 * core)
    forwards = []
    for s in range(16):
        slot = source(s)[0]
        remote(send_buf.at[0], xrecv.at[slot], c_send.at[s], c_recv.at[slot], source(s)).wait_recv()
        remote(gsend, gbuf.at[slot], g_send.at[s], g_recv.at[slot], source(s)).wait_recv()
        forwards.append(remote(xrecv.at[slot], xrecv.at[slot], f_send.at[s], c_recv.at[slot], other))
        forwards.append(remote(gbuf.at[slot], gbuf.at[slot], fg_send.at[s], g_recv.at[slot], other))
        forwards[-1].start()
        forwards[-2].start()
    factors(1)

    for s in range(16):
        slot = source(s)[0] + 1 - 2 * core
        remote(xrecv.at[slot], xrecv.at[slot], f_send.at[s], c_recv.at[slot], other).wait_recv()
        remote(gbuf.at[slot], gbuf.at[slot], fg_send.at[s], g_recv.at[slot], other).wait_recv()

    scales = gbuf[:, 0, :]
    scales = jnp.concatenate([scales, jnp.zeros((LANES - TM, LANES), f32)], 0).T[0:SPAN]
    for b in range(TM):
        g = jnp.broadcast_to(scales[:, b:b + 1], (SPAN, LANES))
        xre[b * SPAN:(b + 1) * SPAN, :] = xrecv[b, 0:SPAN, :].astype(f32) * g
        xim[b * SPAN:(b + 1) * SPAN, :] = xrecv[b, SPAN:, :].astype(f32) * g

    def pair_rows(turns, n, carry):
        b, part = n // 2, n % 2
        r0 = pl.multiple_of(b * 16, 16)
        lags = [lag_ref[6 * part + q] for q in range(6)]
        sums = [None] * 6
        for m in range(turns):
            here = pl.ds(r0 + PERIOD * m, 16)
            a, bb = xre[here, :], xim[here, :]
            for q in range(6):
                far = pl.ds(r0 + PERIOD * m + lags[q], 16)
                w = wl[6 * part + q, here, :]
                c, d = xre[far, :] * w, xim[far, :] * w
                new = [a * c + bb * d, a * d - bb * c]
                sums[q] = new if m == 0 else [v + w_ for v, w_ in zip(sums[q], new)]
        for q in range(6):
            out = pl.multiple_of((6 * part + q) * (2 * FOLD) + r0, 16)
            pairs[pl.ds(out, 16), :] = sums[q][0].astype(bf16)
            pairs[pl.ds(out + FOLD, 16), :] = sums[q][1].astype(bf16)
        return carry

    last = (NSFT - PERIOD * (TURNS - 1) + 15) // 16
    lax.fori_loop(0, last * 2, functools.partial(pair_rows, TURNS), 0)
    lax.fori_loop(last * 2, 18 * 2, functools.partial(pair_rows, TURNS - 1), 0)

    for l in range(2 * NLAG):
        pairs[l * FOLD + PERIOD:(l + 1) * FOLD, :] = jnp.zeros((FOLD - PERIOD, LANES), bf16)

    def turn(b, carry):
        for q in range(9):
            at = pl.ds(pl.multiple_of((b * 9 + q) * LANES, LANES), LANES)
            pairs_t[b * 9 + q] = pairs[at, :].T
        return carry

    lax.fori_loop(0, DEPTH // LANES // 9, turn, 0)

    scale = 1.0 / math.sqrt(NSFT * NLAG)

    def multiply(n, carry):
        b = n
        lhs = jnp.concatenate([pairs_t[k] for k in range(DEPTH // LANES)], 1)
        rhs = jnp.concatenate([fac[2 * b], fac[2 * b + 1]], 1)
        stat = jnp.dot(lhs, rhs, preferred_element_type=f32) * scale
        for q in range(2):
            s = 2 * b + q
            osend[s] = stat[:, q * LANES:(q + 1) * LANES].T.astype(bf16)
            remote(osend.at[s], orecv.at[tm // 4], o_send.at[s], o_recv.at[tm // 4], owner(s)).start()
        return carry

    lax.fori_loop(0, PART // WIDE, multiply, 0)

    for copy in id_copies + chunk_copies + scale_copies + forwards:
        copy.wait_send()

    for k in range(8):
        remote(osend.at[k], orecv.at[k], o_send.at[k], o_recv.at[k], home(k, x // 2)).wait_recv()
        o_ref[:, k * LANES:(k + 1) * LANES] = orecv[k]

    for s in range(8):
        remote(osend.at[s], orecv.at[tm // 4], o_send.at[s], o_recv.at[tm // 4], owner(s)).wait_send()


def shards(sfts, detector_ids, intersection, lags, template_ids):
    bf16, f32 = jnp.bfloat16, jnp.float32
    vmem = pl.BlockSpec(memory_space=pltpu.VMEM)
    hbm = pl.BlockSpec(memory_space=pltpu.HBM)
    dma = pltpu.SemaphoreType.DMA
    rows = sfts.reshape(SPAN, 2, 8, LANES).transpose(0, 2, 1, 3).reshape(SPAN * 16, LANES)
    out = pl.pallas_call(
        kernel,
        out_shape=pltpu.VMEM((LANES, 8 * LANES), bf16),
        in_specs=[hbm] * 5,
        out_specs=vmem,
        scratch_shapes=[
            pltpu.VMEM((SPAN * 16, LANES), f32),
            pltpu.VMEM((12, LANES), jnp.int32),
            pltpu.VMEM((2, LANES), jnp.int32),
            pltpu.SMEM((NDET, NDET), f32),
            pltpu.SMEM((NLAG,), jnp.int32),
            pltpu.VMEM((4, 1, LANES), f32),
            pltpu.VMEM((1, LANES), f32),
            pltpu.VMEM((TM, 1, LANES), f32),
            pltpu.VMEM((8, 2, LANES), jnp.int32),
            pltpu.VMEM((8, 2 * SPAN, LANES), bf16),
            pltpu.VMEM((TM, 2 * SPAN, LANES), bf16),
            pltpu.VMEM((8, LANES, LANES), bf16),
            pltpu.VMEM((8, LANES, LANES), bf16),
            pltpu.VMEM((ROWS, LANES), f32),
            pltpu.VMEM((ROWS, LANES), f32),
            pltpu.VMEM((ROWS, LANES), f32),
            pltpu.VMEM((NLAG, ROWS, LANES), f32),
            pltpu.VMEM((8, LANES), f32),
            pltpu.VMEM((8, LANES), f32),
            pltpu.VMEM((ZROWS, LANES), f32),
            pltpu.VMEM((ZROWS, LANES), f32),
            pltpu.VMEM((8, ZROWS, LANES), f32),
            pltpu.VMEM((8, ZROWS, LANES), f32),
            pltpu.VMEM((8, DEPTH, LANES), bf16),
            pltpu.VMEM((DEPTH, LANES), bf16),
            pltpu.VMEM((DEPTH // LANES, LANES, LANES), bf16),
            dma((5,)), dma((4,)), dma((4,)), dma((8,)), dma((8,)), dma((16,)), dma((TM,)), dma((16,)), dma((TM,)),
            dma((16,)), dma((16,)), dma((8,)), dma((8,)),
        ],
        compiler_params=pltpu.CompilerParams(
            collective_id=0, has_side_effects=True, vmem_limit_bytes=60 * 1024 * 1024),
    )(rows, detector_ids.reshape(12, LANES), template_ids.T, intersection, lags)
    return out.astype(f32)


def solution(mesh):
    in_specs = (P("tm", None, "freq"), P(), P(), P(), P("tm", None))
    out_specs = P("tm", "freq")
    return jax.shard_map(shards, mesh=mesh, in_specs=in_specs, out_specs=out_specs, check_vma=False)
```

```python
import functools
import math

import jax
import jax.numpy as jnp
from jax import lax
from jax.experimental import pallas as pl
from jax.experimental.pallas import tpu as pltpu
from jax.sharding import PartitionSpec as P

NSFT = 1536
NBIN = 4096
LAGMAX = 16
NLAG = 12
NDET = 3
NGRID = 64
PERIOD = 283
TM = 32
SPAN = 48
FOLD = 288
TURNS = 6
LANES = 128
ROWS = 1600
ZROWS = 320
DEPTH = 2 * NLAG * FOLD
PART = 1024
WIDE = 256
MESH = pl.DeviceIdType.MESH

COS = (0.9999999890590238, -19.739204499453965, 64.93911745989729, -85.45013953090921,
       60.167630951124465, -25.967599248993793, 6.528658161871135)
SIN = (6.28318527244795, -41.34169703820007, 81.60502363804078, -76.7015376703427,
       42.016075762415646, -14.86832275264805, 3.199338844584104)


def cos_sin(turns):
    u = turns - jnp.floor(turns + 0.5)
    t = u * u
    c = jnp.full_like(t, COS[-1])
    for k in COS[-2::-1]:
        c = c * t + k
    s = jnp.full_like(t, SIN[-1])
    for k in SIN[-2::-1]:
        s = s * t + k
    return c, s * u


def kernel(x_hbm, det_hbm, tid_hbm, inter_hbm, lag_hbm, o_ref,
           x_ref, det_ref, tid_ref, inter_ref, lag_ref, pbuf, gsend, gbuf, idbuf, send_buf, xrecv, osend, orecv,
           xre, xim, det, wl, amp_cos, amp_sin, orbit_cos, orbit_sin, zc, zs, fac, pairs, pairs_t,
           l_sem, p_send, p_recv, i_send, i_recv, g_send, g_recv, c_send, c_recv, fg_send, f_send, o_send, o_recv):
    tm = lax.axis_index("tm")
    h = lax.axis_index("freq")
    core, z_lo = h % 2, h // 2
    x = tm % 4
    f32, bf16 = jnp.float32, jnp.bfloat16

    quarter = (1 - z_lo) * 2 + x % 2
    group = 2 * (x // 2) + core

    def home(k, e):
        return 4 * k + core + 2 * e, (1 - z_lo) * 2 + x % 2

    def source(s):
        return 4 * (s // 2) + 2 * (s % 2) + core, quarter

    y = tm // 4 % 4

    def owner(p):
        return 4 * p + group, quarter

    def place(to):
        return tm // 4

    def remote(src, dst, send, recv, to):
        return pltpu.make_async_remote_copy(
            src_ref=src, dst_ref=dst, send_sem=send, recv_sem=recv, device_id=to, device_id_type=MESH)

    det_in = pltpu.make_async_copy(det_hbm, det_ref, l_sem.at[0])
    x_in = pltpu.make_async_copy(x_hbm, x_ref, l_sem.at[1])
    tid_in = pltpu.make_async_copy(tid_hbm, tid_ref, l_sem.at[2])
    inter_in = pltpu.make_async_copy(inter_hbm, inter_ref, l_sem.at[3])
    lag_in = pltpu.make_async_copy(lag_hbm, lag_ref, l_sem.at[4])
    x_in.start()
    det_in.start()
    inter_in.start()
    lag_in.start()
    tid_in.start()

    barrier = pltpu.get_barrier_semaphore()
    for k in range(8):
        for e in range(2):
            pl.semaphore_signal(barrier, inc=1, device_id=home(k, e), device_id_type=MESH)
    for s in range(16):
        pl.semaphore_signal(barrier, inc=1, device_id=source(s), device_id_type=MESH)
    for d in range(1, 4):
        pl.semaphore_signal(barrier, inc=1, device_id=(tm, (h + d) % 4), device_id_type=MESH)

    x_in.wait()
    part = jnp.zeros((SPAN, LANES), f32)
    for k in range(8):
        re = x_ref[pl.ds(2 * k, SPAN, stride=16), :]
        im = x_ref[pl.ds(2 * k + 1, SPAN, stride=16), :]
        part = part + (re * re + im * im)
        send_buf[k, 0:SPAN, :] = re.astype(bf16)
        send_buf[k, SPAN:, :] = im.astype(bf16)
    part = jnp.concatenate([part, jnp.zeros((LANES - SPAN, LANES), f32)], 0)
    pbuf[h] = jnp.sum(part.T, axis=0, keepdims=True)
    det_in.wait()
    inter_in.wait()
    lag_in.wait()
    det[NSFT:, :] = jnp.full((ROWS - NSFT, LANES), float(NDET), f32)
    for k in range(12):
        row = jnp.broadcast_to(det_ref[k:k + 1, :].astype(f32), (LANES, LANES))
        det[k * LANES:(k + 1) * LANES, :] = row.T

    def weight_rows(last, b, carry):
        at = pl.ds(pl.multiple_of(b * 16, 16), 16)
        d = det[at, :]
        with_far = [
            jnp.where(d == 0.0, inter_ref[0, e], jnp.where(d == 1.0, inter_ref[1, e], inter_ref[2, e]))
            for e in range(NDET)]
        for l in range(NLAG):
            far = det[pl.ds(b * 16 + lag_ref[l], 16), :]
            w = jnp.where(far == 0.0, with_far[0], jnp.where(far == 1.0, with_far[1], with_far[2]))
            wl[l, at, :] = jnp.where(far == float(NDET), 0.0, w) if last else w
        return carry

    whole = NSFT // 16 - 1
    lax.fori_loop(0, 40, functools.partial(weight_rows, False), 0)
    weight_rows(True, whole, 0)
    for l in range(NLAG):
        wl[l, NSFT:, :] = jnp.zeros((ROWS - NSFT, LANES), f32)
    xre[NSFT:, :] = jnp.zeros((ROWS - NSFT, LANES), f32)
    xim[NSFT:, :] = jnp.zeros((ROWS - NSFT, LANES), f32)

    def orbit_rows(b, carry):
        at = pl.ds(pl.multiple_of(b * 64, 64), 64)
        row = lax.broadcasted_iota(jnp.int32, (64, LANES), 0) + b * 64
        row = jnp.where(row >= PERIOD, row - PERIOD, row).astype(f32)
        orbit_cos[at, :], orbit_sin[at, :] = cos_sin(row * (1.0 / PERIOD))
        return carry

    lax.fori_loop(0, ZROWS // 64, orbit_rows, 0)

    tid_in.wait()

    pl.semaphore_wait(barrier, 35)

    power_copies = [
        remote(pbuf.at[h], pbuf.at[h], p_send.at[d], p_recv.at[4 - d], (tm, (h + d) % 4)) for d in range(1, 4)]
    id_copies = [
        remote(tid_ref, idbuf.at[place(home(k, x // 2))], i_send.at[k], i_recv.at[place(home(k, x // 2))], home(k, x // 2))
        for k in range(8)]
    chunk_copies = [
        remote(send_buf.at[k], xrecv.at[tm], c_send.at[2 * k + e], c_recv.at[tm], home(k, e))
        for e in range(2) for k in range(8)]
    for copy in power_copies + id_copies + chunk_copies[:12]:
        copy.start()

    for copy in power_copies:
        copy.wait()
    power = ((pbuf[0] + pbuf[1]) + (pbuf[2] + pbuf[3])) / NBIN
    gsend[...] = lax.rsqrt(power + 1e-06)
    scale_copies = [
        remote(gsend, gbuf.at[tm], g_send.at[2 * k + e], g_recv.at[tm], home(k, e))
        for k in range(8) for e in range(2)]
    for copy in scale_copies + chunk_copies[12:]:
        copy.start()
    lax.fori_loop(40, whole, functools.partial(weight_rows, False), 0)

    def factors(s):
        remote(tid_ref, idbuf.at[s], i_send.at[s], i_recv.at[s], owner(s)).wait_recv()
        ids = idbuf[s].astype(f32)
        amp = (8.0 + 4.0 * ids[0:1, :]) * (0.5 / math.pi)
        cq, sq_ = cos_sin(ids[1:2, :] * (1.0 / NGRID))
        amp_cos[...] = jnp.broadcast_to(amp * cq, (8, LANES))
        amp_sin[...] = jnp.broadcast_to(amp * sq_, (8, LANES))

        def z_rows(b, carry):
            at = pl.ds(pl.multiple_of(b * 64, 64), 64)
            turns = orbit_sin[at, :] * amp_cos[0:1, :] + orbit_cos[at, :] * amp_sin[0:1, :]
            zc[s, at, :], zs[s, at, :] = cos_sin(turns)
            return carry

        lax.fori_loop(0, ZROWS // 64, z_rows, 0)

        def factor_rows(b, carry):
            r0 = pl.multiple_of(b * 32, 32)
            ci, si = zc[s, pl.ds(r0, 32), :], zs[s, pl.ds(r0, 32), :]
            for l in range(NLAG):
                far = pl.ds(r0 + lag_ref[l], 32)
                cj, sj = zc[s, far, :], zs[s, far, :]
                out = pl.multiple_of(l * (2 * FOLD) + r0, 32)
                fac[s, pl.ds(out, 32), :] = (cj * ci + sj * si).astype(bf16)
                fac[s, pl.ds(out + FOLD, 32), :] = (sj * ci - cj * si).astype(bf16)
            return carry

        lax.fori_loop(0, FOLD // 32, factor_rows, 0)

    for s in (4, 5, 6, 7, 2, 3, 0):
        factors(s)

    other = (tm, h + 1 - 2 * core)
    forwards = []
    for s in range(16):
        slot = source(s)[0]
        remote(send_buf.at[0], xrecv.at[slot], c_send.at[s], c_recv.at[slot], source(s)).wait_recv()
        remote(gsend, gbuf.at[slot], g_send.at[s], g_recv.at[slot], source(s)).wait_recv()
        forwards.append(remote(xrecv.at[slot], xrecv.at[slot], f_send.at[s], c_recv.at[slot], other))
        forwards.append(remote(gbuf.at[slot], gbuf.at[slot], fg_send.at[s], g_recv.at[slot], other))
        forwards[-1].start()
        forwards[-2].start()
    factors(1)

    for s in range(16):
        slot = source(s)[0] + 1 - 2 * core
        remote(xrecv.at[slot], xrecv.at[slot], f_send.at[s], c_recv.at[slot], other).wait_recv()
        remote(gbuf.at[slot], gbuf.at[slot], fg_send.at[s], g_recv.at[slot], other).wait_recv()

    scales = gbuf[:, 0, :]
    scales = jnp.concatenate([scales, jnp.zeros((LANES - TM, LANES), f32)], 0).T[0:SPAN]
    for b in range(TM):
        g = jnp.broadcast_to(scales[:, b:b + 1], (SPAN, LANES))
        xre[b * SPAN:(b + 1) * SPAN, :] = xrecv[b, 0:SPAN, :].astype(f32) * g
        xim[b * SPAN:(b + 1) * SPAN, :] = xrecv[b, SPAN:, :].astype(f32) * g

    def pair_rows(turns, n, carry):
        b, part = n // 2, n % 2
        r0 = pl.multiple_of(b * 16, 16)
        lags = [lag_ref[6 * part + q] for q in range(6)]
        sums = [None] * 6
        for m in range(turns):
            here = pl.ds(r0 + PERIOD * m, 16)
            a, bb = xre[here, :], xim[here, :]
            for q in range(6):
                far = pl.ds(r0 + PERIOD * m + lags[q], 16)
                w = wl[6 * part + q, here, :]
                c, d = xre[far, :] * w, xim[far, :] * w
                new = [a * c + bb * d, a * d - bb * c]
                sums[q] = new if m == 0 else [v + w_ for v, w_ in zip(sums[q], new)]
        for q in range(6):
            out = pl.multiple_of((6 * part + q) * (2 * FOLD) + r0, 16)
            pairs[pl.ds(out, 16), :] = sums[q][0].astype(bf16)
            pairs[pl.ds(out + FOLD, 16), :] = sums[q][1].astype(bf16)
        return carry

    last = (NSFT - PERIOD * (TURNS - 1) + 15) // 16
    lax.fori_loop(0, last * 2, functools.partial(pair_rows, TURNS), 0)
    lax.fori_loop(last * 2, 18 * 2, functools.partial(pair_rows, TURNS - 1), 0)

    for l in range(2 * NLAG):
        pairs[l * FOLD + PERIOD:(l + 1) * FOLD, :] = jnp.zeros((FOLD - PERIOD, LANES), bf16)

    def turn(b, carry):
        for q in range(18):
            at = pl.ds(pl.multiple_of((b * 18 + q) * LANES, LANES), LANES)
            pairs_t[b * 18 + q] = pairs[at, :].T
        return carry

    lax.fori_loop(0, DEPTH // LANES // 18, turn, 0)

    scale = 1.0 / math.sqrt(NSFT * NLAG)

    def multiply(n, carry):
        b = n
        lhs = jnp.concatenate([pairs_t[k] for k in range(DEPTH // LANES)], 1)
        rhs = jnp.concatenate([fac[2 * b], fac[2 * b + 1]], 1)
        stat = jnp.dot(lhs, rhs, preferred_element_type=f32) * scale
        for q in range(2):
            s = 2 * b + q
            osend[s] = stat[:, q * LANES:(q + 1) * LANES].T.astype(bf16)
            remote(osend.at[s], orecv.at[tm // 4], o_send.at[s], o_recv.at[tm // 4], owner(s)).start()
        return carry

    lax.fori_loop(0, PART // WIDE, multiply, 0)

    for copy in id_copies + chunk_copies + scale_copies + forwards:
        copy.wait_send()

    for k in range(8):
        remote(osend.at[k], orecv.at[k], o_send.at[k], o_recv.at[k], home(k, x // 2)).wait_recv()
        o_ref[:, k * LANES:(k + 1) * LANES] = orecv[k]

    for s in range(8):
        remote(osend.at[s], orecv.at[tm // 4], o_send.at[s], o_recv.at[tm // 4], owner(s)).wait_send()


def shards(sfts, detector_ids, intersection, lags, template_ids):
    bf16, f32 = jnp.bfloat16, jnp.float32
    vmem = pl.BlockSpec(memory_space=pltpu.VMEM)
    hbm = pl.BlockSpec(memory_space=pltpu.HBM)
    dma = pltpu.SemaphoreType.DMA
    rows = sfts.reshape(SPAN, 2, 8, LANES).transpose(0, 2, 1, 3).reshape(SPAN * 16, LANES)
    out = pl.pallas_call(
        kernel,
        out_shape=pltpu.VMEM((LANES, 8 * LANES), bf16),
        in_specs=[hbm] * 5,
        out_specs=vmem,
        scratch_shapes=[
            pltpu.VMEM((SPAN * 16, LANES), f32),
            pltpu.VMEM((12, LANES), jnp.int32),
            pltpu.VMEM((2, LANES), jnp.int32),
            pltpu.SMEM((NDET, NDET), f32),
            pltpu.SMEM((NLAG,), jnp.int32),
            pltpu.VMEM((4, 1, LANES), f32),
            pltpu.VMEM((1, LANES), f32),
            pltpu.VMEM((TM, 1, LANES), f32),
            pltpu.VMEM((8, 2, LANES), jnp.int32),
            pltpu.VMEM((8, 2 * SPAN, LANES), bf16),
            pltpu.VMEM((TM, 2 * SPAN, LANES), bf16),
            pltpu.VMEM((8, LANES, LANES), bf16),
            pltpu.VMEM((8, LANES, LANES), bf16),
            pltpu.VMEM((ROWS, LANES), f32),
            pltpu.VMEM((ROWS, LANES), f32),
            pltpu.VMEM((ROWS, LANES), f32),
            pltpu.VMEM((NLAG, ROWS, LANES), f32),
            pltpu.VMEM((8, LANES), f32),
            pltpu.VMEM((8, LANES), f32),
            pltpu.VMEM((ZROWS, LANES), f32),
            pltpu.VMEM((ZROWS, LANES), f32),
            pltpu.VMEM((8, ZROWS, LANES), f32),
            pltpu.VMEM((8, ZROWS, LANES), f32),
            pltpu.VMEM((8, DEPTH, LANES), bf16),
            pltpu.VMEM((DEPTH, LANES), bf16),
            pltpu.VMEM((DEPTH // LANES, LANES, LANES), bf16),
            dma((5,)), dma((4,)), dma((4,)), dma((8,)), dma((8,)), dma((16,)), dma((TM,)), dma((16,)), dma((TM,)),
            dma((16,)), dma((16,)), dma((8,)), dma((8,)),
        ],
        compiler_params=pltpu.CompilerParams(
            collective_id=0, has_side_effects=True, vmem_limit_bytes=60 * 1024 * 1024),
    )(rows, detector_ids.reshape(12, LANES), template_ids.T, intersection, lags)
    return out.astype(f32)


def solution(mesh):
    in_specs = (P("tm", None, "freq"), P(), P(), P(), P("tm", None))
    out_specs = P("tm", "freq")
    return jax.shard_map(shards, mesh=mesh, in_specs=in_specs, out_specs=out_specs, check_vma=False)
```

```python
import functools
import math

import jax
import jax.numpy as jnp
from jax import lax
from jax.experimental import pallas as pl
from jax.experimental.pallas import tpu as pltpu
from jax.sharding import PartitionSpec as P

NSFT = 1536
NBIN = 4096
LAGMAX = 16
NLAG = 12
NDET = 3
NGRID = 64
PERIOD = 283
TM = 32
SPAN = 48
FOLD = 288
TURNS = 6
LANES = 128
ROWS = 1600
ZROWS = 304
DEPTH = 2 * NLAG * FOLD
PART = 1024
WIDE = 256
MESH = pl.DeviceIdType.MESH

COS = (0.9999999890590238, -19.739204499453965, 64.93911745989729, -85.45013953090921,
       60.167630951124465, -25.967599248993793, 6.528658161871135)
SIN = (6.28318527244795, -41.34169703820007, 81.60502363804078, -76.7015376703427,
       42.016075762415646, -14.86832275264805, 3.199338844584104)


def cos_sin(turns):
    u = turns - jnp.round(turns)
    t = u * u
    c = jnp.full_like(t, COS[-1])
    for k in COS[-2::-1]:
        c = c * t + k
    s = jnp.full_like(t, SIN[-1])
    for k in SIN[-2::-1]:
        s = s * t + k
    return c, s * u


def kernel(x_hbm, det_hbm, tid_hbm, inter_hbm, lag_hbm, o_ref,
           x_ref, det_ref, tid_ref, inter_ref, lag_ref, pbuf, gsend, gbuf, idbuf, send_buf, xrecv, osend, orecv,
           xre, xim, det, wl, amp_cos, amp_sin, orbit_cos, orbit_sin, zc, zs, fac, pairs, pairs_t, scales,
           l_sem, p_send, p_recv, i_send, i_recv, g_send, g_recv, c_send, c_recv, fg_send, f_send, o_send, o_recv):
    tm = lax.axis_index("tm")
    h = lax.axis_index("freq")
    core, z_lo = h % 2, h // 2
    x = tm % 4
    f32, bf16 = jnp.float32, jnp.bfloat16

    quarter = (1 - z_lo) * 2 + x % 2
    group = 2 * (x // 2) + core

    def home(k, e):
        return 4 * k + core + 2 * e, (1 - z_lo) * 2 + x % 2

    def source(s):
        return 4 * (s // 2) + 2 * (s % 2) + core, quarter

    y = tm // 4 % 4

    def owner(p):
        return 4 * p + group, quarter

    def place(to):
        return tm // 4

    def remote(src, dst, send, recv, to):
        return pltpu.make_async_remote_copy(
            src_ref=src, dst_ref=dst, send_sem=send, recv_sem=recv, device_id=to, device_id_type=MESH)

    det_in = pltpu.make_async_copy(det_hbm, det_ref, l_sem.at[0])
    x_in = pltpu.make_async_copy(x_hbm, x_ref, l_sem.at[1])
    tid_in = pltpu.make_async_copy(tid_hbm, tid_ref, l_sem.at[2])
    inter_in = pltpu.make_async_copy(inter_hbm, inter_ref, l_sem.at[3])
    lag_in = pltpu.make_async_copy(lag_hbm, lag_ref, l_sem.at[4])
    x_in.start()
    det_in.start()
    inter_in.start()
    lag_in.start()
    tid_in.start()

    barrier = pltpu.get_barrier_semaphore()
    for k in range(8):
        for e in range(2):
            pl.semaphore_signal(barrier, inc=1, device_id=home(k, e), device_id_type=MESH)
    for s in range(16):
        pl.semaphore_signal(barrier, inc=1, device_id=source(s), device_id_type=MESH)
    for d in range(1, 4):
        pl.semaphore_signal(barrier, inc=1, device_id=(tm, (h + d) % 4), device_id_type=MESH)

    x_in.wait()
    part = jnp.zeros((SPAN, LANES), f32)
    for k in range(8):
        re = x_ref[pl.ds(2 * k, SPAN, stride=16), :]
        im = x_ref[pl.ds(2 * k + 1, SPAN, stride=16), :]
        part = part + (re * re + im * im)
        send_buf[k, 0:SPAN, :] = re.astype(bf16)
        send_buf[k, SPAN:, :] = im.astype(bf16)
    part = jnp.concatenate([part, jnp.zeros((LANES - SPAN, LANES), f32)], 0)
    pbuf[h] = jnp.sum(part.T, axis=0, keepdims=True)
    det_in.wait()
    inter_in.wait()
    lag_in.wait()
    det[NSFT:, :] = jnp.full((ROWS - NSFT, LANES), float(NDET), f32)
    for k in range(12):
        row = jnp.broadcast_to(det_ref[k:k + 1, :].astype(f32), (LANES, LANES))
        det[k * LANES:(k + 1) * LANES, :] = row.T

    def weight_rows(last, b, carry):
        at = pl.ds(pl.multiple_of(b * 16, 16), 16)
        d = det[at, :]
        with_far = [
            jnp.where(d == 0.0, inter_ref[0, e], jnp.where(d == 1.0, inter_ref[1, e], inter_ref[2, e]))
            for e in range(NDET)]
        for l in range(NLAG):
            far = det[pl.ds(b * 16 + lag_ref[l], 16), :]
            w = jnp.where(far == 0.0, with_far[0], jnp.where(far == 1.0, with_far[1], with_far[2]))
            wl[l, at, :] = jnp.where(far == float(NDET), 0.0, w) if last else w
        return carry

    whole = NSFT // 16 - 1
    lax.fori_loop(0, 40, functools.partial(weight_rows, False), 0)
    weight_rows(True, whole, 0)
    for l in range(NLAG):
        wl[l, NSFT:, :] = jnp.zeros((ROWS - NSFT, LANES), f32)
    xre[NSFT:, :] = jnp.zeros((ROWS - NSFT, LANES), f32)
    xim[NSFT:, :] = jnp.zeros((ROWS - NSFT, LANES), f32)

    def orbit_rows(b, carry):
        at = pl.ds(pl.multiple_of(b * 152, 8), 152)
        row = lax.broadcasted_iota(jnp.int32, (152, LANES), 0) + b * 152
        row = jnp.where(row >= PERIOD, row - PERIOD, row).astype(f32)
        orbit_cos[at, :], orbit_sin[at, :] = cos_sin(row * (1.0 / PERIOD))
        return carry

    lax.fori_loop(0, ZROWS // 152, orbit_rows, 0)

    tid_in.wait()

    pl.semaphore_wait(barrier, 35)

    power_copies = [
        remote(pbuf.at[h], pbuf.at[h], p_send.at[d], p_recv.at[4 - d], (tm, (h + d) % 4)) for d in range(1, 4)]
    id_copies = [
        remote(tid_ref, idbuf.at[place(home(k, x // 2))], i_send.at[k], i_recv.at[place(home(k, x // 2))], home(k, x // 2))
        for k in range(8)]
    chunk_copies = [
        remote(send_buf.at[k], xrecv.at[tm], c_send.at[2 * k + e], c_recv.at[tm], home(k, e))
        for e in range(2) for k in range(8)]
    for copy in power_copies + id_copies + chunk_copies[:12]:
        copy.start()

    for copy in power_copies:
        copy.wait()
    power = ((pbuf[0] + pbuf[1]) + (pbuf[2] + pbuf[3])) / NBIN
    gsend[...] = lax.rsqrt(power + 1e-06)
    scale_copies = [
        remote(gsend, gbuf.at[tm], g_send.at[2 * k + e], g_recv.at[tm], home(k, e))
        for k in range(8) for e in range(2)]
    for copy in scale_copies + chunk_copies[12:]:
        copy.start()
    lax.fori_loop(40, whole, functools.partial(weight_rows, False), 0)

    def factors(s):
        remote(tid_ref, idbuf.at[s], i_send.at[s], i_recv.at[s], owner(s)).wait_recv()
        ids = idbuf[s].astype(f32)
        amp = (8.0 + 4.0 * ids[0:1, :]) * (0.5 / math.pi)
        cq, sq_ = cos_sin(ids[1:2, :] * (1.0 / NGRID))
        amp_cos[...] = jnp.broadcast_to(amp * cq, (8, LANES))
        amp_sin[...] = jnp.broadcast_to(amp * sq_, (8, LANES))

        def z_rows(b, carry):
            at = pl.ds(pl.multiple_of(b * 152, 8), 152)
            turns = orbit_sin[at, :] * amp_cos[0:1, :] + orbit_cos[at, :] * amp_sin[0:1, :]
            zc[s, at, :], zs[s, at, :] = cos_sin(turns)
            return carry

        lax.fori_loop(0, ZROWS // 152, z_rows, 0)

        def factor_rows(b, carry):
            r0 = pl.multiple_of(b * 32, 32)
            ci, si = zc[s, pl.ds(r0, 32), :], zs[s, pl.ds(r0, 32), :]
            for l in range(NLAG):
                far = pl.ds(r0 + lag_ref[l], 32)
                cj, sj = zc[s, far, :], zs[s, far, :]
                out = pl.multiple_of(l * (2 * FOLD) + r0, 32)
                fac[s, pl.ds(out, 32), :] = (cj * ci + sj * si).astype(bf16)
                fac[s, pl.ds(out + FOLD, 32), :] = (sj * ci - cj * si).astype(bf16)
            return carry

        lax.fori_loop(0, FOLD // 32, factor_rows, 0)

    for s in (4, 5, 6, 7, 2, 3, 0):
        factors(s)

    other = (tm, h + 1 - 2 * core)
    forwards = []
    for s in range(16):
        slot = source(s)[0]
        remote(send_buf.at[0], xrecv.at[slot], c_send.at[s], c_recv.at[slot], source(s)).wait_recv()
        remote(gsend, gbuf.at[slot], g_send.at[s], g_recv.at[slot], source(s)).wait_recv()
        forwards.append(remote(xrecv.at[slot], xrecv.at[slot], f_send.at[s], c_recv.at[slot], other))
        forwards.append(remote(gbuf.at[slot], gbuf.at[slot], fg_send.at[s], g_recv.at[slot], other))
        forwards[-1].start()
        forwards[-2].start()
    factors(1)

    def unpack(slots):
        for s, slot in enumerate(slots):
            scales[s:s + 1, :] = gbuf[slot]
        columns = jnp.concatenate([scales[...], jnp.zeros((LANES - 16, LANES), f32)], 0).T[0:SPAN]
        for s, slot in enumerate(slots):
            g = jnp.broadcast_to(columns[:, s:s + 1], (SPAN, LANES))
            at = pl.ds(pl.multiple_of(slot * SPAN, 16), SPAN)
            xre[at, :] = xrecv[slot, 0:SPAN, :].astype(f32) * g
            xim[at, :] = xrecv[slot, SPAN:, :].astype(f32) * g

    unpack([source(s)[0] for s in range(16)])
    there = [source(s)[0] + 1 - 2 * core for s in range(16)]
    for s, slot in enumerate(there):
        remote(xrecv.at[slot], xrecv.at[slot], f_send.at[s], c_recv.at[slot], other).wait_recv()
        remote(gbuf.at[slot], gbuf.at[slot], fg_send.at[s], g_recv.at[slot], other).wait_recv()
    unpack(there)

    def pair_rows(turns, n, carry):
        b, part = n // 2, n % 2
        r0 = pl.multiple_of(b * 16, 16)
        lags = [lag_ref[6 * part + q] for q in range(6)]
        sums = [None] * 6
        for m in range(turns):
            here = pl.ds(r0 + PERIOD * m, 16)
            a, bb = xre[here, :], xim[here, :]
            for q in range(6):
                far = pl.ds(r0 + PERIOD * m + lags[q], 16)
                w = wl[6 * part + q, here, :]
                c, d = xre[far, :] * w, xim[far, :] * w
                new = [a * c + bb * d, a * d - bb * c]
                sums[q] = new if m == 0 else [v + w_ for v, w_ in zip(sums[q], new)]
        for q in range(6):
            out = pl.multiple_of((6 * part + q) * (2 * FOLD) + r0, 16)
            pairs[pl.ds(out, 16), :] = sums[q][0].astype(bf16)
            pairs[pl.ds(out + FOLD, 16), :] = sums[q][1].astype(bf16)
        return carry

    last = (NSFT - PERIOD * (TURNS - 1) + 15) // 16
    lax.fori_loop(0, last * 2, functools.partial(pair_rows, TURNS), 0)
    lax.fori_loop(last * 2, 18 * 2, functools.partial(pair_rows, TURNS - 1), 0)

    for l in range(2 * NLAG):
        pairs[l * FOLD + PERIOD:(l + 1) * FOLD, :] = jnp.zeros((FOLD - PERIOD, LANES), bf16)

    def turn(b, carry):
        for q in range(18):
            at = pl.ds(pl.multiple_of((b * 18 + q) * LANES, LANES), LANES)
            pairs_t[b * 18 + q] = pairs[at, :].T
        return carry

    lax.fori_loop(0, DEPTH // LANES // 18, turn, 0)

    scale = 1.0 / math.sqrt(NSFT * NLAG)

    def multiply(n, carry):
        b = n
        lhs = jnp.concatenate([pairs_t[k] for k in range(DEPTH // LANES)], 1)
        rhs = jnp.concatenate([fac[2 * b], fac[2 * b + 1]], 1)
        stat = jnp.dot(lhs, rhs, preferred_element_type=f32) * scale
        for q in range(2):
            s = 2 * b + q
            osend[s] = stat[:, q * LANES:(q + 1) * LANES].T.astype(bf16)
            remote(osend.at[s], orecv.at[tm // 4], o_send.at[s], o_recv.at[tm // 4], owner(s)).start()
        return carry

    lax.fori_loop(0, PART // WIDE, multiply, 0)

    for copy in id_copies + chunk_copies + scale_copies + forwards:
        copy.wait_send()

    for k in range(8):
        remote(osend.at[k], orecv.at[k], o_send.at[k], o_recv.at[k], home(k, x // 2)).wait_recv()
        o_ref[:, k * LANES:(k + 1) * LANES] = orecv[k]

    for s in range(8):
        remote(osend.at[s], orecv.at[tm // 4], o_send.at[s], o_recv.at[tm // 4], owner(s)).wait_send()


def shards(sfts, detector_ids, intersection, lags, template_ids):
    bf16, f32 = jnp.bfloat16, jnp.float32
    vmem = pl.BlockSpec(memory_space=pltpu.VMEM)
    hbm = pl.BlockSpec(memory_space=pltpu.HBM)
    dma = pltpu.SemaphoreType.DMA
    rows = sfts.reshape(SPAN, 2, 8, LANES).transpose(0, 2, 1, 3).reshape(SPAN * 16, LANES)
    out = pl.pallas_call(
        kernel,
        out_shape=pltpu.VMEM((LANES, 8 * LANES), bf16),
        in_specs=[hbm] * 5,
        out_specs=vmem,
        scratch_shapes=[
            pltpu.VMEM((SPAN * 16, LANES), f32),
            pltpu.VMEM((12, LANES), jnp.int32),
            pltpu.VMEM((2, LANES), jnp.int32),
            pltpu.SMEM((NDET, NDET), f32),
            pltpu.SMEM((NLAG,), jnp.int32),
            pltpu.VMEM((4, 1, LANES), f32),
            pltpu.VMEM((1, LANES), f32),
            pltpu.VMEM((TM, 1, LANES), f32),
            pltpu.VMEM((8, 2, LANES), jnp.int32),
            pltpu.VMEM((8, 2 * SPAN, LANES), bf16),
            pltpu.VMEM((TM, 2 * SPAN, LANES), bf16),
            pltpu.VMEM((8, LANES, LANES), bf16),
            pltpu.VMEM((8, LANES, LANES), bf16),
            pltpu.VMEM((ROWS, LANES), f32),
            pltpu.VMEM((ROWS, LANES), f32),
            pltpu.VMEM((ROWS, LANES), f32),
            pltpu.VMEM((NLAG, ROWS, LANES), f32),
            pltpu.VMEM((8, LANES), f32),
            pltpu.VMEM((8, LANES), f32),
            pltpu.VMEM((ZROWS, LANES), f32),
            pltpu.VMEM((ZROWS, LANES), f32),
            pltpu.VMEM((8, ZROWS, LANES), f32),
            pltpu.VMEM((8, ZROWS, LANES), f32),
            pltpu.VMEM((8, DEPTH, LANES), bf16),
            pltpu.VMEM((DEPTH, LANES), bf16),
            pltpu.VMEM((DEPTH // LANES, LANES, LANES), bf16),
            pltpu.VMEM((16, LANES), f32),
            dma((5,)), dma((4,)), dma((4,)), dma((8,)), dma((8,)), dma((16,)), dma((TM,)), dma((16,)), dma((TM,)),
            dma((16,)), dma((16,)), dma((8,)), dma((8,)),
        ],
        compiler_params=pltpu.CompilerParams(
            collective_id=0, has_side_effects=True, vmem_limit_bytes=60 * 1024 * 1024),
    )(rows, detector_ids.reshape(12, LANES), template_ids.T, intersection, lags)
    return out.astype(f32)


def solution(mesh):
    in_specs = (P("tm", None, "freq"), P(), P(), P(), P("tm", None))
    out_specs = P("tm", "freq")
    return jax.shard_map(shards, mesh=mesh, in_specs=in_specs, out_specs=out_specs, check_vma=False)
```

```python
import functools
import math

import jax
import jax.numpy as jnp
from jax import lax
from jax.experimental import pallas as pl
from jax.experimental.pallas import tpu as pltpu
from jax.sharding import PartitionSpec as P

NSFT = 1536
NBIN = 4096
LAGMAX = 16
NLAG = 12
NDET = 3
NGRID = 64
PERIOD = 283
TM = 32
SPAN = 48
FOLD = 288
TURNS = 6
LANES = 128
ROWS = 1600
ZROWS = 320
DEPTH = 2 * NLAG * FOLD
PART = 1024
WIDE = 256
MESH = pl.DeviceIdType.MESH

COS = (0.9999999890590238, -19.739204499453965, 64.93911745989729, -85.45013953090921,
       60.167630951124465, -25.967599248993793, 6.528658161871135)
SIN = (6.28318527244795, -41.34169703820007, 81.60502363804078, -76.7015376703427,
       42.016075762415646, -14.86832275264805, 3.199338844584104)


def cos_sin(turns):
    u = turns - jnp.floor(turns + 0.5)
    t = u * u
    c = jnp.full_like(t, COS[-1])
    for k in COS[-2::-1]:
        c = c * t + k
    s = jnp.full_like(t, SIN[-1])
    for k in SIN[-2::-1]:
        s = s * t + k
    return c, s * u


def kernel(x_hbm, det_hbm, tid_hbm, inter_hbm, lag_hbm, o_ref,
           x_ref, det_ref, tid_ref, inter_ref, lag_ref, pbuf, gsend, gbuf, idbuf, send_buf, xrecv, osend, orecv,
           xre, xim, det, wl, amp_cos, amp_sin, orbit_cos, orbit_sin, zc, zs, fac, pairs, pairs_t,
           l_sem, p_send, p_recv, i_send, i_recv, g_send, g_recv, c_send, c_recv, fg_send, f_send, o_send, o_recv):
    tm = lax.axis_index("tm")
    h = lax.axis_index("freq")
    core, z_lo = h % 2, h // 2
    x = tm % 4
    f32, bf16 = jnp.float32, jnp.bfloat16

    quarter = (1 - z_lo) * 2 + x % 2
    group = 2 * (x // 2) + core

    def home(k, e):
        return 4 * k + core + 2 * e, (1 - z_lo) * 2 + x % 2

    def source(s):
        return 4 * (s // 2) + 2 * (s % 2) + core, quarter

    y = tm // 4 % 4

    def owner(p):
        return 4 * p + group, quarter

    def place(to):
        return tm // 4

    def remote(src, dst, send, recv, to):
        return pltpu.make_async_remote_copy(
            src_ref=src, dst_ref=dst, send_sem=send, recv_sem=recv, device_id=to, device_id_type=MESH)

    det_in = pltpu.make_async_copy(det_hbm, det_ref, l_sem.at[0])
    x_in = pltpu.make_async_copy(x_hbm, x_ref, l_sem.at[1])
    tid_in = pltpu.make_async_copy(tid_hbm, tid_ref, l_sem.at[2])
    inter_in = pltpu.make_async_copy(inter_hbm, inter_ref, l_sem.at[3])
    lag_in = pltpu.make_async_copy(lag_hbm, lag_ref, l_sem.at[4])
    x_in.start()
    det_in.start()
    inter_in.start()
    lag_in.start()
    tid_in.start()

    barrier = pltpu.get_barrier_semaphore()
    for k in range(8):
        for e in range(2):
            pl.semaphore_signal(barrier, inc=1, device_id=home(k, e), device_id_type=MESH)
    for s in range(16):
        pl.semaphore_signal(barrier, inc=1, device_id=source(s), device_id_type=MESH)
    for d in range(1, 4):
        pl.semaphore_signal(barrier, inc=1, device_id=(tm, (h + d) % 4), device_id_type=MESH)

    x_in.wait()
    part = jnp.zeros((SPAN, LANES), f32)
    for k in range(8):
        re = x_ref[pl.ds(2 * k, SPAN, stride=16), :]
        im = x_ref[pl.ds(2 * k + 1, SPAN, stride=16), :]
        part = part + (re * re + im * im)
        send_buf[k, 0:SPAN, :] = re.astype(bf16)
        send_buf[k, SPAN:, :] = im.astype(bf16)
    part = jnp.concatenate([part, jnp.zeros((LANES - SPAN, LANES), f32)], 0)
    pbuf[h] = jnp.sum(part.T, axis=0, keepdims=True)
    det_in.wait()
    inter_in.wait()
    lag_in.wait()
    det[NSFT:, :] = jnp.full((ROWS - NSFT, LANES), float(NDET), f32)
    for k in range(12):
        row = jnp.broadcast_to(det_ref[k:k + 1, :].astype(f32), (LANES, LANES))
        det[k * LANES:(k + 1) * LANES, :] = row.T

    def weight_rows(last, b, carry):
        at = pl.ds(pl.multiple_of(b * 16, 16), 16)
        d = det[at, :]
        with_far = [
            jnp.where(d == 0.0, inter_ref[0, e], jnp.where(d == 1.0, inter_ref[1, e], inter_ref[2, e]))
            for e in range(NDET)]
        for l in range(NLAG):
            far = det[pl.ds(b * 16 + lag_ref[l], 16), :]
            w = jnp.where(far == 0.0, with_far[0], jnp.where(far == 1.0, with_far[1], with_far[2]))
            wl[l, at, :] = jnp.where(far == float(NDET), 0.0, w) if last else w
        return carry

    whole = NSFT // 16 - 1
    lax.fori_loop(0, 40, functools.partial(weight_rows, False), 0)
    weight_rows(True, whole, 0)
    for l in range(NLAG):
        wl[l, NSFT:, :] = jnp.zeros((ROWS - NSFT, LANES), f32)
    xre[NSFT:, :] = jnp.zeros((ROWS - NSFT, LANES), f32)
    xim[NSFT:, :] = jnp.zeros((ROWS - NSFT, LANES), f32)

    def orbit_rows(b, carry):
        at = pl.ds(pl.multiple_of(b * 64, 64), 64)
        row = lax.broadcasted_iota(jnp.int32, (64, LANES), 0) + b * 64
        row = jnp.where(row >= PERIOD, row - PERIOD, row).astype(f32)
        orbit_cos[at, :], orbit_sin[at, :] = cos_sin(row * (1.0 / PERIOD))
        return carry

    lax.fori_loop(0, ZROWS // 64, orbit_rows, 0)

    tid_in.wait()

    pl.semaphore_wait(barrier, 35)

    power_copies = [
        remote(pbuf.at[h], pbuf.at[h], p_send.at[d], p_recv.at[4 - d], (tm, (h + d) % 4)) for d in range(1, 4)]
    id_copies = [
        remote(tid_ref, idbuf.at[place(home(k, x // 2))], i_send.at[k], i_recv.at[place(home(k, x // 2))], home(k, x // 2))
        for k in range(8)]
    chunk_copies = [
        remote(send_buf.at[k], xrecv.at[tm], c_send.at[2 * k + e], c_recv.at[tm], home(k, e))
        for e in range(2) for k in range(8)]
    for copy in power_copies + id_copies + chunk_copies[:12]:
        copy.start()

    for copy in power_copies:
        copy.wait()
    power = ((pbuf[0] + pbuf[1]) + (pbuf[2] + pbuf[3])) / NBIN
    gsend[...] = lax.rsqrt(power + 1e-06)
    scale_copies = [
        remote(gsend, gbuf.at[tm], g_send.at[2 * k + e], g_recv.at[tm], home(k, e))
        for k in range(8) for e in range(2)]
    for copy in scale_copies + chunk_copies[12:]:
        copy.start()
    lax.fori_loop(40, whole, functools.partial(weight_rows, False), 0)

    def factors(s):
        remote(tid_ref, idbuf.at[s], i_send.at[s], i_recv.at[s], owner(s)).wait_recv()
        ids = idbuf[s].astype(f32)
        amp = (8.0 + 4.0 * ids[0:1, :]) * (0.5 / math.pi)
        cq, sq_ = cos_sin(ids[1:2, :] * (1.0 / NGRID))
        amp_cos[...] = jnp.broadcast_to(amp * cq, (8, LANES))
        amp_sin[...] = jnp.broadcast_to(amp * sq_, (8, LANES))

        def z_rows(b, carry):
            at = pl.ds(pl.multiple_of(b * 64, 64), 64)
            turns = orbit_sin[at, :] * amp_cos[0:1, :] + orbit_cos[at, :] * amp_sin[0:1, :]
            zc[s, at, :], zs[s, at, :] = cos_sin(turns)
            return carry

        lax.fori_loop(0, ZROWS // 64, z_rows, 0)

        def factor_rows(b, carry):
            r0 = pl.multiple_of(b * 32, 32)
            ci, si = zc[s, pl.ds(r0, 32), :], zs[s, pl.ds(r0, 32), :]
            for l in range(NLAG):
                far = pl.ds(r0 + lag_ref[l], 32)
                cj, sj = zc[s, far, :], zs[s, far, :]
                out = pl.multiple_of(l * (2 * FOLD) + r0, 32)
                fac[s, pl.ds(out, 32), :] = (cj * ci + sj * si).astype(bf16)
                fac[s, pl.ds(out + FOLD, 32), :] = (sj * ci - cj * si).astype(bf16)
            return carry

        lax.fori_loop(0, FOLD // 32, factor_rows, 0)

    for s in (4, 5, 6, 7, 2, 3, 0):
        factors(s)

    other = (tm, h + 1 - 2 * core)
    forwards = []
    for s in range(16):
        slot = source(s)[0]
        remote(send_buf.at[0], xrecv.at[slot], c_send.at[s], c_recv.at[slot], source(s)).wait_recv()
        remote(gsend, gbuf.at[slot], g_send.at[s], g_recv.at[slot], source(s)).wait_recv()
        forwards.append(remote(xrecv.at[slot], xrecv.at[slot], f_send.at[s], c_recv.at[slot], other))
        forwards.append(remote(gbuf.at[slot], gbuf.at[slot], fg_send.at[s], g_recv.at[slot], other))
        forwards[-1].start()
        forwards[-2].start()
    factors(1)

    for s in range(16):
        slot = source(s)[0] + 1 - 2 * core
        remote(xrecv.at[slot], xrecv.at[slot], f_send.at[s], c_recv.at[slot], other).wait_recv()
        remote(gbuf.at[slot], gbuf.at[slot], fg_send.at[s], g_recv.at[slot], other).wait_recv()

    scales = gbuf[:, 0, :]
    scales = jnp.concatenate([scales, jnp.zeros((LANES - TM, LANES), f32)], 0).T[0:SPAN]
    for b in range(TM):
        g = jnp.broadcast_to(scales[:, b:b + 1], (SPAN, LANES))
        xre[b * SPAN:(b + 1) * SPAN, :] = xrecv[b, 0:SPAN, :].astype(f32) * g
        xim[b * SPAN:(b + 1) * SPAN, :] = xrecv[b, SPAN:, :].astype(f32) * g

    def pair_rows(turns, n, carry):
        b, part = n // 2, n % 2
        r0 = pl.multiple_of(b * 16, 16)
        lags = [lag_ref[6 * part + q] for q in range(6)]
        sums = [None] * 6
        for m in range(turns):
            here = pl.ds(r0 + PERIOD * m, 16)
            a, bb = xre[here, :], xim[here, :]
            for q in range(6):
                far = pl.ds(r0 + PERIOD * m + lags[q], 16)
                w = wl[6 * part + q, here, :]
                c, d = xre[far, :] * w, xim[far, :] * w
                new = [a * c + bb * d, a * d - bb * c]
                sums[q] = new if m == 0 else [v + w_ for v, w_ in zip(sums[q], new)]
        for q in range(6):
            out = pl.multiple_of((6 * part + q) * (2 * FOLD) + r0, 16)
            pairs[pl.ds(out, 16), :] = sums[q][0].astype(bf16)
            pairs[pl.ds(out + FOLD, 16), :] = sums[q][1].astype(bf16)
        return carry

    last = (NSFT - PERIOD * (TURNS - 1) + 15) // 16
    lax.fori_loop(0, last * 2, functools.partial(pair_rows, TURNS), 0)
    lax.fori_loop(last * 2, 18 * 2, functools.partial(pair_rows, TURNS - 1), 0)

    for l in range(2 * NLAG):
        pairs[l * FOLD + PERIOD:(l + 1) * FOLD, :] = jnp.zeros((FOLD - PERIOD, LANES), bf16)

    def turn(b, carry):
        for q in range(18):
            at = pl.ds(pl.multiple_of((b * 18 + q) * LANES, LANES), LANES)
            pairs_t[b * 18 + q] = pairs[at, :].T
        return carry

    lax.fori_loop(0, DEPTH // LANES // 18, turn, 0)

    scale = 1.0 / math.sqrt(NSFT * NLAG)

    def multiply(n, carry):
        b = n
        lhs = jnp.concatenate([pairs_t[k] for k in range(DEPTH // LANES)], 1)
        rhs = jnp.concatenate([fac[2 * b, 0:DEPTH, :], fac[2 * b + 1, 0:DEPTH, :]], 1)
        stat = jnp.dot(lhs, rhs, preferred_element_type=f32) * scale
        for q in range(2):
            s = 2 * b + q
            osend[s] = stat[:, q * LANES:(q + 1) * LANES].T.astype(bf16)
            remote(osend.at[s], orecv.at[tm // 4], o_send.at[s], o_recv.at[tm // 4], owner(s)).start()
        return carry

    lax.fori_loop(0, PART // WIDE, multiply, 0)

    for copy in id_copies + chunk_copies + scale_copies + forwards:
        copy.wait_send()

    for k in range(8):
        remote(osend.at[k], orecv.at[k], o_send.at[k], o_recv.at[k], home(k, x // 2)).wait_recv()
        o_ref[:, k * LANES:(k + 1) * LANES] = orecv[k]

    for s in range(8):
        remote(osend.at[s], orecv.at[tm // 4], o_send.at[s], o_recv.at[tm // 4], owner(s)).wait_send()


def shards(sfts, detector_ids, intersection, lags, template_ids):
    bf16, f32 = jnp.bfloat16, jnp.float32
    vmem = pl.BlockSpec(memory_space=pltpu.VMEM)
    hbm = pl.BlockSpec(memory_space=pltpu.HBM)
    dma = pltpu.SemaphoreType.DMA
    rows = sfts.reshape(SPAN, 2, 8, LANES).transpose(0, 2, 1, 3).reshape(SPAN * 16, LANES)
    out = pl.pallas_call(
        kernel,
        out_shape=pltpu.VMEM((LANES, 8 * LANES), bf16),
        in_specs=[hbm] * 5,
        out_specs=vmem,
        scratch_shapes=[
            pltpu.VMEM((SPAN * 16, LANES), f32),
            pltpu.VMEM((12, LANES), jnp.int32),
            pltpu.VMEM((2, LANES), jnp.int32),
            pltpu.SMEM((NDET, NDET), f32),
            pltpu.SMEM((NLAG,), jnp.int32),
            pltpu.VMEM((4, 1, LANES), f32),
            pltpu.VMEM((1, LANES), f32),
            pltpu.VMEM((TM, 1, LANES), f32),
            pltpu.VMEM((8, 2, LANES), jnp.int32),
            pltpu.VMEM((8, 2 * SPAN, LANES), bf16),
            pltpu.VMEM((TM, 2 * SPAN, LANES), bf16),
            pltpu.VMEM((8, LANES, LANES), bf16),
            pltpu.VMEM((8, LANES, LANES), bf16),
            pltpu.VMEM((ROWS, LANES), f32),
            pltpu.VMEM((ROWS, LANES), f32),
            pltpu.VMEM((ROWS, LANES), f32),
            pltpu.VMEM((NLAG, ROWS, LANES), f32),
            pltpu.VMEM((8, LANES), f32),
            pltpu.VMEM((8, LANES), f32),
            pltpu.VMEM((ZROWS, LANES), f32),
            pltpu.VMEM((ZROWS, LANES), f32),
            pltpu.VMEM((8, ZROWS, LANES), f32),
            pltpu.VMEM((8, ZROWS, LANES), f32),
            pltpu.VMEM((8, DEPTH + 16, LANES), bf16),
            pltpu.VMEM((DEPTH, LANES), bf16),
            pltpu.VMEM((DEPTH // LANES, LANES, LANES), bf16),
            dma((5,)), dma((4,)), dma((4,)), dma((8,)), dma((8,)), dma((16,)), dma((TM,)), dma((16,)), dma((TM,)),
            dma((16,)), dma((16,)), dma((8,)), dma((8,)),
        ],
        compiler_params=pltpu.CompilerParams(
            collective_id=0, has_side_effects=True, vmem_limit_bytes=60 * 1024 * 1024),
    )(rows, detector_ids.reshape(12, LANES), template_ids.T, intersection, lags)
    return out.astype(f32)


def solution(mesh):
    in_specs = (P("tm", None, "freq"), P(), P(), P(), P("tm", None))
    out_specs = P("tm", "freq")
    return jax.shard_map(shards, mesh=mesh, in_specs=in_specs, out_specs=out_specs, check_vma=False)
```
